256 devices in a mesh: grid: 32 (over z, y), atom: 8 (over x, core).
Axes of the slice: x: 4, y: 4, z: 8, core: 2. Of those that a mesh axis runs over, the one named last changes fastest.
Arguments:
- weights: float32 [4194304], P(('grid', 'atom')), may hold values from 0.25 to 4
- target: float32 [4194304], P(('grid', 'atom')), may hold values from -6 to 6
- coupling: float32 [4194304], P(('grid', 'atom')), may hold values from -0.9 to 0.9
- multipole_basis: float32 [25, 4194304], P(None, ('grid', 'atom')), may hold values from -6 to 6
- rho_hist: float32 [8, 4194304], P(None, ('grid', 'atom')), may hold values from -6 to 6
- res_hist: float32 [8, 4194304], P(None, ('grid', 'atom')), may hold values from -6 to 6
- batch_atom: int32 [16384], P(('grid', 'atom')), may hold values from 0 to 4095
- owner_slot: int32 [4096], replicated, may hold values from 0 to 4095, each once
- slot_index: int32 [2], replicated, may hold values from 0 to 7
Outputs:
- density: float32 [4194304], P(('grid', 'atom'))
- moments: float32 [25, 4096], P(None, 'atom')
The draws below stay inside these ranges and needn't reach their ends.
Inputs may be any that keep to these rules, and one draw needn't show every extreme that they name: `owner_slot`: each slot 0 to 4095 belongs to exactly one atom.
All inputs are finite; a program needn't handle non-finite values.
Results may differ from the reference program's by a relative error of at most 0.00011.
Values sent between devices are 32-bit elements; how exact they have to be, the bound alone decides.
A program may use at most 64 MiB of HBM per device.

```python
import math
import jax
import jax.numpy as jnp
import numpy as np
from jax import lax

H = 8
LM = 25
BATCH = 256
ITERS = 2
POINTS = 4194304
BATCHES = 16384
ATOMS = 4096
ATOM_PTS = 1024


def place_ends(result, key, least, largest):
    spot = [jax.random.randint(jax.random.fold_in(key, axis), (), 0, length) for axis, length in enumerate(result.shape)]
    longest = result.shape.index(max(result.shape))
    neighbour = spot[:longest] + [(spot[longest] + 1) % result.shape[longest]] + spot[longest + 1:]
    return result.at[tuple(spot)].set(least).at[tuple(neighbour)].set(largest)


def levels(own_key, dims, pieces, smallest, top_value):
    def one(position, shards_of):
        heights = jax.random.uniform(jax.random.fold_in(jax.random.fold_in(own_key, 6), position), (shards_of,), jnp.float32, smallest / len(pieces), top_value / len(pieces))
        return jnp.repeat(jnp.exp(heights), dims[position] // shards_of).reshape((-1,) + (1,) * (len(dims) - position - 1))

    gain = one(*pieces[0])
    for cut in pieces[1:]:
        gain = gain * one(*cut)
    return gain


def noise(stream_key, shape, scale, reach, shards=(), held_as=jnp.bfloat16):
    gain = levels(stream_key, shape, shards, -0.22, 0.18) if shards else 1.0
    entries = jax.random.normal(stream_key, shape, jnp.float32) * scale * gain
    return jnp.minimum(jnp.maximum(entries, -reach), reach).astype(held_as)


def setup_inputs(seed: int = 0) -> dict:
    splits = jax.random.split(jax.random.key(seed), 10)
    return {
        "weights": jnp.clip(jnp.exp(math.log(4.0) - 2.7725887 * jax.random.uniform(splits[0], (POINTS,), jnp.float32) ** levels(splits[0], (POINTS,), ((0, 256),), -0.2, 0.2)), 0.25, 4.0),
        "target": noise(splits[1], (POINTS,), 1.0, 6.0, ((0, 256),), jnp.float32),
        "coupling": jnp.clip(jax.random.uniform(splits[2], (POINTS,), jnp.float32, -0.9, 0.9) * levels(splits[2], (POINTS,), ((0, 256),), -0.4, 0.0), -0.9, 0.9),
        "multipole_basis": noise(splits[3], (LM, POINTS), 1.0, 6.0, ((1, 256),), jnp.float32),
        "rho_hist": noise(splits[4], (H, POINTS), 1.0, 6.0, ((1, 256),), jnp.float32),
        "res_hist": noise(splits[5], (H, POINTS), 1.0, 6.0, ((1, 256),), jnp.float32),
        "batch_atom": place_ends(jax.random.randint(splits[6], (BATCHES,), 0, ATOMS), jax.random.fold_in(splits[6], 1), 0, ATOMS - 1).astype(jnp.int32),
        "owner_slot": jax.random.permutation(splits[7], ATOMS).astype(jnp.int32),
        "slot_index": jax.random.randint(splits[8], (ITERS,), 0, H).astype(jnp.int32),
    }


damping_table = np.array([1.0 / (1 + degree) for degree in range(5) for order in range(2 * degree + 1)], dtype=np.float32)
mixing_beta = 0.5
ridge_share = 0.1

def mixing_weights(intersect):
    hist_len = intersect.shape[0]
    ridge_val = ridge_share * jnp.trace(intersect) / hist_len
    shifted = intersect + ridge_val * jnp.eye(hist_len, dtype=intersect.dtype)
    factor = jnp.linalg.cholesky(shifted)
    forward = []
    for row_at in range(hist_len):
        entry_val = 1.0
        for col_at in range(row_at):
            entry_val = entry_val - factor[row_at, col_at] * forward[col_at]
        forward.append(entry_val / factor[row_at, row_at])
    backward = [None] * hist_len
    for row_at in reversed(range(hist_len)):
        entry_val = forward[row_at]
        for col_at in range(row_at + 1, hist_len):
            entry_val = entry_val - factor[col_at, row_at] * backward[col_at]
        backward[row_at] = entry_val / factor[row_at, row_at]
    solved = jnp.stack(backward)
    return solved / jnp.sum(solved)

def reference(weights, target, coupling, multipole_basis, rho_hist, res_hist, batch_atom, owner_slot, slot_index):
    hi_prec = lax.Precision.HIGHEST
    damping = jnp.asarray(damping_table, dtype=weights.dtype)
    batch_slot = owner_slot[batch_atom].astype(jnp.int32)
    basis_blocks = multipole_basis.reshape(LM, BATCHES, BATCH)
    density = None
    moments = None
    for iteration in range(ITERS):
        intersect = jnp.dot(res_hist * weights[None, :], res_hist.T, precision=hi_prec)
        coeffs = mixing_weights(intersect)
        rho_mix = jnp.dot(coeffs, rho_hist, precision=hi_prec)
        res_mix = jnp.dot(coeffs, res_hist, precision=hi_prec)
        per_batch = lax.optimization_barrier(jnp.sum((weights * res_mix).reshape(1, BATCHES, BATCH) * basis_blocks, axis=2))
        moments = jax.ops.segment_sum(per_batch.T, batch_slot, num_segments=ATOMS).T / jnp.sqrt(jnp.float32(ATOM_PTS)).astype(weights.dtype)
        at_batch = damping[:, None] * moments[:, batch_slot]
        correct = lax.optimization_barrier(jnp.sum(at_batch[:, :, None] * basis_blocks, axis=0)).reshape(POINTS)
        density = rho_mix + mixing_beta * (res_mix - correct)
        res_new = target + coupling * jnp.tanh(density) - density
        where = slot_index[iteration]
        rho_hist = rho_hist.at[where].set(density)
        res_hist = res_hist.at[where].set(res_new)
    return (density, moments)
```

```python
import functools
import math

import jax
import jax.numpy as jnp
import numpy as np
from jax import lax
from jax.experimental import pallas as pl
from jax.experimental.pallas import tpu as pltpu
from jax.sharding import PartitionSpec as P

H = 8
LM = 25
ITERS = 2
BETA = 0.5
RIDGE = 0.1
LANES = 128
NZ, NY, NX, NC = 8, 4, 4, 2
PLANE = NY * NX * NC
MESH = pl.DeviceIdType.MESH
F32 = jnp.float32
I32 = jnp.int32


def kernel(
    tiles, batches, scale,
    w_hbm, tgt_hbm, cpl_hbm, basis_hbm, rho_hbm, res_hbm, atom_sm, owner_sm, hist_sm,
    dens_out, mom_out,
    w, tgt, cpl, basis, rho, res,
    slot_send, slot_recv, irow_send, irow_recv, zrow_send, zrow_recv,
    raw_send, raw_recv, part_send, part_recv, back_send, back_recv, blk_send, blk_recv,
    onehot, xparts,
    load_sem,
    slot_ss, slot_rs, irow_ss, irow_rs, zrow_ss, zrow_rs,
    raw_ss, raw_rs, part_ss, part_rs, back_ss, back_rs, blk_ss, blk_rs,
):
    grid = lax.axis_index("grid")
    atom = lax.axis_index("atom")
    z, y = grid // NY, grid % NY
    x, c = atom // NC, atom % NC
    me = y * (NX * NC) + atom

    ys = [(y + d) % NY for d in range(NY)]
    xs = [(x + d) % NX for d in range(NX)]
    cs = [c, 1 - c]
    peers = []
    for dy in (2, 1, 3, 0):
        for dx in (2, 1, 3, 0):
            for dc in (1, 0):
                if dy or dx or dc:
                    pa = xs[dx] * NC + cs[dc]
                    peers.append((z * NY + ys[dy], pa, ys[dy] * (NX * NC) + pa))
    zpeers = []
    for dz in (4, 3, 5, 2, 6, 1, 7):
        pz = (z + dz) % NZ
        zpeers.append((pz * NY + y, atom, pz))
    ypeers = [(z * NY + ys[dy], atom, ys[dy]) for dy in (2, 1, 3)]

    barrier = pltpu.get_barrier_semaphore()
    for pg, pa, _ in peers + zpeers:
        pl.semaphore_signal(barrier, inc=1, device_id=(pg, pa), device_id_type=MESH)

    loads = [
        pltpu.make_async_copy(src, dst, load_sem.at[n])
        for n, (src, dst) in enumerate(
            [(w_hbm, w), (res_hbm, res), (basis_hbm, basis), (rho_hbm, rho), (tgt_hbm, tgt), (cpl_hbm, cpl)]
        )
    ]
    for load in loads:
        load.start()

    sub = lax.broadcasted_iota(I32, (8, LANES), 0)
    lane = lax.broadcasted_iota(I32, (8, LANES), 1)
    low = lane < 64

    def to_peers(targets, src, dst, slot, ssem, rsem, per_peer=False):
        copies = []
        for n, (pg, pa, pslot) in enumerate(targets):
            copy = pltpu.make_async_remote_copy(
                src_ref=src.at[pslot] if per_peer else src,
                dst_ref=dst.at[slot],
                send_sem=ssem.at[n],
                recv_sem=rsem.at[slot],
                device_id=(pg, pa),
                device_id_type=MESH,
            )
            copy.start()
            copies.append(copy)
        return copies

    def arrived(targets, src, dst, ssem, rsem, per_peer=False):
        for n, (pg, pa, pslot) in enumerate(targets):
            pltpu.make_async_remote_copy(
                src_ref=src.at[pslot] if per_peer else src,
                dst_ref=dst.at[pslot],
                send_sem=ssem.at[n],
                recv_sem=rsem.at[pslot],
                device_id=(pg, pa),
                device_id_type=MESH,
            ).wait_recv()

    def tree_sum(parts):
        parts = list(parts)
        while len(parts) > 1:
            parts = [a + b for a, b in zip(parts[::2], parts[1::2])] + ([parts[-1]] if len(parts) % 2 else [])
        return parts[0]

    def over_subs(v):
        v = v + pltpu.roll(v, 4, 0)
        v = v + pltpu.roll(v, 2, 0)
        return v + pltpu.roll(v, 1, 0)

    def tile_at(ref, at):
        return ref[:, pl.ds(pl.multiple_of(at * LANES, LANES), LANES)]

    def row_at(ref, at):
        return jnp.broadcast_to(ref[pl.ds(at, 1), :], (8, LANES))

    def basis_tile(kt, at):
        cols = pl.ds(pl.multiple_of(at * LANES, LANES), LANES)
        if kt < 3:
            return basis[pl.ds(kt * 8, 8), cols]
        return jnp.broadcast_to(basis[pl.ds(24, 1), cols], (8, LANES))

    def row_of(columns):
        total = jnp.zeros((8, LANES), F32)
        for d, column in enumerate(columns):
            total = jnp.where(lane == d * 8 + sub, column, total)
        return over_subs(total)

    sends = []

    def all_summed(row, it):
        irow_send[it] = row[0:1]
        sends.extend(to_peers(peers, irow_send.at[it], irow_recv.at[it], me, irow_ss.at[it], irow_rs.at[it]))
        return row

    def plane_sum(it):
        arrived(peers, irow_send.at[it], irow_recv.at[it], irow_ss.at[it], irow_rs.at[it])
        row = tree_sum([irow_send[it]] + [irow_recv[it, pslot] for _, _, pslot in peers])
        zrow_send[it] = row
        sends.extend(to_peers(zpeers, zrow_send.at[it], zrow_recv.at[it], z, zrow_ss.at[it], zrow_rs.at[it]))

    def slice_sum(it):
        arrived(zpeers, zrow_send.at[it], zrow_recv.at[it], zrow_ss.at[it], zrow_rs.at[it])
        row = tree_sum([zrow_send[it]] + [zrow_recv[it, pslot] for _, _, pslot in zpeers])
        return jnp.broadcast_to(row, (8, LANES))

    def mixing(total):
        def entry(i, j):
            d = (i - j) % 8
            at = d * 8 + i if d <= 4 else (8 - d) * 8 + j
            return jnp.broadcast_to(total[:, at : at + 1], (8, LANES))

        a = {(i, j): entry(i, j) for i in range(H) for j in range(i + 1)}
        ridge = RIDGE * tree_sum([a[i, i] for i in range(H)]) / H
        for i in range(H):
            a[i, i] = a[i, i] + ridge
        ones = jnp.ones((8, LANES), F32)
        rhs = [ones] * H
        inverse = []
        factor = {}
        for k in range(H):
            inv = 1.0 / a[k, k]
            inverse.append(inv)
            for i in range(k + 1, H):
                factor[i, k] = a[i, k] * inv
            for i in range(k + 1, H):
                for j in range(k + 1, i + 1):
                    a[i, j] = a[i, j] - factor[i, k] * a[j, k]
                rhs[i] = rhs[i] - factor[i, k] * rhs[k]
        solved = [None] * H
        for k in reversed(range(H)):
            value = rhs[k] * inverse[k]
            for i in range(k + 1, H):
                value = value - factor[i, k] * solved[i]
            solved[k] = value
        share = 1.0 / tree_sum(solved)
        column = solved[0]
        for i in range(1, H):
            column = jnp.where(sub == i, solved[i], column)
        return column * share

    def raw_moments(column):
        def step(b, accs):
            accs = list(accs)
            sums = [None] * 4
            for half in range(2):
                at = b * 2 + half
                wr = over_subs(tile_at(res, at) * column) * row_at(w, at)
                for kt in range(4):
                    part = basis_tile(kt, at) * wr
                    sums[kt] = part if half == 0 else sums[kt] + part
            here = lane == b
            return tuple(
                jnp.where(here, jnp.sum(sums[kt], axis=1, keepdims=True), accs[kt]) for kt in range(4)
            )

        zero = jnp.zeros((8, LANES), F32)
        return lax.fori_loop(0, batches, step, (zero,) * 4, unroll=4)

    def packed(t0, t1, t2, t3):
        first = jnp.where(low, t0, pltpu.roll(t1, 64, 1))
        second = jnp.where(
            sub < 4,
            jnp.where(low, t2, pltpu.roll(pltpu.roll(t2, 4, 0), 64, 1)),
            jnp.where((sub == 4) & low, pltpu.roll(t3, 4, 0), 0.0),
        )
        return first, second

    def unpacked(first, second):
        moved = pltpu.roll(second, 64, 1)
        t2 = jnp.where(sub < 4, second, pltpu.roll(moved, 4, 0))
        t3 = jnp.where(sub == 0, pltpu.roll(second, 4, 0), 0.0)
        return first, pltpu.roll(first, 64, 1), t2, t3

    def three(v):
        hi = v.astype(jnp.bfloat16)
        rest = v - hi.astype(F32)
        mid = rest.astype(jnp.bfloat16)
        lo = (rest - mid.astype(F32)).astype(jnp.bfloat16)
        return hi, mid, lo

    def pair_joined(a, b):
        return jnp.where(low, a, pltpu.roll(b, 64, 1)), jnp.where(low, pltpu.roll(a, 64, 1), b)

    def owner_partial(it):
        for pair in range(PLANE // 2):
            cols = pl.ds(pair * LANES, LANES)
            for half in range(2):
                rows = pl.ds(half * 8, 8)
                a, b = pair_joined(raw_recv[it, 2 * pair, rows, :], raw_recv[it, 2 * pair + 1, rows, :])
                both = jnp.concatenate([a, b], axis=0)
                for n, part in enumerate(three(both)):
                    xparts[pl.ds(n * 32 + half * 16, 16), cols] = part
        sums = lax.dot_general(xparts[...], onehot[...], (((1,), (1,)), ((), ())), preferred_element_type=F32)
        sums = sums[0:32] + sums[32:64] + sums[64:96]
        part_send[it, 0:16] = sums[0:16]
        part_send[it, 16:24] = jnp.where(sub < 4, sums[16:24], pltpu.roll(sums[24:32], 4, 0))
        part_send[it, 24:32] = jnp.where(sub < 1, pltpu.roll(sums[16:24], 4, 0), 0.0)

    def back_values(it, block):
        tiles_of = [block[kt * 8 : kt * 8 + 8] for kt in range(4)]
        degree = [lax.broadcasted_iota(I32, (8, LANES), 0) + kt * 8 for kt in range(4)]
        damped = []
        for kt in range(4):
            k = degree[kt]
            damp = jnp.where(k < 1, 1.0, jnp.where(k < 4, 1 / 2, jnp.where(k < 9, 1 / 3, jnp.where(k < 16, 1 / 4, 1 / 5))))
            damped.append(tiles_of[kt] * damp)
        low_rows = jnp.where(sub < 4, damped[2], jnp.where(sub == 4, pltpu.roll(damped[3], 4, 0), 0.0))
        high_rows = jnp.where(sub < 4, pltpu.roll(damped[2], 4, 0), 0.0)
        rows = jnp.concatenate([damped[0], damped[1], low_rows, high_rows], axis=0)
        picked = jnp.dot(jnp.concatenate(three(rows), axis=0), onehot[...], preferred_element_type=F32)
        picked = picked[0:32] + picked[32:64] + picked[64:96]
        for pair in range(PLANE // 2):
            cols = slice(pair * LANES, (pair + 1) * LANES)
            for half in range(2):
                a, b = pair_joined(picked[half * 16 : half * 16 + 8, cols], picked[half * 16 + 8 : half * 16 + 16, cols])
                back_send[it, 2 * pair, half * 8 : half * 8 + 8, :] = a
                back_send[it, 2 * pair + 1, half * 8 : half * 8 + 8, :] = b

    loads[0].wait()
    loads[1].wait()

    def products(step_at, accs):
        accs = list(accs)
        for u in range(4):
            at = step_at * 4 + u
            r = tile_at(res, at)
            wr = r * row_at(w, at)
            accs[0] = accs[0] + wr * r
            for d in range(1, 5):
                accs[d] = accs[d] + wr * pltpu.roll(r, d, 0)
        return tuple(accs)

    accs = lax.fori_loop(0, tiles // 4, products, (jnp.zeros((8, LANES), F32),) * 5)
    first_row = row_of([jnp.sum(acc, axis=1, keepdims=True) for acc in accs])

    pl.semaphore_wait(barrier, len(peers) + len(zpeers))
    all_summed(first_row, 0)

    def slot_step(b, row):
        return jnp.where(lane == b, owner_sm[atom_sm[b]], row)

    slots = lax.fori_loop(0, batches, slot_step, jnp.full((8, LANES), -1, I32), unroll=4)
    slot_send[...] = slots[0:1]
    slot_recv[me] = slots[0:1]
    sends.extend(to_peers(peers, slot_send, slot_recv, me, slot_ss, slot_rs))
    for load in loads[2:]:
        load.wait()

    plane_sum(0)

    arrived(peers, slot_send, slot_recv, slot_ss, slot_rs)
    first_slot = atom * 512 + y * LANES
    for pair in range(PLANE // 2):
        left = jnp.broadcast_to(slot_recv[2 * pair], (8, LANES))
        right = jnp.broadcast_to(slot_recv[2 * pair + 1], (8, LANES))
        rel = jnp.where(low, left, pltpu.roll(right, 64, 1)) - first_slot
        for st in range(LANES // 16):
            halves = [jnp.where(rel == sub + (st * 16 + h * 8), 1.0, 0.0) for h in range(2)]
            onehot[pl.ds(st * 16, 16), pl.ds(pair * LANES, LANES)] = jnp.concatenate(halves, axis=0).astype(jnp.bfloat16)

    total = slice_sum(0)
    for it in range(ITERS):
        column = mixing(total)
        for rows, value in zip((pl.ds(0, 8), pl.ds(8, 8)), packed(*raw_moments(column))):
            raw_send[it, rows, :] = value
            raw_recv[it, me, rows, :] = value
        sends.extend(to_peers(peers, raw_send.at[it], raw_recv.at[it], me, raw_ss.at[it], raw_rs.at[it]))
        arrived(peers, raw_send.at[it], raw_recv.at[it], raw_ss.at[it], raw_rs.at[it])
        owner_partial(it)
        sends.extend(to_peers(zpeers, part_send.at[it], part_recv.at[it], z, part_ss.at[it], part_rs.at[it]))
        arrived(zpeers, part_send.at[it], part_recv.at[it], part_ss.at[it], part_rs.at[it])
        block = tree_sum([part_send[it]] + [part_recv[it, pslot] for _, _, pslot in zpeers]) * scale
        if it == ITERS - 1:
            blk_send[...] = block
            sends.extend(to_peers(ypeers, blk_send, blk_recv, y, blk_ss, blk_rs))
            blk_recv[y] = block
        back_values(it, block)
        sends.extend(
            to_peers(peers, back_send.at[it], back_recv.at[it], me, back_ss.at[it], back_rs.at[it], per_peer=True)
        )
        arrived(peers, back_send.at[it], back_recv.at[it], back_ss.at[it], back_rs.at[it], per_peer=True)
        mine = tree_sum([back_send[it, me]] + [back_recv[it, pslot] for _, _, pslot in peers]) * BETA
        at_batch = unpacked(mine[0:8], mine[8:16])
        hist_at = hist_sm[it]

        def density_step(group, carry):
            at_tiles, acc = carry
            for u in range(8):
                spread = [jnp.broadcast_to(t[:, u : u + 1], (8, LANES)) for t in at_tiles]
                for half in range(2):
                    at = (group * 8 + u) * 2 + half
                    cols = pl.ds(pl.multiple_of(at * LANES, LANES), LANES)
                    r, q = res[:, cols], rho[:, cols]
                    v = column * (q + BETA * r)
                    corr = tree_sum([basis_tile(kt, at) * spread[kt] for kt in range(4)])
                    dens = over_subs(v - corr)
                    if it == ITERS - 1:
                        dens_out[pl.ds(at, 1), :] = dens[0:1]
                    else:
                        new = row_at(tgt, at) + row_at(cpl, at) * jnp.tanh(dens) - dens
                        r = jnp.where(sub == hist_at, new, r)
                        res[:, cols] = r
                        rho[:, cols] = jnp.where(sub == hist_at, dens, q)
                        acc = acc + r * (new * row_at(w, at))
            return tuple(pltpu.roll(t, LANES - 8, 1) for t in at_tiles), acc

        _, acc = lax.fori_loop(0, batches // 8, density_step, (at_batch, jnp.zeros((8, LANES), F32)))
        if it < ITERS - 1:
            mine_new = jnp.broadcast_to(jnp.sum(acc, axis=1, keepdims=True), (8, LANES))
            columns = [
                jnp.where(sub == hist_at, pltpu.roll(mine_new, d, 0) if d else mine_new, mine_new) for d in range(5)
            ]
            all_summed(row_of(columns), it + 1)
            plane_sum(it + 1)
            row_i = lane % 8
            row_j = (row_i - lane // 8 + 8) % 8
            total = jnp.where((row_i == hist_at) | (row_j == hist_at), slice_sum(it + 1), total)

    arrived(ypeers, blk_send, blk_recv, blk_ss, blk_rs)
    for q in range(NY):
        mom_out[:, q * LANES : (q + 1) * LANES] = blk_recv[q, 0:LM]
    for copy in sends:
        copy.wait_send()


def local(weights, target, coupling, multipole_basis, rho_hist, res_hist, batch_atom, owner_slot, slot_index):
    points = weights.shape[0]
    batches = batch_atom.shape[0]
    tiles = points // LANES
    slots = owner_slot.shape[0]
    owned = slots // lax.axis_size("atom")
    scale = 1.0 / math.sqrt(points * lax.axis_size("grid") // owned)
    square = lambda v: v.reshape(tiles, LANES)
    vm, dma = pltpu.VMEM, pltpu.SemaphoreType.DMA
    anywhere = pl.BlockSpec(memory_space=pl.ANY)
    smem = pl.BlockSpec(memory_space=pltpu.SMEM)
    vmem = pl.BlockSpec(memory_space=pltpu.VMEM)
    density, moments = pl.pallas_call(
        functools.partial(kernel, tiles, batches, scale),
        out_shape=(jax.ShapeDtypeStruct((tiles, LANES), F32), jax.ShapeDtypeStruct((LM, owned), F32)),
        in_specs=[anywhere] * 6 + [smem] * 3,
        out_specs=(vmem, vmem),
        scratch_shapes=[
            vm((tiles, LANES), F32), vm((tiles, LANES), F32), vm((tiles, LANES), F32),
            vm((LM, points), F32), vm((H, points), F32), vm((H, points), F32),
            vm((1, LANES), I32), vm((PLANE, 1, LANES), I32),
            vm((ITERS, 1, LANES), F32), vm((ITERS, PLANE, 1, LANES), F32),
            vm((ITERS, 1, LANES), F32), vm((ITERS, NZ, 1, LANES), F32),
            vm((ITERS, 16, LANES), F32), vm((ITERS, PLANE, 16, LANES), F32),
            vm((ITERS, 32, LANES), F32), vm((ITERS, NZ, 32, LANES), F32),
            vm((ITERS, PLANE, 16, LANES), F32), vm((ITERS, PLANE, 16, LANES), F32),
            vm((32, LANES), F32), vm((NY, 32, LANES), F32),
            vm((LANES, PLANE * 64), jnp.bfloat16), vm((96, PLANE * 64), jnp.bfloat16),
            dma((6,)),
            dma((31,)), dma((PLANE,)),
            dma((ITERS, 31)), dma((ITERS, PLANE)),
            dma((ITERS, 7)), dma((ITERS, NZ)),
            dma((ITERS, 31)), dma((ITERS, PLANE)),
            dma((ITERS, 7)), dma((ITERS, NZ)),
            dma((ITERS, 31)), dma((ITERS, PLANE)),
            dma((3,)), dma((NY,)),
        ],
        compiler_params=pltpu.CompilerParams(collective_id=0, has_side_effects=True),
    )(
        square(weights), square(target), square(coupling), multipole_basis, rho_hist, res_hist,
        batch_atom, owner_slot, slot_index,
    )
    return density.reshape(points), moments


def solution(mesh):
    both = ("grid", "atom")
    placed = (P(both), P(both), P(both), P(None, both), P(None, both), P(None, both), P(both), P(), P())
    return jax.shard_map(
        local, mesh=mesh, in_specs=placed, out_specs=(P(both), P(None, "atom")), check_vma=False
    )
```

```python
import functools
import math

import jax
import jax.numpy as jnp
import numpy as np
from jax import lax
from jax.experimental import pallas as pl
from jax.experimental.pallas import tpu as pltpu
from jax.sharding import PartitionSpec as P

H = 8
LM = 25
ITERS = 2
BETA = 0.5
RIDGE = 0.1
LANES = 128
NZ, NY, NX, NC = 8, 4, 4, 2
PLANE = NY * NX * NC
MESH = pl.DeviceIdType.MESH
F32 = jnp.float32
I32 = jnp.int32


def kernel(
    tiles, batches, scale,
    w_hbm, tgt_hbm, cpl_hbm, basis_hbm, rho_hbm, res_hbm, atom_hbm, owner_hbm, hist_hbm,
    dens_out, mom_out,
    w, tgt, cpl, basis, rho, res, fresh, weighted, merged, hist_moms,
    atom_sm, owner_sm, hist_sm,
    slot_send, slot_recv, zslot_recv, irow_send, irow_recv, zrow_send, zrow_recv,
    raw_send, raw_recv, part_send, part_recv, back_send, back_recv, blk_send, blk_recv,
    match, xparts,
    load_sem,
    slot_ss, slot_rs, zslot_ss, zslot_rs, irow_ss, irow_rs, zrow_ss, zrow_rs,
    raw_ss, raw_rs, part_ss, part_rs, back_ss, back_rs, blk_ss, blk_rs,
):
    grid = lax.axis_index("grid")
    atom = lax.axis_index("atom")
    z, y = grid // NY, grid % NY
    x, c = atom // NC, atom % NC
    me = y * (NX * NC) + atom

    ys = [(y + d) % NY for d in range(NY)]
    xs = [(x + d) % NX for d in range(NX)]
    cs = [c, 1 - c]
    peers = []
    for dy in (2, 1, 3, 0):
        for dx in (2, 1, 3, 0):
            for dc in (1, 0):
                if dy or dx or dc:
                    pa = xs[dx] * NC + cs[dc]
                    peers.append((z * NY + ys[dy], pa, ys[dy] * (NX * NC) + pa))
    zpeers = []
    for dz in (4, 3, 5, 2, 6, 1, 7):
        pz = (z + dz) % NZ
        zpeers.append((pz * NY + y, atom, pz))
    ypeers = [(z * NY + ys[dy], atom, ys[dy]) for dy in (2, 1, 3)]

    barrier = pltpu.get_barrier_semaphore()
    for pg, pa, _ in peers + zpeers:
        pl.semaphore_signal(barrier, inc=1, device_id=(pg, pa), device_id_type=MESH)

    loads = [
        pltpu.make_async_copy(src, dst, load_sem.at[n])
        for n, (src, dst) in enumerate(
            [
                (w_hbm, w), (res_hbm, res), (basis_hbm, basis), (atom_hbm, atom_sm), (owner_hbm, owner_sm),
                (hist_hbm, hist_sm), (rho_hbm, rho), (tgt_hbm, tgt), (cpl_hbm, cpl),
            ]
        )
    ]
    for load in loads:
        load.start()

    sub = lax.broadcasted_iota(I32, (8, LANES), 0)
    lane = lax.broadcasted_iota(I32, (8, LANES), 1)
    low = lane < 64

    def to_peers(targets, src, dst, slot, ssem, rsem, per_peer=False):
        copies = []
        for n, (pg, pa, pslot) in enumerate(targets):
            copy = pltpu.make_async_remote_copy(
                src_ref=src.at[pslot] if per_peer else src,
                dst_ref=dst.at[slot],
                send_sem=ssem.at[n],
                recv_sem=rsem.at[slot],
                device_id=(pg, pa),
                device_id_type=MESH,
            )
            copy.start()
            copies.append(copy)
        return copies

    def arrived(targets, src, dst, ssem, rsem, per_peer=False):
        for n, (pg, pa, pslot) in enumerate(targets):
            pltpu.make_async_remote_copy(
                src_ref=src.at[pslot] if per_peer else src,
                dst_ref=dst.at[pslot],
                send_sem=ssem.at[n],
                recv_sem=rsem.at[pslot],
                device_id=(pg, pa),
                device_id_type=MESH,
            ).wait_recv()

    def tree_sum(parts):
        parts = list(parts)
        while len(parts) > 1:
            parts = [a + b for a, b in zip(parts[::2], parts[1::2])] + ([parts[-1]] if len(parts) % 2 else [])
        return parts[0]

    def over_subs(v):
        v = v + pltpu.roll(v, 4, 0)
        v = v + pltpu.roll(v, 2, 0)
        return v + pltpu.roll(v, 1, 0)

    def tile_at(ref, at):
        return ref[:, pl.ds(pl.multiple_of(at * LANES, LANES), LANES)]

    def row_at(ref, at):
        return jnp.broadcast_to(ref[pl.ds(at, 1), :], (8, LANES))

    def basis_tile(kt, at):
        cols = pl.ds(pl.multiple_of(at * LANES, LANES), LANES)
        if kt < 3:
            return basis[pl.ds(kt * 8, 8), cols]
        return jnp.broadcast_to(basis[pl.ds(24, 1), cols], (8, LANES))

    def row_of(columns):
        total = jnp.zeros((8, LANES), F32)
        for d, column in enumerate(columns):
            total = jnp.where(lane == d * 8 + sub, column, total)
        return over_subs(total)

    sends = []

    def all_summed(row, it):
        irow_send[it] = row[0:1]
        sends.extend(to_peers(peers, irow_send.at[it], irow_recv.at[it], me, irow_ss.at[it], irow_rs.at[it]))
        return row

    def plane_sum(it):
        arrived(peers, irow_send.at[it], irow_recv.at[it], irow_ss.at[it], irow_rs.at[it])
        row = tree_sum([irow_send[it]] + [irow_recv[it, pslot] for _, _, pslot in peers])
        zrow_send[it] = row
        sends.extend(to_peers(zpeers, zrow_send.at[it], zrow_recv.at[it], z, zrow_ss.at[it], zrow_rs.at[it]))

    def slice_sum(it):
        arrived(zpeers, zrow_send.at[it], zrow_recv.at[it], zrow_ss.at[it], zrow_rs.at[it])
        row = tree_sum([zrow_send[it]] + [zrow_recv[it, pslot] for _, _, pslot in zpeers])
        return jnp.broadcast_to(row, (8, LANES))

    def mixing(total):
        def entry(i, j):
            d = (i - j) % 8
            at = d * 8 + i if d <= 4 else (8 - d) * 8 + j
            return jnp.broadcast_to(total[:, at : at + 1], (8, LANES))

        a = {(i, j): entry(i, j) for i in range(H) for j in range(i + 1)}
        ridge = RIDGE * tree_sum([a[i, i] for i in range(H)]) / H
        for i in range(H):
            a[i, i] = a[i, i] + ridge
        ones = jnp.ones((8, LANES), F32)
        rhs = [ones] * H
        inverse = []
        factor = {}
        for k in range(H):
            inv = 1.0 / a[k, k]
            inverse.append(inv)
            for i in range(k + 1, H):
                factor[i, k] = a[i, k] * inv
            for i in range(k + 1, H):
                for j in range(k + 1, i + 1):
                    a[i, j] = a[i, j] - factor[i, k] * a[j, k]
                rhs[i] = rhs[i] - factor[i, k] * rhs[k]
        solved = [None] * H
        for k in reversed(range(H)):
            value = rhs[k] * inverse[k]
            for i in range(k + 1, H):
                value = value - factor[i, k] * solved[i]
            solved[k] = value
        share = 1.0 / tree_sum(solved)
        coeffs = [value * share for value in solved]
        column = coeffs[0]
        for i in range(1, H):
            column = jnp.where(sub == i, coeffs[i], column)
        return coeffs, column

    def merge(first, second, bit, axis):
        clear = ((lane if axis == 1 else sub) & bit) == 0
        return jnp.where(clear, first, second) + pltpu.roll(jnp.where(clear, second, first), bit, axis)

    def merge_all(values, bit, axis):
        while len(values) > 1:
            values = [merge(p, q, bit, axis) for p, q in zip(values[::2], values[1::2])]
            bit *= 2
        return values[0]

    def weigh(group):
        for u in range(16):
            at = group * 16 + u
            wrow = row_at(w, at)
            for kt in range(4):
                weighted[u, kt] = basis_tile(kt, at) * wrow

    def batch_sums(group, kt, field):
        return merge_all([weighted[2 * u, kt] * field(2 * u) + weighted[2 * u + 1, kt] * field(2 * u + 1) for u in range(8)], 1, 1)

    def joined(n):
        total = merge_all([merged[g, n] for g in range(batches // 8)], 8, 1)
        return total + pltpu.roll(total, 64, 1)

    def history_moments():
        def step(group, carry):
            weigh(group)

            def cols(u):
                return pl.ds(pl.multiple_of((group * 16 + u) * LANES, LANES), LANES)

            for i in range(H):
                for kt in range(3):
                    merged[group, i * 3 + kt] = batch_sums(
                        group, kt, lambda u: jnp.broadcast_to(res[pl.ds(i, 1), cols(u)], (8, LANES))
                    )
            merged[group, 24] = batch_sums(group, 3, lambda u: res[:, cols(u)])
            return carry

        lax.fori_loop(0, batches // 8, step, 0)
        for n in range(25):
            hist_moms[n] = joined(n)

    def fresh_moments(hist_at):
        def step(group, carry):
            weigh(group)
            for kt in range(4):
                merged[group, kt] = batch_sums(group, kt, lambda u: row_at(fresh, group * 16 + u))
            return carry

        lax.fori_loop(0, batches // 8, step, 0)
        for kt in range(3):
            value = joined(kt)
            for i in range(H):
                hist_moms[i * 3 + kt] = jnp.where(hist_at == i, value, hist_moms[i * 3 + kt])
        hist_moms[24] = jnp.where(sub == hist_at, joined(3), hist_moms[24])

    def raw_moments(coeffs, column):
        return [tree_sum([coeffs[i] * hist_moms[i * 3 + kt] for i in range(H)]) for kt in range(3)] + [
            over_subs(column * hist_moms[24])
        ]

    def packed(t0, t1, t2, t3):
        first = jnp.where(low, t0, t1)
        second = jnp.where(
            sub < 4, jnp.where(low, t2, pltpu.roll(t2, 4, 0)), jnp.where((sub == 4) & low, t3, 0.0)
        )
        return first, second

    def unpacked(first, second):
        moved = pltpu.roll(second, 64, 1)
        t2 = jnp.where(sub < 4, second, pltpu.roll(moved, 4, 0))
        t3 = jnp.where(sub == 0, pltpu.roll(second, 4, 0), 0.0)
        return first, pltpu.roll(first, 64, 1), t2, t3

    def three(v):
        hi = v.astype(jnp.bfloat16)
        rest = v - hi.astype(F32)
        mid = rest.astype(jnp.bfloat16)
        lo = (rest - mid.astype(F32)).astype(jnp.bfloat16)
        return hi, mid, lo

    def pair_joined(a, b):
        return jnp.where(low, a, pltpu.roll(b, 64, 1)), jnp.where(low, pltpu.roll(a, 64, 1), b)

    def gather_parts(it):
        for pair in range(PLANE // 2):
            cols = pl.ds(pair * LANES, LANES)
            for half in range(2):
                rows = pl.ds(half * 8, 8)
                a, b = pair_joined(raw_recv[it, 2 * pair, rows, :], raw_recv[it, 2 * pair + 1, rows, :])
                both = jnp.concatenate([a, b], axis=0)
                for n, part in enumerate(three(both)):
                    xparts[pl.ds(n * 32 + half * 16, 16), cols] = part

    def matched(first_row, count):
        sums = lax.dot_general(
            xparts[...], match[pl.ds(first_row, count), :], (((1,), (1,)), ((), ())), preferred_element_type=F32
        )
        return sums[0:32] + sums[32:64] + sums[64:96]

    def owner_partial():
        sums = matched(NZ * 64, LANES)
        part_send[0:16] = sums[0:16]
        part_send[16:24] = jnp.where(sub < 4, sums[16:24], pltpu.roll(sums[24:32], 4, 0))
        part_send[24:32] = jnp.where(sub < 1, pltpu.roll(sums[16:24], 4, 0), 0.0)

    def peer_values(it):
        picked = matched(0, NZ * 64)
        for pair in range(NZ // 2):
            cols = slice(pair * LANES, (pair + 1) * LANES)
            for half in range(2):
                a, b = pair_joined(picked[half * 16 : half * 16 + 8, cols], picked[half * 16 + 8 : half * 16 + 16, cols])
                back_send[it, 2 * pair, half * 8 : half * 8 + 8, :] = a
                back_send[it, 2 * pair + 1, half * 8 : half * 8 + 8, :] = b

    def damped(kt, value):
        k = sub + kt * 8
        damp = jnp.where(k < 1, 1.0, jnp.where(k < 4, 1 / 2, jnp.where(k < 9, 1 / 3, jnp.where(k < 16, 1 / 4, 1 / 5))))
        return value * (damp * (scale * BETA))

    loads[0].wait()
    loads[1].wait()

    def products(step_at, accs):
        accs = list(accs)
        for u in range(4):
            at = step_at * 4 + u
            r = tile_at(res, at)
            wr = r * row_at(w, at)
            accs[0] = accs[0] + wr * r
            for d in range(1, 5):
                accs[d] = accs[d] + wr * pltpu.roll(r, d, 0)
        return tuple(accs)

    accs = lax.fori_loop(0, tiles // 4, products, (jnp.zeros((8, LANES), F32),) * 5)
    first_row = row_of([jnp.sum(acc, axis=1, keepdims=True) for acc in accs])

    loads[2].wait()
    history_moments()
    for load in loads[3:6]:
        load.wait()

    def slot_step(b, row):
        return jnp.where(lane == b, owner_sm[atom_sm[b]], row)

    slots = lax.fori_loop(0, batches, slot_step, jnp.full((8, LANES), -1, I32), unroll=4)
    slot_send[...] = slots[0:1]
    slot_recv[me] = slots[0:1]
    zslot_recv[z] = slots[0:1]

    pl.semaphore_wait(barrier, len(peers) + len(zpeers))
    all_summed(first_row, 0)
    sends.extend(to_peers(peers, slot_send, slot_recv, me, slot_ss, slot_rs))
    sends.extend(to_peers(zpeers, slot_send, zslot_recv, z, zslot_ss, zslot_rs))
    for load in loads[6:]:
        load.wait()

    plane_sum(0)

    arrived(peers, slot_send, slot_recv, slot_ss, slot_rs)
    arrived(zpeers, slot_send, zslot_recv, zslot_ss, zslot_rs)
    first_slot = atom * 512 + y * LANES
    sources = []
    for pair in range(PLANE // 2):
        left = jnp.broadcast_to(slot_recv[2 * pair], (8, LANES))
        right = jnp.broadcast_to(slot_recv[2 * pair + 1], (8, LANES))
        sources.append(jnp.where(low, left, pltpu.roll(right, 64, 1)))

    def match_rows(at, wanted):
        for pair in range(PLANE // 2):
            halves = [jnp.where(sources[pair] == one, 1.0, 0.0) for one in wanted]
            match[pl.ds(at, 16), pl.ds(pair * LANES, LANES)] = jnp.concatenate(halves, axis=0).astype(jnp.bfloat16)

    def target_step(step_at, carry):
        row = jnp.broadcast_to(zslot_recv[step_at // 4], (8, LANES)).astype(F32)
        wanted = []
        for h in range(2):
            hit = lane == sub + ((step_at % 4) * 16 + h * 8)
            column = jnp.sum(jnp.where(hit, row, 0.0), axis=1, keepdims=True)
            wanted.append(jnp.broadcast_to(column, (8, LANES)).astype(I32))
        match_rows(pl.multiple_of(step_at * 16, 16), wanted)
        return carry

    lax.fori_loop(0, NZ * 4, target_step, 0)
    for st in range(LANES // 16):
        match_rows(NZ * 64 + st * 16, [sub + (first_slot + st * 16 + h * 8) for h in range(2)])

    total = slice_sum(0)
    for it in range(ITERS):
        last = it == ITERS - 1
        coeffs, column = mixing(total)
        for rows, value in zip((pl.ds(0, 8), pl.ds(8, 8)), packed(*raw_moments(coeffs, column))):
            raw_send[it, rows, :] = value
            raw_recv[it, me, rows, :] = value
        sends.extend(to_peers(peers, raw_send.at[it], raw_recv.at[it], me, raw_ss.at[it], raw_rs.at[it]))
        arrived(peers, raw_send.at[it], raw_recv.at[it], raw_ss.at[it], raw_rs.at[it])
        gather_parts(it)
        if last:
            owner_partial()
            sends.extend(to_peers(zpeers, part_send, part_recv, z, part_ss, part_rs))
        peer_values(it)
        sends.extend(
            to_peers(zpeers, back_send.at[it], back_recv.at[it], z, back_ss.at[it], back_rs.at[it], per_peer=True)
        )
        if last:
            arrived(zpeers, part_send, part_recv, part_ss, part_rs)
            block = tree_sum([part_send[...]] + [part_recv[pslot] for _, _, pslot in zpeers]) * scale
            blk_send[...] = block
            sends.extend(to_peers(ypeers, blk_send, blk_recv, y, blk_ss, blk_rs))
            blk_recv[y] = block
        arrived(zpeers, back_send.at[it], back_recv.at[it], back_ss.at[it], back_rs.at[it], per_peer=True)
        mine = tree_sum([back_send[it, z]] + [back_recv[it, pslot] for _, _, pslot in zpeers])
        at_batch = tuple(damped(kt, t) for kt, t in enumerate(unpacked(mine[0:8], mine[8:16])))
        hist_at = hist_sm[it]

        def density_step(group, carry):
            at_tiles, acc = carry
            rows = pl.ds(pl.multiple_of(group * 8, 8), 8)
            parts = []
            for u in range(4):
                spread = [jnp.broadcast_to(t[:, u : u + 1], (8, LANES)) for t in at_tiles]
                for half in range(2):
                    at = group * 8 + u * 2 + half
                    v = column * (tile_at(rho, at) + BETA * tile_at(res, at))
                    parts.append(v - tree_sum([basis_tile(kt, at) * spread[kt] for kt in range(4)]))
            dens = merge_all(parts, 1, 0)
            if last:
                dens_out[rows, :] = dens
            else:
                new = tgt[rows, :] + cpl[rows, :] * jnp.tanh(dens) - dens
                fresh[rows, :] = new
                weighed = new * w[rows, :]
                for u in range(8):
                    cols = pl.ds(pl.multiple_of((group * 8 + u) * LANES, LANES), LANES)
                    r = jnp.where(sub == hist_at, jnp.broadcast_to(new[u : u + 1], (8, LANES)), res[:, cols])
                    res[:, cols] = r
                    rho[:, cols] = jnp.where(sub == hist_at, jnp.broadcast_to(dens[u : u + 1], (8, LANES)), rho[:, cols])
                    acc = acc + r * jnp.broadcast_to(weighed[u : u + 1], (8, LANES))
            return tuple(pltpu.roll(t, LANES - 4, 1) for t in at_tiles), acc

        _, acc = lax.fori_loop(0, batches // 4, density_step, (at_batch, jnp.zeros((8, LANES), F32)))
        if not last:
            mine_new = jnp.broadcast_to(jnp.sum(acc, axis=1, keepdims=True), (8, LANES))
            columns = [
                jnp.where(sub == hist_at, pltpu.roll(mine_new, d, 0) if d else mine_new, mine_new) for d in range(5)
            ]
            all_summed(row_of(columns), it + 1)
            fresh_moments(hist_at)
            plane_sum(it + 1)
            row_i = lane % 8
            row_j = (row_i - lane // 8 + 8) % 8
            total = jnp.where((row_i == hist_at) | (row_j == hist_at), slice_sum(it + 1), total)

    arrived(ypeers, blk_send, blk_recv, blk_ss, blk_rs)
    for q in range(NY):
        mom_out[:, q * LANES : (q + 1) * LANES] = blk_recv[q, 0:LM]
    for copy in sends:
        copy.wait_send()


def local(weights, target, coupling, multipole_basis, rho_hist, res_hist, batch_atom, owner_slot, slot_index):
    points = weights.shape[0]
    batches = batch_atom.shape[0]
    tiles = points // LANES
    slots = owner_slot.shape[0]
    owned = slots // lax.axis_size("atom")
    scale = 1.0 / math.sqrt(points * lax.axis_size("grid") // owned)
    square = lambda v: v.reshape(tiles, LANES)
    vm, sm, dma = pltpu.VMEM, pltpu.SMEM, pltpu.SemaphoreType.DMA
    anywhere = pl.BlockSpec(memory_space=pl.ANY)
    vmem = pl.BlockSpec(memory_space=pltpu.VMEM)
    density, moments = pl.pallas_call(
        functools.partial(kernel, tiles, batches, scale),
        out_shape=(jax.ShapeDtypeStruct((tiles, LANES), F32), jax.ShapeDtypeStruct((LM, owned), F32)),
        in_specs=[anywhere] * 9,
        out_specs=(vmem, vmem),
        scratch_shapes=[
            vm((tiles, LANES), F32), vm((tiles, LANES), F32), vm((tiles, LANES), F32),
            vm((LM, points), F32), vm((H, points), F32), vm((H, points), F32),
            vm((tiles, LANES), F32), vm((16, 4, 8, LANES), F32), vm((batches // 8, 25, 8, LANES), F32), vm((25, 8, LANES), F32),
            sm((batches,), I32), sm((slots,), I32), sm((ITERS,), I32),
            vm((1, LANES), I32), vm((PLANE, 1, LANES), I32), vm((NZ, 1, LANES), I32),
            vm((ITERS, 1, LANES), F32), vm((ITERS, PLANE, 1, LANES), F32),
            vm((ITERS, 1, LANES), F32), vm((ITERS, NZ, 1, LANES), F32),
            vm((ITERS, 16, LANES), F32), vm((ITERS, PLANE, 16, LANES), F32),
            vm((32, LANES), F32), vm((NZ, 32, LANES), F32),
            vm((ITERS, NZ, 16, LANES), F32), vm((ITERS, NZ, 16, LANES), F32),
            vm((32, LANES), F32), vm((NY, 32, LANES), F32),
            vm((NZ * 64 + LANES, PLANE * 64), jnp.bfloat16), vm((96, PLANE * 64), jnp.bfloat16),
            dma((9,)),
            dma((31,)), dma((PLANE,)),
            dma((7,)), dma((NZ,)),
            dma((ITERS, 31)), dma((ITERS, PLANE)),
            dma((ITERS, 7)), dma((ITERS, NZ)),
            dma((ITERS, 31)), dma((ITERS, PLANE)),
            dma((7,)), dma((NZ,)),
            dma((ITERS, 7)), dma((ITERS, NZ)),
            dma((3,)), dma((NY,)),
        ],
        compiler_params=pltpu.CompilerParams(collective_id=0, has_side_effects=True),
    )(
        square(weights), square(target), square(coupling), multipole_basis, rho_hist, res_hist,
        batch_atom, owner_slot, slot_index,
    )
    return density.reshape(points), moments


def solution(mesh):
    both = ("grid", "atom")
    placed = (P(both), P(both), P(both), P(None, both), P(None, both), P(None, both), P(both), P(), P())
    return jax.shard_map(
        local, mesh=mesh, in_specs=placed, out_specs=(P(both), P(None, "atom")), check_vma=False
    )
```

```python
import functools
import math

import jax
import jax.numpy as jnp
import numpy as np
from jax import lax
from jax.experimental import pallas as pl
from jax.experimental.pallas import tpu as pltpu
from jax.sharding import PartitionSpec as P

H = 8
LM = 25
ITERS = 2
BETA = 0.5
RIDGE = 0.1
LANES = 128
NZ, NY, NX, NC = 8, 4, 4, 2
PLANE = NY * NX * NC
MESH = pl.DeviceIdType.MESH
F32 = jnp.float32
I32 = jnp.int32


def kernel(
    tiles, batches, scale,
    w_hbm, tgt_hbm, cpl_hbm, basis_hbm, rho_hbm, res_hbm, atom_hbm, owner_hbm, hist_hbm,
    dens_out, mom_out,
    w, tgt, cpl, basis, rho, res, fresh, weighted, merged, hist_moms,
    atom_sm, owner_sm, hist_sm,
    slot_send, slot_recv, zslot_recv, irow_send, irow_recv, zrow_send, zrow_recv,
    raw_send, raw_recv, part_send, part_recv, back_send, back_recv, blk_send, blk_recv,
    match, xparts,
    load_sem,
    slot_ss, slot_rs, zslot_ss, zslot_rs, irow_ss, irow_rs, zrow_ss, zrow_rs,
    raw_ss, raw_rs, part_ss, part_rs, back_ss, back_rs, blk_ss, blk_rs,
):
    grid = lax.axis_index("grid")
    atom = lax.axis_index("atom")
    z, y = grid // NY, grid % NY
    x, c = atom // NC, atom % NC
    me = y * (NX * NC) + atom

    ys = [(y + d) % NY for d in range(NY)]
    xs = [(x + d) % NX for d in range(NX)]
    cs = [c, 1 - c]
    peers = []
    for dy in (2, 1, 3, 0):
        for dx in (2, 1, 3, 0):
            for dc in (1, 0):
                if dy or dx or dc:
                    pa = xs[dx] * NC + cs[dc]
                    peers.append((z * NY + ys[dy], pa, ys[dy] * (NX * NC) + pa))
    zpeers = []
    for dz in (4, 3, 5, 2, 6, 1, 7):
        pz = (z + dz) % NZ
        zpeers.append((pz * NY + y, atom, pz))
    ypeers = [(z * NY + ys[dy], atom, ys[dy]) for dy in (2, 1, 3)]

    barrier = pltpu.get_barrier_semaphore()
    for pg, pa, _ in peers + zpeers:
        pl.semaphore_signal(barrier, inc=1, device_id=(pg, pa), device_id_type=MESH)

    loads = [
        pltpu.make_async_copy(src, dst, load_sem.at[n])
        for n, (src, dst) in enumerate(
            [
                (w_hbm, w), (res_hbm, res), (basis_hbm, basis), (atom_hbm, atom_sm), (owner_hbm, owner_sm),
                (hist_hbm, hist_sm), (rho_hbm, rho), (tgt_hbm, tgt), (cpl_hbm, cpl),
            ]
        )
    ]
    for load in loads:
        load.start()

    sub = lax.broadcasted_iota(I32, (8, LANES), 0)
    lane = lax.broadcasted_iota(I32, (8, LANES), 1)
    low = lane < 64

    def to_peers(targets, src, dst, slot, ssem, rsem, per_peer=False):
        for pg, pa, pslot in targets:
            pltpu.make_async_remote_copy(
                src_ref=src.at[pslot] if per_peer else src,
                dst_ref=dst.at[slot],
                send_sem=ssem,
                recv_sem=rsem,
                device_id=(pg, pa),
                device_id_type=MESH,
            ).start()
        sends.append((dst, len(targets), ssem))

    def all_bytes(dst, count, sem):
        span = dst.at[pl.ds(0, count)]
        pltpu.make_async_copy(span, span, sem).wait()

    def arrived(targets, dst, rsem):
        all_bytes(dst, len(targets), rsem)

    def tree_sum(parts):
        parts = list(parts)
        while len(parts) > 1:
            parts = [a + b for a, b in zip(parts[::2], parts[1::2])] + ([parts[-1]] if len(parts) % 2 else [])
        return parts[0]

    def over_subs(v):
        v = v + pltpu.roll(v, 4, 0)
        v = v + pltpu.roll(v, 2, 0)
        return v + pltpu.roll(v, 1, 0)

    def tile_at(ref, at):
        return ref[:, pl.ds(pl.multiple_of(at * LANES, LANES), LANES)]

    def row_at(ref, at):
        return jnp.broadcast_to(ref[pl.ds(at, 1), :], (8, LANES))

    def basis_tile(kt, at):
        cols = pl.ds(pl.multiple_of(at * LANES, LANES), LANES)
        if kt < 3:
            return basis[pl.ds(kt * 8, 8), cols]
        return jnp.broadcast_to(basis[pl.ds(24, 1), cols], (8, LANES))

    def row_of(columns):
        total = jnp.zeros((8, LANES), F32)
        for d, column in enumerate(columns):
            total = jnp.where(lane == d * 8 + sub, column, total)
        return over_subs(total)

    sends = []

    def all_summed(row, it):
        irow_send[it] = row[0:1]
        to_peers(peers, irow_send.at[it], irow_recv.at[it], me, irow_ss.at[it], irow_rs.at[it])
        return row

    def plane_sum(it):
        arrived(peers, irow_recv.at[it], irow_rs.at[it])
        row = tree_sum([irow_send[it]] + [irow_recv[it, pslot] for _, _, pslot in peers])
        zrow_send[it] = row
        to_peers(zpeers, zrow_send.at[it], zrow_recv.at[it], z, zrow_ss.at[it], zrow_rs.at[it])

    def slice_sum(it):
        arrived(zpeers, zrow_recv.at[it], zrow_rs.at[it])
        row = tree_sum([zrow_send[it]] + [zrow_recv[it, pslot] for _, _, pslot in zpeers])
        return jnp.broadcast_to(row, (8, LANES))

    def mixing(total):
        def entry(i, j):
            d = (i - j) % 8
            at = d * 8 + i if d <= 4 else (8 - d) * 8 + j
            return jnp.broadcast_to(total[:, at : at + 1], (8, LANES))

        a = {(i, j): entry(i, j) for i in range(H) for j in range(i + 1)}
        ridge = RIDGE * tree_sum([a[i, i] for i in range(H)]) / H
        for i in range(H):
            a[i, i] = a[i, i] + ridge
        ones = jnp.ones((8, LANES), F32)
        rhs = [ones] * H
        inverse = []
        factor = {}
        for k in range(H):
            inv = 1.0 / a[k, k]
            inverse.append(inv)
            for i in range(k + 1, H):
                factor[i, k] = a[i, k] * inv
            for i in range(k + 1, H):
                for j in range(k + 1, i + 1):
                    a[i, j] = a[i, j] - factor[i, k] * a[j, k]
                rhs[i] = rhs[i] - factor[i, k] * rhs[k]
        solved = [None] * H
        for k in reversed(range(H)):
            value = rhs[k] * inverse[k]
            for i in range(k + 1, H):
                value = value - factor[i, k] * solved[i]
            solved[k] = value
        share = 1.0 / tree_sum(solved)
        coeffs = [value * share for value in solved]
        column = coeffs[0]
        for i in range(1, H):
            column = jnp.where(sub == i, coeffs[i], column)
        return coeffs, column

    def merge(first, second, bit, axis):
        clear = ((lane if axis == 1 else sub) & bit) == 0
        return jnp.where(clear, first, second) + pltpu.roll(jnp.where(clear, second, first), bit, axis)

    def merge_all(values, bit, axis):
        while len(values) > 1:
            values = [merge(p, q, bit, axis) for p, q in zip(values[::2], values[1::2])]
            bit *= 2
        return values[0]

    def weigh(group):
        for u in range(16):
            at = group * 16 + u
            wrow = row_at(w, at)
            for kt in range(4):
                weighted[u, kt] = basis_tile(kt, at) * wrow

    def batch_sums(group, kt, field):
        return merge_all([weighted[2 * u, kt] * field(2 * u) + weighted[2 * u + 1, kt] * field(2 * u + 1) for u in range(8)], 1, 1)

    def joined(n):
        total = merge_all([merged[g, n] for g in range(batches // 8)], 8, 1)
        return total + pltpu.roll(total, 64, 1)

    def history_moments():
        def step(group, carry):
            weigh(group)

            def cols(u):
                return pl.ds(pl.multiple_of((group * 16 + u) * LANES, LANES), LANES)

            for i in range(H):
                for kt in range(3):
                    merged[group, i * 3 + kt] = batch_sums(
                        group, kt, lambda u: jnp.broadcast_to(res[pl.ds(i, 1), cols(u)], (8, LANES))
                    )
            merged[group, 24] = batch_sums(group, 3, lambda u: res[:, cols(u)])
            return carry

        lax.fori_loop(0, batches // 8, step, 0)
        for n in range(25):
            hist_moms[n] = joined(n)

    def fresh_moments(hist_at):
        def step(group, carry):
            weigh(group)
            for kt in range(4):
                merged[group, kt] = batch_sums(group, kt, lambda u: row_at(fresh, group * 16 + u))
            return carry

        lax.fori_loop(0, batches // 8, step, 0)
        for kt in range(3):
            value = joined(kt)
            for i in range(H):
                hist_moms[i * 3 + kt] = jnp.where(hist_at == i, value, hist_moms[i * 3 + kt])
        hist_moms[24] = jnp.where(sub == hist_at, joined(3), hist_moms[24])

    def raw_moments(coeffs, column):
        return [tree_sum([coeffs[i] * hist_moms[i * 3 + kt] for i in range(H)]) for kt in range(3)] + [
            over_subs(column * hist_moms[24])
        ]

    def packed(t0, t1, t2, t3):
        first = jnp.where(low, t0, t1)
        second = jnp.where(
            sub < 4, jnp.where(low, t2, pltpu.roll(t2, 4, 0)), jnp.where((sub == 4) & low, t3, 0.0)
        )
        return first, second

    def unpacked(first, second):
        moved = pltpu.roll(second, 64, 1)
        t2 = jnp.where(sub < 4, second, pltpu.roll(moved, 4, 0))
        t3 = jnp.where(sub == 0, pltpu.roll(second, 4, 0), 0.0)
        return first, pltpu.roll(first, 64, 1), t2, t3

    def three(v):
        hi = v.astype(jnp.bfloat16)
        rest = v - hi.astype(F32)
        mid = rest.astype(jnp.bfloat16)
        lo = (rest - mid.astype(F32)).astype(jnp.bfloat16)
        return hi, mid, lo

    def pair_joined(a, b):
        return jnp.where(low, a, pltpu.roll(b, 64, 1)), jnp.where(low, pltpu.roll(a, 64, 1), b)

    def gather_parts(it):
        for pair in range(PLANE // 2):
            cols = pl.ds(pair * LANES, LANES)
            for half in range(2):
                rows = pl.ds(half * 8, 8)
                a, b = pair_joined(raw_recv[it, 2 * pair, rows, :], raw_recv[it, 2 * pair + 1, rows, :])
                both = jnp.concatenate([a, b], axis=0)
                for n, part in enumerate(three(both)):
                    xparts[pl.ds(n * 32 + half * 16, 16), cols] = part

    def matched(first_row, count):
        sums = lax.dot_general(
            xparts[...], match[pl.ds(first_row, count), :], (((1,), (1,)), ((), ())), preferred_element_type=F32
        )
        return sums[0:32] + sums[32:64] + sums[64:96]

    def owner_partial():
        sums = matched(NZ * 64, LANES)
        part_send[0:16] = sums[0:16]
        part_send[16:24] = jnp.where(sub < 4, sums[16:24], pltpu.roll(sums[24:32], 4, 0))
        part_send[24:32] = jnp.where(sub < 1, pltpu.roll(sums[16:24], 4, 0), 0.0)

    def peer_values(it):
        picked = matched(0, NZ * 64)
        for pair in range(NZ // 2):
            cols = slice(pair * LANES, (pair + 1) * LANES)
            for half in range(2):
                a, b = pair_joined(picked[half * 16 : half * 16 + 8, cols], picked[half * 16 + 8 : half * 16 + 16, cols])
                back_send[it, 2 * pair, half * 8 : half * 8 + 8, :] = a
                back_send[it, 2 * pair + 1, half * 8 : half * 8 + 8, :] = b

    def damped(kt, value):
        k = sub + kt * 8
        damp = jnp.where(k < 1, 1.0, jnp.where(k < 4, 1 / 2, jnp.where(k < 9, 1 / 3, jnp.where(k < 16, 1 / 4, 1 / 5))))
        return value * (damp * (scale * BETA))

    loads[0].wait()
    loads[1].wait()

    def products(step_at, accs):
        accs = list(accs)
        for u in range(4):
            at = step_at * 4 + u
            r = tile_at(res, at)
            wr = r * row_at(w, at)
            accs[0] = accs[0] + wr * r
            for d in range(1, 5):
                accs[d] = accs[d] + wr * pltpu.roll(r, d, 0)
        return tuple(accs)

    accs = lax.fori_loop(0, tiles // 4, products, (jnp.zeros((8, LANES), F32),) * 5)
    first_row = row_of([jnp.sum(acc, axis=1, keepdims=True) for acc in accs])

    for load in loads[3:6]:
        load.wait()

    def slot_step(b, row):
        return jnp.where(lane == b, owner_sm[atom_sm[b]], row)

    slots = lax.fori_loop(0, batches, slot_step, jnp.full((8, LANES), -1, I32), unroll=4)
    slot_send[...] = slots[0:1]
    slot_recv[me] = slots[0:1]
    zslot_recv[z] = slots[0:1]

    pl.semaphore_wait(barrier, len(peers) + len(zpeers))
    all_summed(first_row, 0)
    to_peers(peers, slot_send, slot_recv, me, slot_ss, slot_rs)
    to_peers(zpeers, slot_send, zslot_recv, z, zslot_ss, zslot_rs)
    loads[2].wait()
    history_moments()
    for load in loads[6:]:
        load.wait()

    plane_sum(0)

    arrived(peers, slot_recv, slot_rs)
    arrived(zpeers, zslot_recv, zslot_rs)
    first_slot = atom * 512 + y * LANES
    sources = []
    for pair in range(PLANE // 2):
        left = jnp.broadcast_to(slot_recv[2 * pair], (8, LANES))
        right = jnp.broadcast_to(slot_recv[2 * pair + 1], (8, LANES))
        sources.append(jnp.where(low, left, pltpu.roll(right, 64, 1)))

    def match_rows(at, wanted):
        for pair in range(PLANE // 2):
            halves = [jnp.where(sources[pair] == one, 1.0, 0.0) for one in wanted]
            match[pl.ds(at, 16), pl.ds(pair * LANES, LANES)] = jnp.concatenate(halves, axis=0).astype(jnp.bfloat16)

    def target_step(step_at, carry):
        row = jnp.broadcast_to(zslot_recv[step_at // 4], (8, LANES)).astype(F32)
        wanted = []
        for h in range(2):
            hit = lane == sub + ((step_at % 4) * 16 + h * 8)
            column = jnp.sum(jnp.where(hit, row, 0.0), axis=1, keepdims=True)
            wanted.append(jnp.broadcast_to(column, (8, LANES)).astype(I32))
        match_rows(pl.multiple_of(step_at * 16, 16), wanted)
        return carry

    lax.fori_loop(0, NZ * 4, target_step, 0)
    for st in range(LANES // 16):
        match_rows(NZ * 64 + st * 16, [sub + (first_slot + st * 16 + h * 8) for h in range(2)])

    total = slice_sum(0)
    for it in range(ITERS):
        last = it == ITERS - 1
        coeffs, column = mixing(total)
        for rows, value in zip((pl.ds(0, 8), pl.ds(8, 8)), packed(*raw_moments(coeffs, column))):
            raw_send[it, rows, :] = value
            raw_recv[it, me, rows, :] = value
        to_peers(peers, raw_send.at[it], raw_recv.at[it], me, raw_ss.at[it], raw_rs.at[it])
        arrived(peers, raw_recv.at[it], raw_rs.at[it])
        gather_parts(it)
        if last:
            owner_partial()
            to_peers(zpeers, part_send, part_recv, z, part_ss, part_rs)
        peer_values(it)
        to_peers(zpeers, back_send.at[it], back_recv.at[it], z, back_ss.at[it], back_rs.at[it], per_peer=True)
        if last:
            arrived(zpeers, part_recv, part_rs)
            block = tree_sum([part_send[...]] + [part_recv[pslot] for _, _, pslot in zpeers]) * scale
            blk_send[...] = block
            to_peers(ypeers, blk_send, blk_recv, y, blk_ss, blk_rs)
            blk_recv[y] = block
        arrived(zpeers, back_recv.at[it], back_rs.at[it])
        mine = tree_sum([back_send[it, z]] + [back_recv[it, pslot] for _, _, pslot in zpeers])
        at_batch = tuple(damped(kt, t) for kt, t in enumerate(unpacked(mine[0:8], mine[8:16])))
        hist_at = hist_sm[it]

        def density_step(group, carry):
            at_tiles, acc = carry
            rows = pl.ds(pl.multiple_of(group * 8, 8), 8)
            parts = []
            for u in range(4):
                spread = [jnp.broadcast_to(t[:, u : u + 1], (8, LANES)) for t in at_tiles]
                for half in range(2):
                    at = group * 8 + u * 2 + half
                    v = column * (tile_at(rho, at) + BETA * tile_at(res, at))
                    parts.append(v - tree_sum([basis_tile(kt, at) * spread[kt] for kt in range(4)]))
            dens = merge_all(parts, 1, 0)
            if last:
                dens_out[rows, :] = dens
            else:
                new = tgt[rows, :] + cpl[rows, :] * jnp.tanh(dens) - dens
                fresh[rows, :] = new
                weighed = new * w[rows, :]
                for u in range(8):
                    cols = pl.ds(pl.multiple_of((group * 8 + u) * LANES, LANES), LANES)
                    r = jnp.where(sub == hist_at, jnp.broadcast_to(new[u : u + 1], (8, LANES)), res[:, cols])
                    res[:, cols] = r
                    rho[:, cols] = jnp.where(sub == hist_at, jnp.broadcast_to(dens[u : u + 1], (8, LANES)), rho[:, cols])
                    acc = acc + r * jnp.broadcast_to(weighed[u : u + 1], (8, LANES))
            return tuple(pltpu.roll(t, LANES - 4, 1) for t in at_tiles), acc

        _, acc = lax.fori_loop(0, batches // 4, density_step, (at_batch, jnp.zeros((8, LANES), F32)), unroll=4)
        if not last:
            mine_new = jnp.broadcast_to(jnp.sum(acc, axis=1, keepdims=True), (8, LANES))
            columns = [
                jnp.where(sub == hist_at, pltpu.roll(mine_new, d, 0) if d else mine_new, mine_new) for d in range(5)
            ]
            all_summed(row_of(columns), it + 1)
            fresh_moments(hist_at)
            plane_sum(it + 1)
            row_i = lane % 8
            row_j = (row_i - lane // 8 + 8) % 8
            total = jnp.where((row_i == hist_at) | (row_j == hist_at), slice_sum(it + 1), total)

    arrived(ypeers, blk_recv, blk_rs)
    for q in range(NY):
        mom_out[:, q * LANES : (q + 1) * LANES] = blk_recv[q, 0:LM]
    for dst, count, ssem in sends:
        all_bytes(dst, count, ssem)


def local(weights, target, coupling, multipole_basis, rho_hist, res_hist, batch_atom, owner_slot, slot_index):
    points = weights.shape[0]
    batches = batch_atom.shape[0]
    tiles = points // LANES
    slots = owner_slot.shape[0]
    owned = slots // lax.axis_size("atom")
    scale = 1.0 / math.sqrt(points * lax.axis_size("grid") // owned)
    square = lambda v: v.reshape(tiles, LANES)
    vm, sm, dma = pltpu.VMEM, pltpu.SMEM, pltpu.SemaphoreType.DMA
    anywhere = pl.BlockSpec(memory_space=pl.ANY)
    vmem = pl.BlockSpec(memory_space=pltpu.VMEM)
    density, moments = pl.pallas_call(
        functools.partial(kernel, tiles, batches, scale),
        out_shape=(pltpu.VMEM((tiles, LANES), F32), pltpu.VMEM((LM, owned), F32)),
        in_specs=[anywhere] * 9,
        out_specs=(vmem, vmem),
        scratch_shapes=[
            vm((tiles, LANES), F32), vm((tiles, LANES), F32), vm((tiles, LANES), F32),
            vm((LM, points), F32), vm((H, points), F32), vm((H, points), F32),
            vm((tiles, LANES), F32), vm((16, 4, 8, LANES), F32), vm((batches // 8, 25, 8, LANES), F32), vm((25, 8, LANES), F32),
            sm((batches,), I32), sm((slots,), I32), sm((ITERS,), I32),
            vm((1, LANES), I32), vm((PLANE, 1, LANES), I32), vm((NZ, 1, LANES), I32),
            vm((ITERS, 1, LANES), F32), vm((ITERS, PLANE, 1, LANES), F32),
            vm((ITERS, 1, LANES), F32), vm((ITERS, NZ, 1, LANES), F32),
            vm((ITERS, 16, LANES), F32), vm((ITERS, PLANE, 16, LANES), F32),
            vm((32, LANES), F32), vm((NZ, 32, LANES), F32),
            vm((ITERS, NZ, 16, LANES), F32), vm((ITERS, NZ, 16, LANES), F32),
            vm((32, LANES), F32), vm((NY, 32, LANES), F32),
            vm((NZ * 64 + LANES, PLANE * 64), jnp.bfloat16), vm((96, PLANE * 64), jnp.bfloat16),
            dma((9,)),
            dma, dma, dma, dma, dma((ITERS,)), dma((ITERS,)), dma((ITERS,)), dma((ITERS,)),
            dma((ITERS,)), dma((ITERS,)), dma, dma, dma((ITERS,)), dma((ITERS,)), dma, dma,
        ],
        compiler_params=pltpu.CompilerParams(collective_id=0, has_side_effects=True),
    )(
        square(weights), square(target), square(coupling), multipole_basis, rho_hist, res_hist,
        batch_atom, owner_slot, slot_index,
    )
    return density.reshape(points), moments


def solution(mesh):
    both = ("grid", "atom")
    placed = (P(both), P(both), P(both), P(None, both), P(None, both), P(None, both), P(both), P(), P())
    return jax.shard_map(
        local, mesh=mesh, in_specs=placed, out_specs=(P(both), P(None, "atom")), check_vma=False
    )
```

```python
import functools
import math

import jax
import jax.numpy as jnp
import numpy as np
from jax import lax
from jax.experimental import pallas as pl
from jax.experimental.pallas import tpu as pltpu
from jax.sharding import PartitionSpec as P

H = 8
LM = 25
ITERS = 2
BETA = 0.5
RIDGE = 0.1
LANES = 128
NZ, NY, NX, NC = 8, 4, 4, 2
PLANE = NY * NX * NC
MESH = pl.DeviceIdType.MESH
F32 = jnp.float32
I32 = jnp.int32


def kernel(
    tiles, batches, scale,
    w_hbm, tgt_hbm, cpl_hbm, basis_hbm, rho_hbm, res_hbm, atom_hbm, owner_hbm, hist_hbm,
    dens_out, mom_out,
    w, tgt, cpl, basis, rho, res, fresh, weighted, merged, hist_moms,
    atom_sm, owner_sm, hist_sm,
    slot_send, slot_recv, zslot_recv, irow_send, irow_recv, zrow_send, zrow_recv,
    raw_send, raw_recv, part_send, part_recv, back_send, back_recv, blk_send, blk_recv,
    keep_send, kept, match, xparts,
    load_sem,
    slot_ss, slot_rs, zslot_ss, zslot_rs, irow_ss, irow_rs, zrow_ss, zrow_rs,
    raw_ss, raw_rs, part_ss, part_rs, back_ss, back_rs, blk_ss, blk_rs, keep_ss, keep_rs, pair_ss, pair_rs,
):
    grid = lax.axis_index("grid")
    atom = lax.axis_index("atom")
    z, y = grid // NY, grid % NY
    x, c = atom // NC, atom % NC
    me = y * (NX * NC) + atom

    ys = [(y + d) % NY for d in range(NY)]
    xs = [(x + d) % NX for d in range(NX)]
    cs = [c, 1 - c]
    peers = []
    for dy in (2, 1, 3, 0):
        for dx in (2, 1, 3, 0):
            for dc in (1, 0):
                if dy or dx or dc:
                    pa = xs[dx] * NC + cs[dc]
                    peers.append((z * NY + ys[dy], pa, ys[dy] * (NX * NC) + pa))
    zpeers = []
    for dz in (4, 3, 5, 2, 6, 1, 7):
        pz = (z + dz) % NZ
        zpeers.append((pz * NY + y, atom, pz))
    spot = y * NX + x
    alike = [(pg, xs[dx] * NC + c, 0) for dy in (2, 1, 3, 0) for dx in (2, 1, 3, 0) if dy or dx for pg in [z * NY + ys[dy]]]
    other = [(grid, x * NC + cs[1], 0)]
    ypeers = [(z * NY + ys[dy], atom, ys[dy]) for dy in (2, 1, 3)]

    barrier = pltpu.get_barrier_semaphore()
    for pg, pa, _ in peers + zpeers:
        pl.semaphore_signal(barrier, inc=1, device_id=(pg, pa), device_id_type=MESH)

    loads = [
        pltpu.make_async_copy(src, dst, load_sem.at[n])
        for n, (src, dst) in enumerate(
            [
                (w_hbm, w), (res_hbm, res), (basis_hbm, basis), (atom_hbm, atom_sm), (owner_hbm, owner_sm),
                (hist_hbm, hist_sm), (rho_hbm, rho), (tgt_hbm, tgt), (cpl_hbm, cpl),
            ]
        )
    ]
    for load in loads:
        load.start()

    sub = lax.broadcasted_iota(I32, (8, LANES), 0)
    lane = lax.broadcasted_iota(I32, (8, LANES), 1)
    low = lane < 64

    def to_peers(targets, src, dst, slot, ssem, rsem, per_peer=False):
        for pg, pa, pslot in targets:
            pltpu.make_async_remote_copy(
                src_ref=src.at[pslot] if per_peer else src,
                dst_ref=dst.at[slot],
                send_sem=ssem,
                recv_sem=rsem,
                device_id=(pg, pa),
                device_id_type=MESH,
            ).start()
        sends.append((dst, len(targets), ssem))

    def all_bytes(dst, count, sem):
        span = dst.at[pl.ds(0, count)]
        pltpu.make_async_copy(span, span, sem).wait()

    def arrived(targets, dst, rsem):
        all_bytes(dst, len(targets), rsem)

    def tree_sum(parts):
        parts = list(parts)
        while len(parts) > 1:
            parts = [a + b for a, b in zip(parts[::2], parts[1::2])] + ([parts[-1]] if len(parts) % 2 else [])
        return parts[0]

    def over_subs(v):
        v = v + pltpu.roll(v, 4, 0)
        v = v + pltpu.roll(v, 2, 0)
        return v + pltpu.roll(v, 1, 0)

    def tile_at(ref, at):
        return ref[:, pl.ds(pl.multiple_of(at * LANES, LANES), LANES)]

    def row_at(ref, at):
        return jnp.broadcast_to(ref[pl.ds(at, 1), :], (8, LANES))

    def basis_tile(kt, at):
        cols = pl.ds(pl.multiple_of(at * LANES, LANES), LANES)
        if kt < 3:
            return basis[pl.ds(kt * 8, 8), cols]
        return jnp.broadcast_to(basis[pl.ds(24, 1), cols], (8, LANES))

    def row_of(columns):
        total = jnp.zeros((8, LANES), F32)
        for d, column in enumerate(columns):
            total = jnp.where(lane == d * 8 + sub, column, total)
        return over_subs(total)

    sends = []

    def all_summed(row, it):
        irow_send[it] = row[0:1]
        to_peers(peers, irow_send.at[it], irow_recv.at[it], me, irow_ss.at[it], irow_rs.at[it])
        return row

    def plane_sum(it):
        arrived(peers, irow_recv.at[it], irow_rs.at[it])
        row = tree_sum([irow_send[it]] + [irow_recv[it, pslot] for _, _, pslot in peers])
        zrow_send[it] = row
        to_peers(zpeers, zrow_send.at[it], zrow_recv.at[it], z, zrow_ss.at[it], zrow_rs.at[it])

    def slice_sum(it):
        arrived(zpeers, zrow_recv.at[it], zrow_rs.at[it])
        row = tree_sum([zrow_send[it]] + [zrow_recv[it, pslot] for _, _, pslot in zpeers])
        return jnp.broadcast_to(row, (8, LANES))

    def mixing(total):
        def entry(i, j):
            d = (i - j) % 8
            at = d * 8 + i if d <= 4 else (8 - d) * 8 + j
            return jnp.broadcast_to(total[:, at : at + 1], (8, LANES))

        a = {(i, j): entry(i, j) for i in range(H) for j in range(i + 1)}
        ridge = RIDGE * tree_sum([a[i, i] for i in range(H)]) / H
        for i in range(H):
            a[i, i] = a[i, i] + ridge
        ones = jnp.ones((8, LANES), F32)
        rhs = [ones] * H
        inverse = []
        factor = {}
        for k in range(H):
            inv = 1.0 / a[k, k]
            inverse.append(inv)
            for i in range(k + 1, H):
                factor[i, k] = a[i, k] * inv
            for i in range(k + 1, H):
                for j in range(k + 1, i + 1):
                    a[i, j] = a[i, j] - factor[i, k] * a[j, k]
                rhs[i] = rhs[i] - factor[i, k] * rhs[k]
        solved = [None] * H
        for k in reversed(range(H)):
            value = rhs[k] * inverse[k]
            for i in range(k + 1, H):
                value = value - factor[i, k] * solved[i]
            solved[k] = value
        share = 1.0 / tree_sum(solved)
        coeffs = [value * share for value in solved]
        column = coeffs[0]
        for i in range(1, H):
            column = jnp.where(sub == i, coeffs[i], column)
        return coeffs, column

    def merge(first, second, bit, axis):
        clear = ((lane if axis == 1 else sub) & bit) == 0
        return jnp.where(clear, first, second) + pltpu.roll(jnp.where(clear, second, first), bit, axis)

    def merge_all(values, bit, axis):
        while len(values) > 1:
            values = [merge(p, q, bit, axis) for p, q in zip(values[::2], values[1::2])]
            bit *= 2
        return values[0]

    def weigh(group):
        for u in range(16):
            at = group * 16 + u
            wrow = row_at(w, at)
            for kt in range(4):
                weighted[u, kt] = basis_tile(kt, at) * wrow

    def batch_sums(group, kt, field):
        return merge_all([weighted[2 * u, kt] * field(2 * u) + weighted[2 * u + 1, kt] * field(2 * u + 1) for u in range(8)], 1, 1)

    def joined(n):
        total = merge_all([merged[g, n] for g in range(batches // 8)], 8, 1)
        return total + pltpu.roll(total, 64, 1)

    def history_moments():
        def step(group, carry):
            weigh(group)

            def cols(u):
                return pl.ds(pl.multiple_of((group * 16 + u) * LANES, LANES), LANES)

            for i in range(H):
                for kt in range(3):
                    merged[group, i * 3 + kt] = batch_sums(
                        group, kt, lambda u: jnp.broadcast_to(res[pl.ds(i, 1), cols(u)], (8, LANES))
                    )
            merged[group, 24] = batch_sums(group, 3, lambda u: res[:, cols(u)])
            return carry

        lax.fori_loop(0, batches // 8, step, 0)
        for n in range(25):
            hist_moms[n] = joined(n)

    def fresh_moments():
        def step(group, carry):
            weigh(group)
            for kt in range(4):
                merged[group, kt] = batch_sums(group, kt, lambda u: row_at(fresh, group * 16 + u))
            return carry

        lax.fori_loop(0, batches // 8, step, 0)
        return [joined(kt) for kt in range(4)]

    def raw_moments(coeffs, column):
        return [tree_sum([coeffs[i] * hist_moms[i * 3 + kt] for i in range(H)]) for kt in range(3)] + [
            over_subs(column * hist_moms[24])
        ]

    def packed(t0, t1, t2, t3):
        first = jnp.where(low, t0, t1)
        second = jnp.where(
            sub < 4, jnp.where(low, t2, pltpu.roll(t2, 4, 0)), jnp.where((sub == 4) & low, t3, 0.0)
        )
        return first, second

    def unpacked(first, second):
        moved = pltpu.roll(second, 64, 1)
        t2 = jnp.where(sub < 4, second, pltpu.roll(moved, 4, 0))
        t3 = jnp.where(sub == 0, pltpu.roll(second, 4, 0), 0.0)
        return first, pltpu.roll(first, 64, 1), t2, t3

    def three(v):
        hi = v.astype(jnp.bfloat16)
        rest = v - hi.astype(F32)
        mid = rest.astype(jnp.bfloat16)
        lo = (rest - mid.astype(F32)).astype(jnp.bfloat16)
        return hi, mid, lo

    def pair_joined(a, b):
        return jnp.where(low, a, pltpu.roll(b, 64, 1)), jnp.where(low, pltpu.roll(a, 64, 1), b)

    def keep_moments(hist_at):
        def stays(j, kt):
            return jnp.where(hist_at > j, hist_moms[j * 3 + kt], hist_moms[(j + 1) * 3 + kt])

        tiles_of = [jnp.where(low, stays(j, 0), stays(j, 1)) for j in range(7)]
        tiles_of += [jnp.where(low, stays(2 * m, 2), stays(2 * m + 1, 2)) for m in range(3)]
        tiles_of += [jnp.where(low, stays(6, 2), hist_moms[24])]
        for n, value in enumerate(tiles_of):
            keep_send[n * 8 : n * 8 + 8, :] = value
            kept[c, spot, n * 8 : n * 8 + 8, :] = value

    def combined(coeffs, column, hist_at):
        own = [jnp.where(hist_at > j, coeffs[j], coeffs[j + 1]) for j in range(7)]
        fresh_share = tree_sum([jnp.where(hist_at == i, coeffs[i], 0.0) for i in range(H)])
        doubles = [jnp.where(low, own[2 * m], own[2 * m + 1]) for m in range(3)]
        tail = jnp.where(low, own[6], jnp.where(sub == hist_at, 0.0, column))

        def of(core, at, new_first, new_second):
            t = [kept[core, at, n * 8 : n * 8 + 8, :] for n in range(11)]
            first = tree_sum([own[j] * t[j] for j in range(7)] + [fresh_share * new_first])
            u = tree_sum([doubles[m] * t[7 + m] for m in range(3)])
            v = tail * t[10]
            turned = pltpu.roll(v, 64, 1)
            t2 = u + pltpu.roll(u, 64, 1) + jnp.where(low, v, turned)
            second = jnp.where(
                sub < 4,
                jnp.where(low, t2, pltpu.roll(t2, 4, 0)),
                jnp.where((sub == 4) & low, over_subs(turned), 0.0),
            )
            return first, second + fresh_share * new_second

        return of

    def gather_parts(it, combine=None):
        for pair in range(PLANE // 2):
            cols = pl.ds(pair * LANES, LANES)
            raws = [[raw_recv[it, 2 * pair + core, pl.ds(half * 8, 8), :] for half in range(2)] for core in range(2)]
            if combine:
                raws = [combine(core, pair, *raws[core]) for core in range(2)]
            for half in range(2):
                a, b = pair_joined(raws[0][half], raws[1][half])
                both = jnp.concatenate([a, b], axis=0)
                for n, part in enumerate(three(both)):
                    xparts[pl.ds(n * 32 + half * 16, 16), cols] = part

    def matched(first_row, count):
        sums = lax.dot_general(
            xparts[...], match[pl.ds(first_row, count), :], (((1,), (1,)), ((), ())), preferred_element_type=F32
        )
        return sums[0:32] + sums[32:64] + sums[64:96]

    def owner_partial():
        sums = matched(NZ * 64, LANES)
        part_send[0:16] = sums[0:16]
        part_send[16:24] = jnp.where(sub < 4, sums[16:24], pltpu.roll(sums[24:32], 4, 0))
        part_send[24:32] = jnp.where(sub < 1, pltpu.roll(sums[16:24], 4, 0), 0.0)

    def peer_values(it):
        picked = matched(0, NZ * 64)
        for pair in range(NZ // 2):
            cols = slice(pair * LANES, (pair + 1) * LANES)
            for half in range(2):
                a, b = pair_joined(picked[half * 16 : half * 16 + 8, cols], picked[half * 16 + 8 : half * 16 + 16, cols])
                back_send[it, 2 * pair, half * 8 : half * 8 + 8, :] = a
                back_send[it, 2 * pair + 1, half * 8 : half * 8 + 8, :] = b

    def damped(kt, value):
        k = sub + kt * 8
        damp = jnp.where(k < 1, 1.0, jnp.where(k < 4, 1 / 2, jnp.where(k < 9, 1 / 3, jnp.where(k < 16, 1 / 4, 1 / 5))))
        return value * (damp * (scale * BETA))

    def send_raw(it, values):
        for rows, value in zip((pl.ds(0, 8), pl.ds(8, 8)), packed(*values)):
            raw_send[it, rows, :] = value
            raw_recv[it, me, rows, :] = value
        to_peers(peers, raw_send.at[it], raw_recv.at[it], me, raw_ss.at[it], raw_rs.at[it])

    loads[0].wait()
    loads[1].wait()

    def products(step_at, accs):
        accs = list(accs)
        for u in range(4):
            at = step_at * 4 + u
            r = tile_at(res, at)
            wr = r * row_at(w, at)
            accs[0] = accs[0] + wr * r
            for d in range(1, 5):
                accs[d] = accs[d] + wr * pltpu.roll(r, d, 0)
        return tuple(accs)

    accs = lax.fori_loop(0, tiles // 4, products, (jnp.zeros((8, LANES), F32),) * 5)
    first_row = row_of([jnp.sum(acc, axis=1, keepdims=True) for acc in accs])

    pl.semaphore_wait(barrier, len(peers) + len(zpeers))
    all_summed(first_row, 0)
    for load in loads[3:6]:
        load.wait()

    def slot_step(b, row):
        return jnp.where(lane == b, owner_sm[atom_sm[b]], row)

    slots = lax.fori_loop(0, batches, slot_step, jnp.full((8, LANES), -1, I32), unroll=4)
    slot_send[...] = slots[0:1]
    slot_recv[me] = slots[0:1]
    zslot_recv[z] = slots[0:1]
    to_peers(peers, slot_send, slot_recv, me, slot_ss, slot_rs)
    to_peers(zpeers, slot_send, zslot_recv, z, zslot_ss, zslot_rs)
    loads[2].wait()
    history_moments()
    for load in loads[6:]:
        load.wait()

    plane_sum(0)

    arrived(peers, slot_recv, slot_rs)
    arrived(zpeers, zslot_recv, zslot_rs)
    first_slot = atom * 512 + y * LANES
    sources = []
    for pair in range(PLANE // 2):
        left = jnp.broadcast_to(slot_recv[2 * pair], (8, LANES))
        right = jnp.broadcast_to(slot_recv[2 * pair + 1], (8, LANES))
        sources.append(jnp.where(low, left, pltpu.roll(right, 64, 1)))

    def match_rows(at, wanted):
        for pair in range(PLANE // 2):
            halves = [jnp.where(sources[pair] == one, 1.0, 0.0) for one in wanted]
            match[pl.ds(at, 16), pl.ds(pair * LANES, LANES)] = jnp.concatenate(halves, axis=0).astype(jnp.bfloat16)

    def target_step(step_at, carry):
        row = jnp.broadcast_to(zslot_recv[step_at // 4], (8, LANES)).astype(F32)
        wanted = []
        for h in range(2):
            hit = lane == sub + ((step_at % 4) * 16 + h * 8)
            column = jnp.sum(jnp.where(hit, row, 0.0), axis=1, keepdims=True)
            wanted.append(jnp.broadcast_to(column, (8, LANES)).astype(I32))
        match_rows(pl.multiple_of(step_at * 16, 16), wanted)
        return carry

    lax.fori_loop(0, NZ * 4, target_step, 0)
    for st in range(LANES // 16):
        match_rows(NZ * 64 + st * 16, [sub + (first_slot + st * 16 + h * 8) for h in range(2)])

    total = slice_sum(0)
    for it in range(ITERS):
        last = it == ITERS - 1
        coeffs, column = mixing(total)
        if last:
            gather_parts(it, combined(coeffs, column, hist_sm[0]))
        else:
            send_raw(it, raw_moments(coeffs, column))
            keep_moments(hist_sm[it])
            arrived(peers, raw_recv.at[it], raw_rs.at[it])
            to_peers(alike, keep_send, kept.at[c], spot, keep_ss, keep_rs)
            gather_parts(it)
        if last:
            owner_partial()
            to_peers(zpeers, part_send, part_recv, z, part_ss, part_rs)
        peer_values(it)
        to_peers(zpeers, back_send.at[it], back_recv.at[it], z, back_ss.at[it], back_rs.at[it], per_peer=True)
        if last:
            arrived(zpeers, part_recv, part_rs)
            block = tree_sum([part_send[...]] + [part_recv[pslot] for _, _, pslot in zpeers]) * scale
            blk_send[...] = block
            to_peers(ypeers, blk_send, blk_recv, y, blk_ss, blk_rs)
            blk_recv[y] = block
        arrived(zpeers, back_recv.at[it], back_rs.at[it])
        mine = tree_sum([back_send[it, z]] + [back_recv[it, pslot] for _, _, pslot in zpeers])
        at_batch = tuple(damped(kt, t) for kt, t in enumerate(unpacked(mine[0:8], mine[8:16])))
        hist_at = hist_sm[it]

        def density_step(group, carry):
            at_tiles, acc = carry
            rows = pl.ds(pl.multiple_of(group * 8, 8), 8)
            parts = []
            for u in range(4):
                spread = [jnp.broadcast_to(t[:, u : u + 1], (8, LANES)) for t in at_tiles]
                for half in range(2):
                    at = group * 8 + u * 2 + half
                    v = column * (tile_at(rho, at) + BETA * tile_at(res, at))
                    parts.append(v - tree_sum([basis_tile(kt, at) * spread[kt] for kt in range(4)]))
            dens = merge_all(parts, 1, 0)
            if last:
                dens_out[rows, :] = dens
            else:
                new = tgt[rows, :] + cpl[rows, :] * jnp.tanh(dens) - dens
                fresh[rows, :] = new
                weighed = new * w[rows, :]
                for u in range(8):
                    cols = pl.ds(pl.multiple_of((group * 8 + u) * LANES, LANES), LANES)
                    r = jnp.where(sub == hist_at, jnp.broadcast_to(new[u : u + 1], (8, LANES)), res[:, cols])
                    res[:, cols] = r
                    rho[:, cols] = jnp.where(sub == hist_at, jnp.broadcast_to(dens[u : u + 1], (8, LANES)), rho[:, cols])
                    acc = acc + r * jnp.broadcast_to(weighed[u : u + 1], (8, LANES))
            return tuple(pltpu.roll(t, LANES - 4, 1) for t in at_tiles), acc

        _, acc = lax.fori_loop(0, batches // 4, density_step, (at_batch, jnp.zeros((8, LANES), F32)), unroll=4)
        if not last:
            mine_new = jnp.broadcast_to(jnp.sum(acc, axis=1, keepdims=True), (8, LANES))
            columns = [
                jnp.where(sub == hist_at, pltpu.roll(mine_new, d, 0) if d else mine_new, mine_new) for d in range(5)
            ]
            all_summed(row_of(columns), it + 1)
            send_raw(it + 1, fresh_moments())
            arrived(alike, kept.at[0], keep_rs)
            to_peers(other, kept.at[c], kept, c, pair_ss, pair_rs)
            plane_sum(it + 1)
            arrived(peers, raw_recv.at[it + 1], raw_rs.at[it + 1])
            arrived(other, kept, pair_rs)
            row_i = lane % 8
            row_j = (row_i - lane // 8 + 8) % 8
            total = jnp.where((row_i == hist_at) | (row_j == hist_at), slice_sum(it + 1), total)

    arrived(ypeers, blk_recv, blk_rs)
    for q in range(NY):
        mom_out[:, q * LANES : (q + 1) * LANES] = blk_recv[q, 0:LM]
    for dst, count, ssem in sends:
        all_bytes(dst, count, ssem)


def local(weights, target, coupling, multipole_basis, rho_hist, res_hist, batch_atom, owner_slot, slot_index):
    points = weights.shape[0]
    batches = batch_atom.shape[0]
    tiles = points // LANES
    slots = owner_slot.shape[0]
    owned = slots // lax.axis_size("atom")
    scale = 1.0 / math.sqrt(points * lax.axis_size("grid") // owned)
    square = lambda v: v.reshape(tiles, LANES)
    vm, sm, dma = pltpu.VMEM, pltpu.SMEM, pltpu.SemaphoreType.DMA
    anywhere = pl.BlockSpec(memory_space=pl.ANY)
    vmem = pl.BlockSpec(memory_space=pltpu.VMEM)
    density, moments = pl.pallas_call(
        functools.partial(kernel, tiles, batches, scale),
        out_shape=(pltpu.VMEM((tiles, LANES), F32), pltpu.VMEM((LM, owned), F32)),
        in_specs=[anywhere] * 9,
        out_specs=(vmem, vmem),
        scratch_shapes=[
            vm((tiles, LANES), F32), vm((tiles, LANES), F32), vm((tiles, LANES), F32),
            vm((LM, points), F32), vm((H, points), F32), vm((H, points), F32),
            vm((tiles, LANES), F32), vm((16, 4, 8, LANES), F32), vm((batches // 8, 25, 8, LANES), F32), vm((25, 8, LANES), F32),
            sm((batches,), I32), sm((slots,), I32), sm((ITERS,), I32),
            vm((1, LANES), I32), vm((PLANE, 1, LANES), I32), vm((NZ, 1, LANES), I32),
            vm((ITERS, 1, LANES), F32), vm((ITERS, PLANE, 1, LANES), F32),
            vm((ITERS, 1, LANES), F32), vm((ITERS, NZ, 1, LANES), F32),
            vm((ITERS, 16, LANES), F32), vm((ITERS, PLANE, 16, LANES), F32),
            vm((32, LANES), F32), vm((NZ, 32, LANES), F32),
            vm((ITERS, NZ, 16, LANES), F32), vm((ITERS, NZ, 16, LANES), F32),
            vm((32, LANES), F32), vm((NY, 32, LANES), F32),
            vm((88, LANES), F32), vm((NC, NY * NX, 88, LANES), F32),
            vm((NZ * 64 + LANES, PLANE * 64), jnp.bfloat16), vm((96, PLANE * 64), jnp.bfloat16),
            dma((9,)),
            dma, dma, dma, dma, dma((ITERS,)), dma((ITERS,)), dma((ITERS,)), dma((ITERS,)),
            dma((ITERS,)), dma((ITERS,)), dma, dma, dma((ITERS,)), dma((ITERS,)), dma, dma, dma, dma, dma, dma,
        ],
        compiler_params=pltpu.CompilerParams(collective_id=0, has_side_effects=True),
    )(
        square(weights), square(target), square(coupling), multipole_basis, rho_hist, res_hist,
        batch_atom, owner_slot, slot_index,
    )
    return density.reshape(points), moments


def solution(mesh):
    both = ("grid", "atom")
    placed = (P(both), P(both), P(both), P(None, both), P(None, both), P(None, both), P(both), P(), P())
    return jax.shard_map(
        local, mesh=mesh, in_specs=placed, out_specs=(P(both), P(None, "atom")), check_vma=False
    )
```

```python
import functools
import math

import jax
import jax.numpy as jnp
import numpy as np
from jax import lax
from jax.experimental import pallas as pl
from jax.experimental.pallas import tpu as pltpu
from jax.sharding import PartitionSpec as P

H = 8
LM = 25
ITERS = 2
BETA = 0.5
RIDGE = 0.1
LANES = 128
NZ, NY, NX, NC = 8, 4, 4, 2
PLANE = NY * NX * NC
MESH = pl.DeviceIdType.MESH
F32 = jnp.float32
I32 = jnp.int32


def kernel(
    tiles, batches, scale,
    w_hbm, tgt_hbm, cpl_hbm, basis_hbm, rho_hbm, res_hbm, atom_hbm, owner_hbm, hist_hbm,
    dens_out, mom_out,
    w, tgt, cpl, basis, rho, res, fresh, weighted, merged, hist_moms,
    atom_sm, owner_sm, hist_sm,
    slot_send, slot_recv, zslot_recv, irow_send, irow_recv, zrow_send, zrow_recv,
    raw_send, raw_recv, part_send, part_recv, back_send, back_recv, blk_send, blk_recv,
    keep_send, kept, match, xparts, xkept, own_kept, own_fresh,
    load_sem,
    slot_ss, slot_rs, zslot_ss, zslot_rs, irow_ss, irow_rs, zrow_ss, zrow_rs,
    raw_ss, raw_rs, part_ss, part_rs, back_ss, back_rs, blk_ss, blk_rs, keep_ss, keep_rs, pair_ss, pair_rs,
):
    grid = lax.axis_index("grid")
    atom = lax.axis_index("atom")
    z, y = grid // NY, grid % NY
    x, c = atom // NC, atom % NC
    me = y * (NX * NC) + atom

    ys = [(y + d) % NY for d in range(NY)]
    xs = [(x + d) % NX for d in range(NX)]
    cs = [c, 1 - c]
    peers = []
    for dy in (2, 1, 3, 0):
        for dx in (2, 1, 3, 0):
            for dc in (1, 0):
                if dy or dx or dc:
                    pa = xs[dx] * NC + cs[dc]
                    peers.append((z * NY + ys[dy], pa, ys[dy] * (NX * NC) + pa))
    zpeers = []
    zorder = [(z + dz) % NZ for dz in (4, 3, 5, 2, 6, 1, 7, 0)]
    for pz in zorder[:-1]:
        zpeers.append((pz * NY + y, atom, pz))
    spot = y * NX + x
    alike = [(pg, xs[dx] * NC + c, 0) for dy in (2, 1, 3, 0) for dx in (2, 1, 3, 0) if dy or dx for pg in [z * NY + ys[dy]]]
    other = [(grid, x * NC + cs[1], 0)]
    ypeers = [(z * NY + ys[dy], atom, ys[dy]) for dy in (2, 1, 3)]

    barrier = pltpu.get_barrier_semaphore()
    for pg, pa, _ in peers + zpeers:
        pl.semaphore_signal(barrier, inc=1, device_id=(pg, pa), device_id_type=MESH)

    loads = [
        pltpu.make_async_copy(src, dst, load_sem.at[n])
        for n, (src, dst) in enumerate(
            [
                (w_hbm, w), (res_hbm, res), (basis_hbm, basis), (atom_hbm, atom_sm), (owner_hbm, owner_sm),
                (hist_hbm, hist_sm), (rho_hbm, rho), (tgt_hbm, tgt), (cpl_hbm, cpl),
            ]
        )
    ]
    for load in loads:
        load.start()

    sub = lax.broadcasted_iota(I32, (8, LANES), 0)
    lane = lax.broadcasted_iota(I32, (8, LANES), 1)
    low = lane < 64

    def to_peers(targets, src, dst, slot, ssem, rsem, later=False):
        for pg, pa, pslot in targets:
            pltpu.make_async_remote_copy(
                src_ref=src,
                dst_ref=dst.at[slot],
                send_sem=ssem,
                recv_sem=rsem,
                device_id=(pg, pa),
                device_id_type=MESH,
            ).start()
        if not later:
            sends.append((dst, len(targets), ssem))

    def all_bytes(dst, count, sem):
        span = dst.at[pl.ds(0, count)]
        pltpu.make_async_copy(span, span, sem).wait()

    def arrived(targets, dst, rsem):
        all_bytes(dst, len(targets), rsem)

    def tree_sum(parts):
        parts = list(parts)
        while len(parts) > 1:
            parts = [a + b for a, b in zip(parts[::2], parts[1::2])] + ([parts[-1]] if len(parts) % 2 else [])
        return parts[0]

    def over_subs(v):
        v = v + pltpu.roll(v, 4, 0)
        v = v + pltpu.roll(v, 2, 0)
        return v + pltpu.roll(v, 1, 0)

    def tile_at(ref, at):
        return ref[:, pl.ds(pl.multiple_of(at * LANES, LANES), LANES)]

    def row_at(ref, at):
        return jnp.broadcast_to(ref[pl.ds(at, 1), :], (8, LANES))

    def basis_tile(kt, at):
        cols = pl.ds(pl.multiple_of(at * LANES, LANES), LANES)
        if kt < 3:
            return basis[pl.ds(kt * 8, 8), cols]
        return jnp.broadcast_to(basis[pl.ds(24, 1), cols], (8, LANES))

    def row_of(columns):
        total = jnp.zeros((8, LANES), F32)
        for d, column in enumerate(columns):
            total = jnp.where(lane == d * 8 + sub, column, total)
        return over_subs(total)

    sends = []

    def all_summed(row, it):
        irow_send[it] = row[0:1]
        to_peers(peers, irow_send.at[it], irow_recv.at[it], me, irow_ss.at[it], irow_rs.at[it])
        return row

    def plane_sum(it):
        arrived(peers, irow_recv.at[it], irow_rs.at[it])
        row = tree_sum([irow_send[it]] + [irow_recv[it, pslot] for _, _, pslot in peers])
        zrow_send[it] = row
        to_peers(zpeers, zrow_send.at[it], zrow_recv.at[it], z, zrow_ss.at[it], zrow_rs.at[it])

    def slice_sum(it):
        arrived(zpeers, zrow_recv.at[it], zrow_rs.at[it])
        row = tree_sum([zrow_send[it]] + [zrow_recv[it, pslot] for _, _, pslot in zpeers])
        return jnp.broadcast_to(row, (8, LANES))

    def mixing(total):
        def entry(i, j):
            d = (i - j) % 8
            at = d * 8 + i if d <= 4 else (8 - d) * 8 + j
            return jnp.broadcast_to(total[:, at : at + 1], (8, LANES))

        a = {(i, j): entry(i, j) for i in range(H) for j in range(i + 1)}
        ridge = RIDGE * tree_sum([a[i, i] for i in range(H)]) / H
        for i in range(H):
            a[i, i] = a[i, i] + ridge
        ones = jnp.ones((8, LANES), F32)
        rhs = [ones] * H
        inverse = []
        factor = {}
        for k in range(H):
            inv = 1.0 / a[k, k]
            inverse.append(inv)
            for i in range(k + 1, H):
                factor[i, k] = a[i, k] * inv
            for i in range(k + 1, H):
                for j in range(k + 1, i + 1):
                    a[i, j] = a[i, j] - factor[i, k] * a[j, k]
                rhs[i] = rhs[i] - factor[i, k] * rhs[k]
        solved = [None] * H
        for k in reversed(range(H)):
            value = rhs[k] * inverse[k]
            for i in range(k + 1, H):
                value = value - factor[i, k] * solved[i]
            solved[k] = value
        share = 1.0 / tree_sum(solved)
        coeffs = [value * share for value in solved]
        column = coeffs[0]
        for i in range(1, H):
            column = jnp.where(sub == i, coeffs[i], column)
        return coeffs, column

    def merge(first, second, bit, axis):
        clear = ((lane if axis == 1 else sub) & bit) == 0
        return jnp.where(clear, first, second) + pltpu.roll(jnp.where(clear, second, first), bit, axis)

    def merge_all(values, bit, axis):
        while len(values) > 1:
            values = [merge(p, q, bit, axis) for p, q in zip(values[::2], values[1::2])]
            bit *= 2
        return values[0]

    def weigh(group):
        for u in range(16):
            at = group * 16 + u
            wrow = row_at(w, at)
            for kt in range(4):
                weighted[u, kt] = basis_tile(kt, at) * wrow

    def batch_sums(group, kt, field):
        return merge_all([weighted[2 * u, kt] * field(2 * u) + weighted[2 * u + 1, kt] * field(2 * u + 1) for u in range(8)], 1, 1)

    def joined(n):
        total = merge_all([merged[g, n] for g in range(batches // 8)], 8, 1)
        return total + pltpu.roll(total, 64, 1)

    def history_moments():
        def step(group, carry):
            weigh(group)

            def cols(u):
                return pl.ds(pl.multiple_of((group * 16 + u) * LANES, LANES), LANES)

            for i in range(H):
                for kt in range(3):
                    merged[group, i * 3 + kt] = batch_sums(
                        group, kt, lambda u: jnp.broadcast_to(res[pl.ds(i, 1), cols(u)], (8, LANES))
                    )
            merged[group, 24] = batch_sums(group, 3, lambda u: res[:, cols(u)])
            return carry

        lax.fori_loop(0, batches // 8, step, 0)
        for n in range(25):
            hist_moms[n] = joined(n)

    def fresh_moments():
        def step(group, carry):
            weigh(group)
            for kt in range(4):
                merged[group, kt] = batch_sums(group, kt, lambda u: row_at(fresh, group * 16 + u))
            return carry

        lax.fori_loop(0, batches // 8, step, 0)
        return [joined(kt) for kt in range(4)]

    def raw_moments(coeffs, column):
        return [tree_sum([coeffs[i] * hist_moms[i * 3 + kt] for i in range(H)]) for kt in range(3)] + [
            over_subs(column * hist_moms[24])
        ]

    def packed(t0, t1, t2, t3):
        first = jnp.where(low, t0, t1)
        second = jnp.where(
            sub < 4, jnp.where(low, t2, pltpu.roll(t2, 4, 0)), jnp.where((sub == 4) & low, t3, 0.0)
        )
        return first, second

    def unpacked(first, second):
        moved = pltpu.roll(second, 64, 1)
        t2 = jnp.where(sub < 4, second, pltpu.roll(moved, 4, 0))
        t3 = jnp.where(sub == 0, pltpu.roll(second, 4, 0), 0.0)
        return first, pltpu.roll(first, 64, 1), t2, t3

    def both_tiles(load):
        return load(pl.ds(0, 8)), pltpu.roll(load(pl.ds(5, 8)), 5, 0)

    def three(v):
        hi = v.astype(jnp.bfloat16)
        rest = v - hi.astype(F32)
        mid = rest.astype(jnp.bfloat16)
        lo = (rest - mid.astype(F32)).astype(jnp.bfloat16)
        return hi, mid, lo

    def pair_joined(a, b):
        return jnp.where(low, a, pltpu.roll(b, 64, 1)), jnp.where(low, pltpu.roll(a, 64, 1), b)

    def keep_moments(hist_at):
        def stays(j, kt):
            return jnp.where(hist_at > j, hist_moms[j * 3 + kt], hist_moms[(j + 1) * 3 + kt])

        tiles_of = [jnp.where(low, stays(j, 0), stays(j, 1)) for j in range(7)]
        tiles_of += [jnp.where(low, stays(2 * m, 2), stays(2 * m + 1, 2)) for m in range(3)]
        tiles_of += [jnp.where(low, stays(6, 2), hist_moms[24])]
        for n, value in enumerate(tiles_of):
            keep_send[n * 8 : n * 8 + 8, :] = value
            kept[c, spot, n * 8 : n * 8 + 8, :] = value

    def shares(coeffs, column, hist_at):
        own = [jnp.where(hist_at > j, coeffs[j], coeffs[j + 1]) for j in range(7)]
        fresh_share = tree_sum([jnp.where(hist_at == i, coeffs[i], 0.0) for i in range(H)])
        return own, fresh_share, jnp.where(sub == hist_at, 0.0, column)

    def combined(own, fresh_share, stay_column):
        doubles = [jnp.where(low, own[2 * m], own[2 * m + 1]) for m in range(3)]
        tail = jnp.where(low, own[6], stay_column)

        def of(core, at, new_first, new_second):
            t = [kept[core, at, n * 8 : n * 8 + 8, :] for n in range(11)]
            first = tree_sum([own[j] * t[j] for j in range(7)] + [fresh_share * new_first])
            u = tree_sum([doubles[m] * t[7 + m] for m in range(3)])
            v = tail * t[10]
            turned = pltpu.roll(v, 64, 1)
            t2 = u + pltpu.roll(u, 64, 1) + jnp.where(low, v, turned)
            second = jnp.where(
                sub < 4,
                jnp.where(low, t2, pltpu.roll(t2, 4, 0)),
                jnp.where((sub == 4) & low, over_subs(turned), 0.0),
            )
            return first, second + fresh_share * new_second

        return of

    def gather_parts(it, combine=None):
        for pair in range(PLANE // 2):
            cols = pl.ds(pair * LANES, LANES)
            raws = [both_tiles(lambda rows: raw_recv[it, 2 * pair + core, rows, :]) for core in range(2)]
            if combine:
                raws = [combine(core, pair, *raws[core]) for core in range(2)]
            for half in range(2):
                a, b = pair_joined(raws[0][half], raws[1][half])
                both = jnp.concatenate([a, b], axis=0)
                for n, part in enumerate(three(both)):
                    xparts[pl.ds(n * 32 + half * 16, 16), cols] = part

    def matched(first_row, count):
        sums = lax.dot_general(
            xparts[...], match[pl.ds(first_row, count), :], (((1,), (1,)), ((), ())), preferred_element_type=F32
        )
        return sums[0:32] + sums[32:64] + sums[64:96]

    def owner_kept():
        for pair in range(PLANE // 2):
            cols = pl.ds(pair * LANES, LANES)
            for n in range(11):
                both = pair_joined(kept[0, pair, n * 8 : n * 8 + 8, :], kept[1, pair, n * 8 : n * 8 + 8, :])
                for m, part in enumerate(three(jnp.concatenate(both, axis=0))):
                    xkept[pl.ds(m * 176 + n * 16, 16), cols] = part
        sums = lax.dot_general(
            xkept[...], match[pl.ds(NZ * 64, LANES), :], (((1,), (1,)), ((), ())), preferred_element_type=F32
        )
        own_kept[...] = sums[0:176] + sums[176:352] + sums[352:528]

    def owner_fresh(it):
        gather_parts(it)
        own_fresh[...] = matched(NZ * 64, LANES)

    def owner_partial(own, fresh_share, stay_column):
        def of(n):
            return own_kept[n * 8 : n * 8 + 8]

        new = [fresh_share * own_fresh[n * 8 : n * 8 + 8] for n in range(4)]
        part_send[0:8] = tree_sum([own[j] * of(2 * j) for j in range(7)] + [new[0]])
        part_send[8:16] = tree_sum([own[j] * of(2 * j + 1) for j in range(7)] + [new[1]])
        part_send[16:24] = tree_sum(
            [own[j] * of(14 + j) for j in range(7)] + [jnp.where(sub < 4, new[2], pltpu.roll(new[3], 4, 0))]
        )
        part_send[24:25] = (over_subs(stay_column * of(21)) + pltpu.roll(new[2], 4, 0))[0:1]

    def peer_values(it, first):
        picked = matched(first * 64, 256)
        for pair in range(2):
            cols = slice(pair * LANES, (pair + 1) * LANES)
            for half in range(2):
                values = pair_joined(picked[half * 16 : half * 16 + 8, cols], picked[half * 16 + 8 : half * 16 + 16, cols])
                for n, value in enumerate(values):
                    size = 5 if half else 8
                    back_send[it, first + 2 * pair + n, half * 8 : half * 8 + size, :] = value[0:size]

    def damped(kt, value):
        k = sub + kt * 8
        damp = jnp.where(k < 1, 1.0, jnp.where(k < 4, 1 / 2, jnp.where(k < 9, 1 / 3, jnp.where(k < 16, 1 / 4, 1 / 5))))
        return value * (damp * (scale * BETA))

    def send_raw(it, values):
        first, second = packed(*values)
        for ref, at in ((raw_send, (it,)), (raw_recv, (it, me))):
            ref[(*at, pl.ds(0, 8))] = first
            ref[(*at, pl.ds(8, 5))] = second[0:5]
        to_peers(peers, raw_send.at[it], raw_recv.at[it], me, raw_ss.at[it], raw_rs.at[it])

    loads[0].wait()
    loads[1].wait()

    def products(step_at, accs):
        accs = list(accs)
        for u in range(4):
            at = step_at * 4 + u
            r = tile_at(res, at)
            wr = r * row_at(w, at)
            accs[0] = accs[0] + wr * r
            for d in range(1, 5):
                accs[d] = accs[d] + wr * pltpu.roll(r, d, 0)
        return tuple(accs)

    accs = lax.fori_loop(0, tiles // 4, products, (jnp.zeros((8, LANES), F32),) * 5)
    first_row = row_of([jnp.sum(acc, axis=1, keepdims=True) for acc in accs])

    pl.semaphore_wait(barrier, len(peers) + len(zpeers))
    all_summed(first_row, 0)
    for load in loads[3:6]:
        load.wait()

    def slot_step(b, row):
        return jnp.where(lane == b, owner_sm[atom_sm[b]], row)

    slots = lax.fori_loop(0, batches, slot_step, jnp.full((8, LANES), -1, I32), unroll=4)
    slot_send[...] = slots[0:1]
    slot_recv[me] = slots[0:1]
    zslot_recv[z] = slots[0:1]
    to_peers(peers, slot_send, slot_recv, me, slot_ss, slot_rs)
    to_peers(zpeers, slot_send, zslot_recv, z, zslot_ss, zslot_rs)
    loads[2].wait()
    history_moments()
    for load in loads[6:]:
        load.wait()

    plane_sum(0)

    arrived(peers, slot_recv, slot_rs)
    arrived(zpeers, zslot_recv, zslot_rs)
    first_slot = atom * 512 + y * LANES
    sources = []
    for pair in range(PLANE // 2):
        left = jnp.broadcast_to(slot_recv[2 * pair], (8, LANES))
        right = jnp.broadcast_to(slot_recv[2 * pair + 1], (8, LANES))
        sources.append(jnp.where(low, left, pltpu.roll(right, 64, 1)))

    def match_rows(at, wanted):
        for pair in range(PLANE // 2):
            halves = [jnp.where(sources[pair] == one, 1.0, 0.0) for one in wanted]
            match[pl.ds(at, 16), pl.ds(pair * LANES, LANES)] = jnp.concatenate(halves, axis=0).astype(jnp.bfloat16)

    for block, pz in enumerate(zorder):
        row = jnp.broadcast_to(zslot_recv[pz], (8, LANES)).astype(F32)

        def target_step(st, carry):
            wanted = []
            for h in range(2):
                hit = lane == sub + (st * 16 + h * 8)
                column = jnp.sum(jnp.where(hit, row, 0.0), axis=1, keepdims=True)
                wanted.append(jnp.broadcast_to(column, (8, LANES)).astype(I32))
            match_rows(pl.multiple_of(block * 64 + st * 16, 16), wanted)
            return carry

        lax.fori_loop(0, 4, target_step, 0)
    for st in range(LANES // 16):
        match_rows(NZ * 64 + st * 16, [sub + (first_slot + st * 16 + h * 8) for h in range(2)])

    total = slice_sum(0)
    for it in range(ITERS):
        last = it == ITERS - 1
        coeffs, column = mixing(total)
        if last:
            split = shares(coeffs, column, hist_sm[0])
            owner_partial(*split)
            to_peers(zpeers, part_send, part_recv, z, part_ss, part_rs)
            gather_parts(it, combined(*split))
        else:
            send_raw(it, raw_moments(coeffs, column))
            keep_moments(hist_sm[it])
            arrived(peers, raw_recv.at[it], raw_rs.at[it])
            to_peers(alike, keep_send, kept.at[c], spot, keep_ss, keep_rs)
            gather_parts(it)
        for first in (0, 4):
            peer_values(it, first)
            for n, target in list(enumerate(zpeers))[first : first + 4]:
                to_peers([target], back_send.at[it, n], back_recv.at[it], z, back_ss.at[it], back_rs.at[it], True)
        sends.append((back_recv.at[it], len(zpeers), back_ss.at[it]))
        if last:
            arrived(zpeers, part_recv, part_rs)
            block = tree_sum([part_send[...]] + [part_recv[pslot] for _, _, pslot in zpeers]) * scale
            blk_send[...] = block
            to_peers(ypeers, blk_send, blk_recv, y, blk_ss, blk_rs)
            blk_recv[y] = block
        arrived(zpeers, back_recv.at[it], back_rs.at[it])
        mine = both_tiles(
            lambda rows: tree_sum([back_send[it, NZ - 1, rows, :]] + [back_recv[it, pslot, rows, :] for _, _, pslot in zpeers])
        )
        at_batch = tuple(damped(kt, t) for kt, t in enumerate(unpacked(*mine)))
        hist_at = hist_sm[it]

        def density_step(group, carry):
            at_tiles, acc = carry
            rows = pl.ds(pl.multiple_of(group * 8, 8), 8)
            parts = []
            for u in range(4):
                spread = [jnp.broadcast_to(t[:, u : u + 1], (8, LANES)) for t in at_tiles]
                for half in range(2):
                    at = group * 8 + u * 2 + half
                    v = column * (tile_at(rho, at) + BETA * tile_at(res, at))
                    parts.append(v - tree_sum([basis_tile(kt, at) * spread[kt] for kt in range(4)]))
            dens = merge_all(parts, 1, 0)
            if last:
                dens_out[rows, :] = dens
            else:
                new = tgt[rows, :] + cpl[rows, :] * jnp.tanh(dens) - dens
                fresh[rows, :] = new
                weighed = new * w[rows, :]
                for u in range(8):
                    cols = pl.ds(pl.multiple_of((group * 8 + u) * LANES, LANES), LANES)
                    r = jnp.where(sub == hist_at, jnp.broadcast_to(new[u : u + 1], (8, LANES)), res[:, cols])
                    res[:, cols] = r
                    rho[:, cols] = jnp.where(sub == hist_at, jnp.broadcast_to(dens[u : u + 1], (8, LANES)), rho[:, cols])
                    acc = acc + r * jnp.broadcast_to(weighed[u : u + 1], (8, LANES))
            return tuple(pltpu.roll(t, LANES - 4, 1) for t in at_tiles), acc

        _, acc = lax.fori_loop(0, batches // 4, density_step, (at_batch, jnp.zeros((8, LANES), F32)), unroll=4)
        if not last:
            mine_new = jnp.broadcast_to(jnp.sum(acc, axis=1, keepdims=True), (8, LANES))
            columns = [
                jnp.where(sub == hist_at, pltpu.roll(mine_new, d, 0) if d else mine_new, mine_new) for d in range(5)
            ]
            all_summed(row_of(columns), it + 1)
            send_raw(it + 1, fresh_moments())
            arrived(alike, kept.at[0], keep_rs)
            to_peers(other, kept.at[c], kept, c, pair_ss, pair_rs)
            plane_sum(it + 1)
            arrived(other, kept, pair_rs)
            owner_kept()
            arrived(peers, raw_recv.at[it + 1], raw_rs.at[it + 1])
            owner_fresh(it + 1)
            row_i = lane % 8
            row_j = (row_i - lane // 8 + 8) % 8
            total = jnp.where((row_i == hist_at) | (row_j == hist_at), slice_sum(it + 1), total)

    arrived(ypeers, blk_recv, blk_rs)
    for q in range(NY):
        mom_out[:, q * LANES : (q + 1) * LANES] = blk_recv[q]
    for dst, count, ssem in sends:
        all_bytes(dst, count, ssem)


def local(weights, target, coupling, multipole_basis, rho_hist, res_hist, batch_atom, owner_slot, slot_index):
    points = weights.shape[0]
    batches = batch_atom.shape[0]
    tiles = points // LANES
    slots = owner_slot.shape[0]
    owned = slots // lax.axis_size("atom")
    scale = 1.0 / math.sqrt(points * lax.axis_size("grid") // owned)
    square = lambda v: v.reshape(tiles, LANES)
    vm, sm, dma = pltpu.VMEM, pltpu.SMEM, pltpu.SemaphoreType.DMA
    anywhere = pl.BlockSpec(memory_space=pl.ANY)
    vmem = pl.BlockSpec(memory_space=pltpu.VMEM)
    density, moments = pl.pallas_call(
        functools.partial(kernel, tiles, batches, scale),
        out_shape=(pltpu.VMEM((tiles, LANES), F32), pltpu.VMEM((LM, owned), F32)),
        in_specs=[anywhere] * 9,
        out_specs=(vmem, vmem),
        scratch_shapes=[
            vm((tiles, LANES), F32), vm((tiles, LANES), F32), vm((tiles, LANES), F32),
            vm((LM, points), F32), vm((H, points), F32), vm((H, points), F32),
            vm((tiles, LANES), F32), vm((16, 4, 8, LANES), F32), vm((batches // 8, 25, 8, LANES), F32), vm((25, 8, LANES), F32),
            sm((batches,), I32), sm((slots,), I32), sm((ITERS,), I32),
            vm((1, LANES), I32), vm((PLANE, 1, LANES), I32), vm((NZ, 1, LANES), I32),
            vm((ITERS, 1, LANES), F32), vm((ITERS, PLANE, 1, LANES), F32),
            vm((ITERS, 1, LANES), F32), vm((ITERS, NZ, 1, LANES), F32),
            vm((ITERS, 13, LANES), F32), vm((ITERS, PLANE, 13, LANES), F32),
            vm((LM, LANES), F32), vm((NZ, LM, LANES), F32),
            vm((ITERS, NZ, 13, LANES), F32), vm((ITERS, NZ, 13, LANES), F32),
            vm((LM, LANES), F32), vm((NY, LM, LANES), F32),
            vm((88, LANES), F32), vm((NC, NY * NX, 88, LANES), F32),
            vm((NZ * 64 + LANES, PLANE * 64), jnp.bfloat16), vm((96, PLANE * 64), jnp.bfloat16),
            vm((528, PLANE * 64), jnp.bfloat16), vm((176, LANES), F32), vm((32, LANES), F32),
            dma((9,)),
            dma, dma, dma, dma, dma((ITERS,)), dma((ITERS,)), dma((ITERS,)), dma((ITERS,)),
            dma((ITERS,)), dma((ITERS,)), dma, dma, dma((ITERS,)), dma((ITERS,)), dma, dma, dma, dma, dma, dma,
        ],
        compiler_params=pltpu.CompilerParams(collective_id=0, has_side_effects=True),
    )(
        square(weights), square(target), square(coupling), multipole_basis, rho_hist, res_hist,
        batch_atom, owner_slot, slot_index,
    )
    return density.reshape(points), moments


def solution(mesh):
    both = ("grid", "atom")
    placed = (P(both), P(both), P(both), P(None, both), P(None, both), P(None, both), P(both), P(), P())
    return jax.shard_map(
        local, mesh=mesh, in_specs=placed, out_specs=(P(both), P(None, "atom")), check_vma=False
    )
```

```python
import functools
import math

import jax
import jax.numpy as jnp
import numpy as np
from jax import lax
from jax.experimental import pallas as pl
from jax.experimental.pallas import tpu as pltpu
from jax.sharding import PartitionSpec as P

H = 8
LM = 25
ITERS = 2
BETA = 0.5
RIDGE = 0.1
LANES = 128
NZ, NY, NX, NC = 8, 4, 4, 2
PLANE = NY * NX * NC
MESH = pl.DeviceIdType.MESH
F32 = jnp.float32
I32 = jnp.int32


def kernel(
    tiles, batches, scale,
    w_hbm, tgt_hbm, cpl_hbm, basis_hbm, rho_hbm, res_hbm, atom_hbm, owner_hbm, hist_hbm,
    dens_out, mom_out,
    w, tgt, cpl, basis, rho, res, fresh, mixed, weighted, merged, hist_moms,
    atom_sm, owner_sm, hist_sm,
    slot_send, slot_recv, zslot_recv, irow_send, irow_recv, zrow_send, zrow_recv,
    raw_send, raw_recv, part_send, part_recv, back_send, back_recv, blk_send, blk_recv,
    early_send, early, keep_send, kept, match, xparts, xkept, own_kept, own_fresh,
    load_sem,
    slot_ss, slot_rs, zslot_ss, zslot_rs, irow_ss, irow_rs, zrow_ss, zrow_rs,
    raw_ss, raw_rs, part_ss, part_rs, back_ss, back_rs, blk_ss, blk_rs, keep_ss, keep_rs, pair_ss, pair_rs,
    early_ss, early_rs, epair_ss, epair_rs,
):
    grid = lax.axis_index("grid")
    atom = lax.axis_index("atom")
    z, y = grid // NY, grid % NY
    x, c = atom // NC, atom % NC
    me = y * (NX * NC) + atom

    ys = [(y + d) % NY for d in range(NY)]
    xs = [(x + d) % NX for d in range(NX)]
    cs = [c, 1 - c]
    peers = []
    for dy in (2, 1, 3, 0):
        for dx in (2, 1, 3, 0):
            for dc in (1, 0):
                if dy or dx or dc:
                    pa = xs[dx] * NC + cs[dc]
                    peers.append((z * NY + ys[dy], pa, ys[dy] * (NX * NC) + pa))
    zpeers = []
    zorder = [(z + dz) % NZ for dz in (4, 3, 5, 2, 6, 1, 7, 0)]
    for pz in zorder[:-1]:
        zpeers.append((pz * NY + y, atom, pz))
    spot = y * NX + x
    alike = [(pg, xs[dx] * NC + c, 0) for dy in (2, 1, 3, 0) for dx in (2, 1, 3, 0) if dy or dx for pg in [z * NY + ys[dy]]]
    other = [(grid, x * NC + cs[1], 0)]
    ypeers = [(z * NY + ys[dy], atom, ys[dy]) for dy in (2, 1, 3)]

    barrier = pltpu.get_barrier_semaphore()
    for pg, pa, _ in peers + zpeers:
        pl.semaphore_signal(barrier, inc=1, device_id=(pg, pa), device_id_type=MESH)

    loads = [
        pltpu.make_async_copy(src, dst, load_sem.at[n])
        for n, (src, dst) in enumerate(
            [
                (w_hbm, w), (res_hbm, res), (basis_hbm, basis), (atom_hbm, atom_sm), (owner_hbm, owner_sm),
                (hist_hbm, hist_sm), (rho_hbm, rho), (tgt_hbm, tgt), (cpl_hbm, cpl),
            ]
        )
    ]
    for load in loads:
        load.start()

    sub = lax.broadcasted_iota(I32, (8, LANES), 0)
    lane = lax.broadcasted_iota(I32, (8, LANES), 1)
    low = lane < 64

    def to_peers(targets, src, dst, slot, ssem, rsem, later=False):
        for pg, pa, pslot in targets:
            pltpu.make_async_remote_copy(
                src_ref=src,
                dst_ref=dst.at[slot],
                send_sem=ssem,
                recv_sem=rsem,
                device_id=(pg, pa),
                device_id_type=MESH,
            ).start()
        if not later:
            sends.append((dst, len(targets), ssem))

    def all_bytes(dst, count, sem):
        span = dst.at[pl.ds(0, count)]
        pltpu.make_async_copy(span, span, sem).wait()

    def arrived(targets, dst, rsem):
        all_bytes(dst, len(targets), rsem)

    def tree_sum(parts):
        parts = list(parts)
        while len(parts) > 1:
            parts = [a + b for a, b in zip(parts[::2], parts[1::2])] + ([parts[-1]] if len(parts) % 2 else [])
        return parts[0]

    def over_subs(v):
        v = v + pltpu.roll(v, 4, 0)
        v = v + pltpu.roll(v, 2, 0)
        return v + pltpu.roll(v, 1, 0)

    def columns_of(at):
        return pl.ds(at * LANES if isinstance(at, int) else pl.multiple_of(at * LANES, LANES), LANES)

    def tile_at(ref, at):
        return ref[:, columns_of(at)]

    def row_at(ref, at):
        return jnp.broadcast_to(ref[pl.ds(at, 1), :], (8, LANES))

    def basis_tile(kt, at):
        cols = columns_of(at)
        if kt < 3:
            return basis[pl.ds(kt * 8, 8), cols]
        return jnp.broadcast_to(basis[pl.ds(24, 1), cols], (8, LANES))

    def row_of(columns):
        total = jnp.zeros((8, LANES), F32)
        for d, column in enumerate(columns):
            total = jnp.where(lane == d * 8 + sub, column, total)
        return over_subs(total)

    sends = []

    def all_summed(row, it):
        irow_send[it] = row[0:1]
        to_peers(peers, irow_send.at[it], irow_recv.at[it], me, irow_ss.at[it], irow_rs.at[it])
        return row

    def plane_sum(it):
        arrived(peers, irow_recv.at[it], irow_rs.at[it])
        row = tree_sum([irow_send[it]] + [irow_recv[it, pslot] for _, _, pslot in peers])
        zrow_send[it] = row
        to_peers(zpeers, zrow_send.at[it], zrow_recv.at[it], z, zrow_ss.at[it], zrow_rs.at[it])

    def slice_sum(it):
        arrived(zpeers, zrow_recv.at[it], zrow_rs.at[it])
        row = tree_sum([zrow_send[it]] + [zrow_recv[it, pslot] for _, _, pslot in zpeers])
        return jnp.broadcast_to(row, (8, LANES))

    def mixing(total):
        def entry(i, j):
            d = (i - j) % 8
            at = d * 8 + i if d <= 4 else (8 - d) * 8 + j
            return jnp.broadcast_to(total[:, at : at + 1], (8, LANES))

        a = {(i, j): entry(i, j) for i in range(H) for j in range(i + 1)}
        ridge = RIDGE * tree_sum([a[i, i] for i in range(H)]) / H
        for i in range(H):
            a[i, i] = a[i, i] + ridge
        ones = jnp.ones((8, LANES), F32)
        rhs = [ones] * H
        inverse = []
        factor = {}
        for k in range(H):
            inv = 1.0 / a[k, k]
            inverse.append(inv)
            for i in range(k + 1, H):
                factor[i, k] = a[i, k] * inv
            for i in range(k + 1, H):
                for j in range(k + 1, i + 1):
                    a[i, j] = a[i, j] - factor[i, k] * a[j, k]
                rhs[i] = rhs[i] - factor[i, k] * rhs[k]
        solved = [None] * H
        for k in reversed(range(H)):
            value = rhs[k] * inverse[k]
            for i in range(k + 1, H):
                value = value - factor[i, k] * solved[i]
            solved[k] = value
        share = 1.0 / tree_sum(solved)
        coeffs = [value * share for value in solved]
        column = coeffs[0]
        for i in range(1, H):
            column = jnp.where(sub == i, coeffs[i], column)
        return coeffs, column

    def merge(first, second, bit, axis):
        clear = ((lane if axis == 1 else sub) & bit) == 0
        return jnp.where(clear, first, second) + pltpu.roll(jnp.where(clear, second, first), bit, axis)

    def merge_all(values, bit, axis):
        while len(values) > 1:
            values = [merge(p, q, bit, axis) for p, q in zip(values[::2], values[1::2])]
            bit *= 2
        return values[0]

    def weigh(group):
        for u in range(16):
            at = group * 16 + u
            wrow = row_at(w, at)
            for kt in range(4):
                weighted[u, kt] = basis_tile(kt, at) * wrow

    def batch_sums(group, kt, field):
        return merge_all([weighted[2 * u, kt] * field(2 * u) + weighted[2 * u + 1, kt] * field(2 * u + 1) for u in range(8)], 1, 1)

    def joined(n):
        total = merge_all([merged[g, n] for g in range(batches // 8)], 8, 1)
        return total + pltpu.roll(total, 64, 1)

    def history_moments():
        def step(group, carry):
            weigh(group)

            def cols(u):
                return pl.ds(pl.multiple_of((group * 16 + u) * LANES, LANES), LANES)

            for i in range(H):
                for kt in range(3):
                    merged[group, i * 3 + kt] = batch_sums(
                        group, kt, lambda u: jnp.broadcast_to(res[pl.ds(i, 1), cols(u)], (8, LANES))
                    )
            merged[group, 24] = batch_sums(group, 3, lambda u: res[:, cols(u)])
            return carry

        lax.fori_loop(0, batches // 8, step, 0)
        for n in range(25):
            hist_moms[n] = joined(n)

    def fresh_moments():
        def step(group, carry):
            weigh(group)
            for kt in range(4):
                merged[group, kt] = batch_sums(group, kt, lambda u: row_at(fresh, group * 16 + u))
            return carry

        lax.fori_loop(0, batches // 8, step, 0)
        return [joined(kt) for kt in range(4)]

    def raw_moments(coeffs, column):
        return [tree_sum([coeffs[i] * hist_moms[i * 3 + kt] for i in range(H)]) for kt in range(3)] + [
            over_subs(column * hist_moms[24])
        ]

    def packed(t0, t1, t2, t3):
        first = jnp.where(low, t0, t1)
        second = jnp.where(
            sub < 4, jnp.where(low, t2, pltpu.roll(t2, 4, 0)), jnp.where((sub == 4) & low, t3, 0.0)
        )
        return first, second

    def unpacked(first, second):
        moved = pltpu.roll(second, 64, 1)
        t2 = jnp.where(sub < 4, second, pltpu.roll(moved, 4, 0))
        t3 = jnp.where(sub == 0, pltpu.roll(second, 4, 0), 0.0)
        return first, pltpu.roll(first, 64, 1), t2, t3

    def both_tiles(load):
        return load(pl.ds(0, 8)), pltpu.roll(load(pl.ds(5, 8)), 5, 0)

    def three(v):
        hi = v.astype(jnp.bfloat16)
        rest = v - hi.astype(F32)
        mid = rest.astype(jnp.bfloat16)
        lo = (rest - mid.astype(F32)).astype(jnp.bfloat16)
        return hi, mid, lo

    def pair_joined(a, b):
        return jnp.where(low, a, pltpu.roll(b, 64, 1)), jnp.where(low, pltpu.roll(a, 64, 1), b)

    def keep_moments(hist_at):
        def stays(j, kt):
            return jnp.where(hist_at > j, hist_moms[j * 3 + kt], hist_moms[(j + 1) * 3 + kt])

        tiles_of = [jnp.where(low, stays(j, 0), stays(j, 1)) for j in range(7)]
        tiles_of += [jnp.where(low, stays(2 * m, 2), stays(2 * m + 1, 2)) for m in range(3)]
        tiles_of += [jnp.where(low, stays(6, 2), hist_moms[24])]
        for n, value in enumerate(tiles_of):
            send, ref, at = (early_send, early, n) if n < 5 else (keep_send, kept, n - 5)
            send[at * 8 : at * 8 + 8, :] = value
            ref[c, spot, at * 8 : at * 8 + 8, :] = value

    def kept_tile(core, at, n):
        ref, n = (early, n) if n < 5 else (kept, n - 5)
        return ref[core, at, n * 8 : n * 8 + 8, :]

    def shares(coeffs, column, hist_at):
        own = [jnp.where(hist_at > j, coeffs[j], coeffs[j + 1]) for j in range(7)]
        fresh_share = tree_sum([jnp.where(hist_at == i, coeffs[i], 0.0) for i in range(H)])
        return own, fresh_share, jnp.where(sub == hist_at, 0.0, column)

    def combined(own, fresh_share, stay_column):
        doubles = [jnp.where(low, own[2 * m], own[2 * m + 1]) for m in range(3)]
        tail = jnp.where(low, own[6], stay_column)

        def of(core, at, new_first, new_second):
            t = [kept_tile(core, at, n) for n in range(11)]
            first = tree_sum([own[j] * t[j] for j in range(7)] + [fresh_share * new_first])
            u = tree_sum([doubles[m] * t[7 + m] for m in range(3)])
            v = tail * t[10]
            turned = pltpu.roll(v, 64, 1)
            t2 = u + pltpu.roll(u, 64, 1) + jnp.where(low, v, turned)
            second = jnp.where(
                sub < 4,
                jnp.where(low, t2, pltpu.roll(t2, 4, 0)),
                jnp.where((sub == 4) & low, over_subs(turned), 0.0),
            )
            return first, second + fresh_share * new_second

        return of

    def gather_parts(it, combine=None):
        for pair in range(PLANE // 2):
            cols = pl.ds(pair * LANES, LANES)
            raws = [both_tiles(lambda rows: raw_recv[it, 2 * pair + core, rows, :]) for core in range(2)]
            if combine:
                raws = [combine(core, pair, *raws[core]) for core in range(2)]
            for half in range(2):
                a, b = pair_joined(raws[0][half], raws[1][half])
                both = jnp.concatenate([a, b], axis=0)
                for n, part in enumerate(three(both)):
                    xparts[pl.ds(n * 32 + half * 16, 16), cols] = part

    def matched(first_row, count):
        sums = lax.dot_general(
            xparts[...], match[pl.ds(first_row, count), :], (((1,), (1,)), ((), ())), preferred_element_type=F32
        )
        return sums[0:32] + sums[32:64] + sums[64:96]

    def owner_kept(first, count):
        size = count * 16
        for pair in range(PLANE // 2):
            cols = pl.ds(pair * LANES, LANES)
            for n in range(count):
                both = pair_joined(kept_tile(0, pair, first + n), kept_tile(1, pair, first + n))
                for m, part in enumerate(three(jnp.concatenate(both, axis=0))):
                    xkept[pl.ds(m * size + n * 16, 16), cols] = part
        sums = lax.dot_general(
            xkept[pl.ds(0, 3 * size), :], match[pl.ds(NZ * 64, LANES), :], (((1,), (1,)), ((), ())), preferred_element_type=F32
        )
        own_kept[first * 16 : first * 16 + size] = sums[0:size] + sums[size : 2 * size] + sums[2 * size : 3 * size]

    def owner_fresh(it):
        gather_parts(it)
        own_fresh[...] = matched(NZ * 64, LANES)

    def owner_partial(own, fresh_share, stay_column):
        def of(n):
            return own_kept[n * 8 : n * 8 + 8]

        new = [fresh_share * own_fresh[n * 8 : n * 8 + 8] for n in range(4)]
        part_send[0:8] = tree_sum([own[j] * of(2 * j) for j in range(7)] + [new[0]])
        part_send[8:16] = tree_sum([own[j] * of(2 * j + 1) for j in range(7)] + [new[1]])
        part_send[16:24] = tree_sum(
            [own[j] * of(14 + j) for j in range(7)] + [jnp.where(sub < 4, new[2], pltpu.roll(new[3], 4, 0))]
        )
        part_send[24:25] = (over_subs(stay_column * of(21)) + pltpu.roll(new[2], 4, 0))[0:1]

    def peer_values(it, first):
        picked = matched(first * 64, LANES)
        for pair in range(1):
            cols = slice(pair * LANES, (pair + 1) * LANES)
            for half in range(2):
                values = pair_joined(picked[half * 16 : half * 16 + 8, cols], picked[half * 16 + 8 : half * 16 + 16, cols])
                for n, value in enumerate(values):
                    size = 5 if half else 8
                    back_send[it, first + 2 * pair + n, half * 8 : half * 8 + size, :] = value[0:size]

    def damped(kt, value):
        k = sub + kt * 8
        damp = jnp.where(k < 1, 1.0, jnp.where(k < 4, 1 / 2, jnp.where(k < 9, 1 / 3, jnp.where(k < 16, 1 / 4, 1 / 5))))
        return value * (damp * (scale * BETA))

    def send_raw(it, values):
        first, second = packed(*values)
        for ref, at in ((raw_send, (it,)), (raw_recv, (it, me))):
            ref[(*at, pl.ds(0, 8))] = first
            ref[(*at, pl.ds(8, 5))] = second[0:5]
        to_peers(peers, raw_send.at[it], raw_recv.at[it], me, raw_ss.at[it], raw_rs.at[it])

    loads[0].wait()
    loads[1].wait()

    def products(step_at, accs):
        accs = list(accs)
        for u in range(4):
            at = step_at * 4 + u
            r = tile_at(res, at)
            wr = r * row_at(w, at)
            accs[0] = accs[0] + wr * r
            for d in range(1, 5):
                accs[d] = accs[d] + wr * pltpu.roll(r, d, 0)
        return tuple(accs)

    accs = lax.fori_loop(0, tiles // 4, products, (jnp.zeros((8, LANES), F32),) * 5)
    first_row = row_of([jnp.sum(acc, axis=1, keepdims=True) for acc in accs])

    pl.semaphore_wait(barrier, len(peers) + len(zpeers))
    all_summed(first_row, 0)
    for load in loads[3:6]:
        load.wait()

    def slot_step(b, row):
        return jnp.where(lane == b, owner_sm[atom_sm[b]], row)

    slots = lax.fori_loop(0, batches, slot_step, jnp.full((8, LANES), -1, I32), unroll=4)
    slot_send[...] = slots[0:1]
    slot_recv[me] = slots[0:1]
    zslot_recv[z] = slots[0:1]
    to_peers(peers, slot_send, slot_recv, me, slot_ss, slot_rs)
    to_peers(zpeers, slot_send, zslot_recv, z, zslot_ss, zslot_rs)
    loads[2].wait()
    history_moments()
    for load in loads[6:]:
        load.wait()

    plane_sum(0)
    keep_moments(hist_sm[0])
    to_peers(alike, early_send, early.at[c], spot, early_ss, early_rs)

    arrived(peers, slot_recv, slot_rs)
    arrived(zpeers, zslot_recv, zslot_rs)
    first_slot = atom * 512 + y * LANES
    sources = []
    for pair in range(PLANE // 2):
        left = jnp.broadcast_to(slot_recv[2 * pair], (8, LANES))
        right = jnp.broadcast_to(slot_recv[2 * pair + 1], (8, LANES))
        sources.append(jnp.where(low, left, pltpu.roll(right, 64, 1)))

    def match_rows(at, wanted):
        for pair in range(PLANE // 2):
            halves = [jnp.where(sources[pair] == one, 1.0, 0.0) for one in wanted]
            match[pl.ds(at, 16), pl.ds(pair * LANES, LANES)] = jnp.concatenate(halves, axis=0).astype(jnp.bfloat16)

    for block, pz in enumerate(zorder):
        row = jnp.broadcast_to(zslot_recv[pz], (8, LANES)).astype(F32)

        def target_step(st, carry):
            wanted = []
            for h in range(2):
                hit = lane == sub + (st * 16 + h * 8)
                column = jnp.sum(jnp.where(hit, row, 0.0), axis=1, keepdims=True)
                wanted.append(jnp.broadcast_to(column, (8, LANES)).astype(I32))
            match_rows(pl.multiple_of(block * 64 + st * 16, 16), wanted)
            return carry

        lax.fori_loop(0, 4, target_step, 0)
    for st in range(LANES // 16):
        match_rows(NZ * 64 + st * 16, [sub + (first_slot + st * 16 + h * 8) for h in range(2)])

    total = slice_sum(0)
    for it in range(ITERS):
        last = it == ITERS - 1
        coeffs, column = mixing(total)
        if last:
            split = shares(coeffs, column, hist_sm[0])
            owner_partial(*split)
            to_peers(zpeers, part_send, part_recv, z, part_ss, part_rs)
            gather_parts(it, combined(*split))
        else:
            send_raw(it, raw_moments(coeffs, column))
            arrived(peers, raw_recv.at[it], raw_rs.at[it])
            to_peers(alike, keep_send, kept.at[c], spot, keep_ss, keep_rs)
            arrived(alike, early.at[0], early_rs)
            to_peers(other, early.at[c], early, c, epair_ss, epair_rs)
            gather_parts(it)
        for first in (0, 2, 4, 6):
            peer_values(it, first)
            for n, target in list(enumerate(zpeers))[first : first + 2]:
                to_peers([target], back_send.at[it, n], back_recv.at[it], z, back_ss.at[it], back_rs.at[it], True)
        sends.append((back_recv.at[it], len(zpeers), back_ss.at[it]))
        if last:
            arrived(zpeers, part_recv, part_rs)
            block = tree_sum([part_send[...]] + [part_recv[pslot] for _, _, pslot in zpeers]) * scale
            blk_send[...] = block
            to_peers(ypeers, blk_send, blk_recv, y, blk_ss, blk_rs)
            blk_recv[y] = block
        if not last:
            arrived(other, early, epair_rs)
            owner_kept(0, 5)
        arrived(zpeers, back_recv.at[it], back_rs.at[it])
        mine = both_tiles(
            lambda rows: tree_sum([back_send[it, NZ - 1, rows, :]] + [back_recv[it, pslot, rows, :] for _, _, pslot in zpeers])
        )
        at_batch = tuple(damped(kt, t) for kt, t in enumerate(unpacked(*mine)))
        hist_at = hist_sm[it]

        accs = []
        for group in range(batches // 4):
            rows = pl.ds(group * 8, 8)
            spread = [[jnp.broadcast_to(t[:, u : u + 1], (8, LANES)) for t in at_batch] for u in range(group * 4, group * 4 + 4)]
            parts = []
            for n in range(8):
                at = group * 8 + n
                v = column * (tile_at(rho, at) + BETA * tile_at(res, at))
                parts.append(v - tree_sum([basis_tile(kt, at) * spread[n // 2][kt] for kt in range(4)]))
            dens = merge_all(parts, 1, 0)
            if last:
                dens_out[rows, :] = dens
            else:
                new = tgt[rows, :] + cpl[rows, :] * jnp.tanh(dens) - dens
                fresh[rows, :] = new
                mixed[rows, :] = dens
                weighed = new * w[rows, :]
                for n in range(8):
                    r = jnp.where(
                        sub == hist_at, jnp.broadcast_to(new[n : n + 1], (8, LANES)), tile_at(res, group * 8 + n)
                    )
                    accs.append(r * jnp.broadcast_to(weighed[n : n + 1], (8, LANES)))
                accs = [tree_sum(accs)]

        if not last:
            mine_new = jnp.broadcast_to(jnp.sum(accs[0], axis=1, keepdims=True), (8, LANES))
            columns = [
                jnp.where(sub == hist_at, pltpu.roll(mine_new, d, 0) if d else mine_new, mine_new) for d in range(5)
            ]
            all_summed(row_of(columns), it + 1)
            send_raw(it + 1, fresh_moments())

            def replace(step_at, carry):
                for n in range(8):
                    at = step_at * 8 + n
                    cols = pl.ds(pl.multiple_of(at * LANES, LANES), LANES)
                    res[:, cols] = jnp.where(sub == hist_at, row_at(fresh, at), res[:, cols])
                    rho[:, cols] = jnp.where(sub == hist_at, row_at(mixed, at), rho[:, cols])
                return carry

            lax.fori_loop(0, tiles // 8, replace, 0)
            plane_sum(it + 1)
            arrived(alike, kept.at[0], keep_rs)
            to_peers(other, kept.at[c], kept, c, pair_ss, pair_rs)
            arrived(other, kept, pair_rs)
            owner_kept(5, 6)
            arrived(peers, raw_recv.at[it + 1], raw_rs.at[it + 1])
            owner_fresh(it + 1)
            row_i = lane % 8
            row_j = (row_i - lane // 8 + 8) % 8
            total = jnp.where((row_i == hist_at) | (row_j == hist_at), slice_sum(it + 1), total)

    arrived(ypeers, blk_recv, blk_rs)
    for q in range(NY):
        mom_out[:, q * LANES : (q + 1) * LANES] = blk_recv[q]
    for dst, count, ssem in sends:
        all_bytes(dst, count, ssem)


def local(weights, target, coupling, multipole_basis, rho_hist, res_hist, batch_atom, owner_slot, slot_index):
    points = weights.shape[0]
    batches = batch_atom.shape[0]
    tiles = points // LANES
    slots = owner_slot.shape[0]
    owned = slots // lax.axis_size("atom")
    scale = 1.0 / math.sqrt(points * lax.axis_size("grid") // owned)
    square = lambda v: v.reshape(tiles, LANES)
    vm, sm, dma = pltpu.VMEM, pltpu.SMEM, pltpu.SemaphoreType.DMA
    anywhere = pl.BlockSpec(memory_space=pl.ANY)
    vmem = pl.BlockSpec(memory_space=pltpu.VMEM)
    density, moments = pl.pallas_call(
        functools.partial(kernel, tiles, batches, scale),
        out_shape=(pltpu.VMEM((tiles, LANES), F32), pltpu.VMEM((LM, owned), F32)),
        in_specs=[anywhere] * 9,
        out_specs=(vmem, vmem),
        scratch_shapes=[
            vm((tiles, LANES), F32), vm((tiles, LANES), F32), vm((tiles, LANES), F32),
            vm((LM, points), F32), vm((H, points), F32), vm((H, points), F32),
            vm((tiles, LANES), F32), vm((tiles, LANES), F32), vm((16, 4, 8, LANES), F32), vm((batches // 8, 25, 8, LANES), F32), vm((25, 8, LANES), F32),
            sm((batches,), I32), sm((slots,), I32), sm((ITERS,), I32),
            vm((1, LANES), I32), vm((PLANE, 1, LANES), I32), vm((NZ, 1, LANES), I32),
            vm((ITERS, 1, LANES), F32), vm((ITERS, PLANE, 1, LANES), F32),
            vm((ITERS, 1, LANES), F32), vm((ITERS, NZ, 1, LANES), F32),
            vm((ITERS, 13, LANES), F32), vm((ITERS, PLANE, 13, LANES), F32),
            vm((LM, LANES), F32), vm((NZ, LM, LANES), F32),
            vm((ITERS, NZ, 13, LANES), F32), vm((ITERS, NZ, 13, LANES), F32),
            vm((LM, LANES), F32), vm((NY, LM, LANES), F32),
            vm((40, LANES), F32), vm((NC, NY * NX, 40, LANES), F32), vm((48, LANES), F32), vm((NC, NY * NX, 48, LANES), F32),
            vm((NZ * 64 + LANES, PLANE * 64), jnp.bfloat16), vm((96, PLANE * 64), jnp.bfloat16),
            vm((288, PLANE * 64), jnp.bfloat16), vm((176, LANES), F32), vm((32, LANES), F32),
            dma((9,)),
            dma, dma, dma, dma, dma((ITERS,)), dma((ITERS,)), dma((ITERS,)), dma((ITERS,)),
            dma((ITERS,)), dma((ITERS,)), dma, dma, dma((ITERS,)), dma((ITERS,)), dma, dma, dma, dma, dma, dma,
            dma, dma, dma, dma,
        ],
        compiler_params=pltpu.CompilerParams(collective_id=0, has_side_effects=True),
    )(
        square(weights), square(target), square(coupling), multipole_basis, rho_hist, res_hist,
        batch_atom, owner_slot, slot_index,
    )
    return density.reshape(points), moments


def solution(mesh):
    both = ("grid", "atom")
    placed = (P(both), P(both), P(both), P(None, both), P(None, both), P(None, both), P(both), P(), P())
    return jax.shard_map(
        local, mesh=mesh, in_specs=placed, out_specs=(P(both), P(None, "atom")), check_vma=False
    )
```

```python
import functools
import math

import jax
import jax.numpy as jnp
import numpy as np
from jax import lax
from jax.experimental import pallas as pl
from jax.experimental.pallas import tpu as pltpu
from jax.sharding import PartitionSpec as P

H = 8
LM = 25
ITERS = 2
BETA = 0.5
RIDGE = 0.1
LANES = 128
NZ, NY, NX, NC = 8, 4, 4, 2
PLANE = NY * NX * NC
MESH = pl.DeviceIdType.MESH
F32 = jnp.float32
I32 = jnp.int32


def kernel(
    tiles, batches, scale,
    w_hbm, tgt_hbm, cpl_hbm, basis_hbm, rho_hbm, res_hbm, atom_hbm, owner_hbm, hist_hbm,
    dens_out, mom_out,
    w, tgt, cpl, basis, rho, res, fresh, mixed, weighted, merged, hist_moms,
    atom_sm, owner_sm, hist_sm,
    slot_send, slot_recv, zslot_recv, irow_send, irow_recv, zrow_send, zrow_recv,
    raw_send, raw_recv, part_send, part_recv, back_send, back_recv, blk_send, blk_recv,
    early_send, early, keep_send, kept, match, xparts, xkept, own_kept, own_fresh,
    load_sem,
    slot_ss, slot_rs, zslot_ss, zslot_rs, irow_ss, irow_rs, zrow_ss, zrow_rs,
    raw_ss, raw_rs, part_ss, part_rs, back_ss, back_rs, blk_ss, blk_rs, keep_ss, keep_rs, pair_ss, pair_rs,
    early_ss, early_rs, epair_ss, epair_rs,
):
    grid = lax.axis_index("grid")
    atom = lax.axis_index("atom")
    z, y = grid // NY, grid % NY
    x, c = atom // NC, atom % NC
    me = y * (NX * NC) + atom

    ys = [(y + d) % NY for d in range(NY)]
    xs = [(x + d) % NX for d in range(NX)]
    peers = []
    for dy in (2, 1, 3, 0):
        for dx in (2, 1, 3, 0):
            for core in (0, 1) if dy or dx else (1 - c,):
                pa = xs[dx] * NC + core
                peers.append((z * NY + ys[dy], pa, ys[dy] * (NX * NC) + pa))
    zpeers = []
    zorder = [(z + dz) % NZ for dz in (4, 3, 5, 2, 6, 1, 7, 0)]
    for pz in zorder[:-1]:
        zpeers.append((pz * NY + y, atom, pz))
    spot = y * NX + x
    alike = [(pg, xs[dx] * NC + c, 0) for dy in (2, 1, 3, 0) for dx in (2, 1, 3, 0) if dy or dx for pg in [z * NY + ys[dy]]]
    other = [(grid, x * NC + 1 - c, 0)]
    ypeers = [(z * NY + ys[dy], atom, ys[dy]) for dy in (2, 1, 3)]

    barrier = pltpu.get_barrier_semaphore()
    for pg, pa, _ in peers + zpeers:
        pl.semaphore_signal(barrier, inc=1, device_id=(pg, pa), device_id_type=MESH)

    loads = [
        pltpu.make_async_copy(src, dst, load_sem.at[n])
        for n, (src, dst) in enumerate(
            [
                (w_hbm, w), (res_hbm, res), (basis_hbm, basis), (atom_hbm, atom_sm), (owner_hbm, owner_sm),
                (hist_hbm, hist_sm), (rho_hbm, rho), (tgt_hbm, tgt), (cpl_hbm, cpl),
            ]
        )
    ]
    for load in loads:
        load.start()

    sub = lax.broadcasted_iota(I32, (8, LANES), 0)
    lane = lax.broadcasted_iota(I32, (8, LANES), 1)
    low = lane < 64

    def to_peers(targets, src, dst, slot, ssem, rsem, later=False):
        for pg, pa, pslot in targets:
            pltpu.make_async_remote_copy(
                src_ref=src,
                dst_ref=dst.at[slot],
                send_sem=ssem,
                recv_sem=rsem,
                device_id=(pg, pa),
                device_id_type=MESH,
            ).start()
        if not later:
            sends.append((dst, len(targets), ssem))

    def all_bytes(dst, count, sem):
        span = dst.at[pl.ds(0, count)]
        pltpu.make_async_copy(span, span, sem).wait()

    def arrived(targets, dst, rsem):
        all_bytes(dst, len(targets), rsem)

    def tree_sum(parts):
        parts = list(parts)
        while len(parts) > 1:
            parts = [a + b for a, b in zip(parts[::2], parts[1::2])] + ([parts[-1]] if len(parts) % 2 else [])
        return parts[0]

    def over_subs(v):
        v = v + pltpu.roll(v, 4, 0)
        v = v + pltpu.roll(v, 2, 0)
        return v + pltpu.roll(v, 1, 0)

    def columns_of(at):
        return pl.ds(at * LANES if isinstance(at, int) else pl.multiple_of(at * LANES, LANES), LANES)

    def tile_at(ref, at):
        return ref[:, columns_of(at)]

    def row_at(ref, at):
        return jnp.broadcast_to(ref[pl.ds(at, 1), :], (8, LANES))

    def basis_tile(kt, at):
        cols = columns_of(at)
        if kt < 3:
            return basis[pl.ds(kt * 8, 8), cols]
        return jnp.broadcast_to(basis[pl.ds(24, 1), cols], (8, LANES))

    def row_of(columns):
        total = jnp.zeros((8, LANES), F32)
        for d, column in enumerate(columns):
            total = jnp.where(lane == d * 8 + sub, column, total)
        return over_subs(total)

    sends = []

    def all_summed(row, it):
        irow_send[it] = row[0:1]
        to_peers(peers, irow_send.at[it], irow_recv.at[it], me, irow_ss.at[it], irow_rs.at[it])
        return row

    def plane_sum(it):
        arrived(peers, irow_recv.at[it], irow_rs.at[it])
        row = tree_sum([irow_send[it]] + [irow_recv[it, pslot] for _, _, pslot in peers])
        zrow_send[it] = row
        to_peers(zpeers, zrow_send.at[it], zrow_recv.at[it], z, zrow_ss.at[it], zrow_rs.at[it])

    def slice_sum(it):
        arrived(zpeers, zrow_recv.at[it], zrow_rs.at[it])
        row = tree_sum([zrow_send[it]] + [zrow_recv[it, pslot] for _, _, pslot in zpeers])
        return jnp.broadcast_to(row, (8, LANES))

    def mixing(total):
        def entry(i, j):
            d = (i - j) % 8
            at = d * 8 + i if d <= 4 else (8 - d) * 8 + j
            return jnp.broadcast_to(total[:, at : at + 1], (8, LANES))

        a = {(i, j): entry(i, j) for i in range(H) for j in range(i + 1)}
        ridge = RIDGE * tree_sum([a[i, i] for i in range(H)]) / H
        for i in range(H):
            a[i, i] = a[i, i] + ridge
        ones = jnp.ones((8, LANES), F32)
        rhs = [ones] * H
        inverse = []
        factor = {}
        for k in range(H):
            inv = 1.0 / a[k, k]
            inverse.append(inv)
            for i in range(k + 1, H):
                factor[i, k] = a[i, k] * inv
            for i in range(k + 1, H):
                for j in range(k + 1, i + 1):
                    a[i, j] = a[i, j] - factor[i, k] * a[j, k]
                rhs[i] = rhs[i] - factor[i, k] * rhs[k]
        solved = [None] * H
        for k in reversed(range(H)):
            value = rhs[k] * inverse[k]
            for i in range(k + 1, H):
                value = value - factor[i, k] * solved[i]
            solved[k] = value
        share = 1.0 / tree_sum(solved)
        coeffs = [value * share for value in solved]
        column = coeffs[0]
        for i in range(1, H):
            column = jnp.where(sub == i, coeffs[i], column)
        return coeffs, column

    def merge(first, second, bit, axis):
        clear = ((lane if axis == 1 else sub) & bit) == 0
        return jnp.where(clear, first, second) + pltpu.roll(jnp.where(clear, second, first), bit, axis)

    def merge_all(values, bit, axis):
        while len(values) > 1:
            values = [merge(p, q, bit, axis) for p, q in zip(values[::2], values[1::2])]
            bit *= 2
        return values[0]

    def weigh(group):
        for u in range(16):
            at = group * 16 + u
            wrow = row_at(w, at)
            for kt in range(4):
                weighted[u, kt] = basis_tile(kt, at) * wrow

    def batch_sums(group, kt, field):
        return merge_all([weighted[2 * u, kt] * field(2 * u) + weighted[2 * u + 1, kt] * field(2 * u + 1) for u in range(8)], 1, 1)

    def joined(n):
        total = merge_all([merged[g, n] for g in range(batches // 8)], 8, 1)
        return total + pltpu.roll(total, 64, 1)

    def history_moments():
        def step(group, carry):
            weigh(group)

            def cols(u):
                return pl.ds(pl.multiple_of((group * 16 + u) * LANES, LANES), LANES)

            for i in range(H):
                for kt in range(3):
                    merged[group, i * 3 + kt] = batch_sums(
                        group, kt, lambda u: jnp.broadcast_to(res[pl.ds(i, 1), cols(u)], (8, LANES))
                    )
            merged[group, 24] = batch_sums(group, 3, lambda u: res[:, cols(u)])
            return carry

        lax.fori_loop(0, batches // 8, step, 0)
        for n in range(25):
            hist_moms[n] = joined(n)

    def fresh_moments():
        def step(group, carry):
            weigh(group)
            for kt in range(4):
                merged[group, kt] = batch_sums(group, kt, lambda u: row_at(fresh, group * 16 + u))
            return carry

        lax.fori_loop(0, batches // 8, step, 0)
        return [joined(kt) for kt in range(4)]

    def raw_moments(coeffs, column):
        return [tree_sum([coeffs[i] * hist_moms[i * 3 + kt] for i in range(H)]) for kt in range(3)] + [
            over_subs(column * hist_moms[24])
        ]

    def packed(t0, t1, t2, t3):
        first = jnp.where(low, t0, t1)
        second = jnp.where(
            sub < 4, jnp.where(low, t2, pltpu.roll(t2, 4, 0)), jnp.where((sub == 4) & low, t3, 0.0)
        )
        return first, second

    def unpacked(first, second):
        moved = pltpu.roll(second, 64, 1)
        t2 = jnp.where(sub < 4, second, pltpu.roll(moved, 4, 0))
        t3 = jnp.where(sub == 0, pltpu.roll(second, 4, 0), 0.0)
        return first, pltpu.roll(first, 64, 1), t2, t3

    def both_tiles(load):
        return load(pl.ds(0, 8)), pltpu.roll(load(pl.ds(5, 8)), 5, 0)

    def three(v):
        hi = v.astype(jnp.bfloat16)
        rest = v - hi.astype(F32)
        mid = rest.astype(jnp.bfloat16)
        lo = (rest - mid.astype(F32)).astype(jnp.bfloat16)
        return hi, mid, lo

    def pair_joined(a, b):
        return jnp.where(low, a, pltpu.roll(b, 64, 1)), jnp.where(low, pltpu.roll(a, 64, 1), b)

    def keep_moments(hist_at):
        def stays(j, kt):
            return jnp.where(hist_at > j, hist_moms[j * 3 + kt], hist_moms[(j + 1) * 3 + kt])

        tiles_of = [jnp.where(low, stays(j, 0), stays(j, 1)) for j in range(7)]
        tiles_of += [jnp.where(low, stays(2 * m, 2), stays(2 * m + 1, 2)) for m in range(3)]
        tiles_of += [jnp.where(low, stays(6, 2), hist_moms[24])]
        for n, value in enumerate(tiles_of):
            send, ref, at = (early_send, early, n) if n < 5 else (keep_send, kept, n - 5)
            send[at * 8 : at * 8 + 8, :] = value
            ref[c, spot, at * 8 : at * 8 + 8, :] = value

    def kept_tile(core, at, n):
        ref, n = (early, n) if n < 5 else (kept, n - 5)
        return ref[core, at, n * 8 : n * 8 + 8, :]

    def shares(coeffs, column, hist_at):
        own = [jnp.where(hist_at > j, coeffs[j], coeffs[j + 1]) for j in range(7)]
        fresh_share = tree_sum([jnp.where(hist_at == i, coeffs[i], 0.0) for i in range(H)])
        return own, fresh_share, jnp.where(sub == hist_at, 0.0, column)

    def combined(own, fresh_share, stay_column):
        doubles = [jnp.where(low, own[2 * m], own[2 * m + 1]) for m in range(3)]
        tail = jnp.where(low, own[6], stay_column)

        def of(core, at, new_first, new_second):
            t = [kept_tile(core, at, n) for n in range(11)]
            first = tree_sum([own[j] * t[j] for j in range(7)] + [fresh_share * new_first])
            u = tree_sum([doubles[m] * t[7 + m] for m in range(3)])
            v = tail * t[10]
            turned = pltpu.roll(v, 64, 1)
            t2 = u + pltpu.roll(u, 64, 1) + jnp.where(low, v, turned)
            second = jnp.where(
                sub < 4,
                jnp.where(low, t2, pltpu.roll(t2, 4, 0)),
                jnp.where((sub == 4) & low, over_subs(turned), 0.0),
            )
            return first, second + fresh_share * new_second

        return of

    def gather_parts(it, combine=None):
        for pair in range(PLANE // 2):
            cols = pl.ds(pair * LANES, LANES)
            raws = [both_tiles(lambda rows: raw_recv[it, 2 * pair + core, rows, :]) for core in range(2)]
            if combine:
                raws = [combine(core, pair, *raws[core]) for core in range(2)]
            for half in range(2):
                a, b = pair_joined(raws[0][half], raws[1][half])
                both = jnp.concatenate([a, b], axis=0)
                for n, part in enumerate(three(both)):
                    xparts[pl.ds(n * 32 + half * 16, 16), cols] = part

    def matched(first_row, count):
        sums = lax.dot_general(
            xparts[...], match[pl.ds(first_row, count), :], (((1,), (1,)), ((), ())), preferred_element_type=F32
        )
        return sums[0:32] + sums[32:64] + sums[64:96]

    def owner_kept(first, count):
        size = count * 16
        for pair in range(PLANE // 2):
            cols = pl.ds(pair * LANES, LANES)
            for n in range(count):
                both = pair_joined(kept_tile(0, pair, first + n), kept_tile(1, pair, first + n))
                for m, part in enumerate(three(jnp.concatenate(both, axis=0))):
                    xkept[pl.ds(m * size + n * 16, 16), cols] = part
        sums = lax.dot_general(
            xkept[pl.ds(0, 3 * size), :], match[pl.ds(NZ * 64, LANES), :], (((1,), (1,)), ((), ())), preferred_element_type=F32
        )
        own_kept[first * 16 : first * 16 + size] = sums[0:size] + sums[size : 2 * size] + sums[2 * size : 3 * size]

    def owner_fresh(it):
        gather_parts(it)
        own_fresh[...] = matched(NZ * 64, LANES)

    def owner_partial(own, fresh_share, stay_column):
        def of(n):
            return own_kept[n * 8 : n * 8 + 8]

        new = [fresh_share * own_fresh[n * 8 : n * 8 + 8] for n in range(4)]
        part_send[0:8] = tree_sum([own[j] * of(2 * j) for j in range(7)] + [new[0]])
        part_send[8:16] = tree_sum([own[j] * of(2 * j + 1) for j in range(7)] + [new[1]])
        part_send[16:24] = tree_sum(
            [own[j] * of(14 + j) for j in range(7)] + [jnp.where(sub < 4, new[2], pltpu.roll(new[3], 4, 0))]
        )
        part_send[24:25] = (over_subs(stay_column * of(21)) + pltpu.roll(new[2], 4, 0))[0:1]

    def peer_values(it, first):
        picked = matched(first * 64, LANES)
        for pair in range(1):
            cols = slice(pair * LANES, (pair + 1) * LANES)
            for half in range(2):
                values = pair_joined(picked[half * 16 : half * 16 + 8, cols], picked[half * 16 + 8 : half * 16 + 16, cols])
                for n, value in enumerate(values):
                    size = 5 if half else 8
                    back_send[it, first + 2 * pair + n, half * 8 : half * 8 + size, :] = value[0:size]

    def damped(kt, value):
        k = sub + kt * 8
        damp = jnp.where(k < 1, 1.0, jnp.where(k < 4, 1 / 2, jnp.where(k < 9, 1 / 3, jnp.where(k < 16, 1 / 4, 1 / 5))))
        return value * (damp * (scale * BETA))

    def send_raw(it, values):
        first, second = packed(*values)
        for ref, at in ((raw_send, (it,)), (raw_recv, (it, me))):
            ref[(*at, pl.ds(0, 8))] = first
            ref[(*at, pl.ds(8, 5))] = second[0:5]
        to_peers(peers, raw_send.at[it], raw_recv.at[it], me, raw_ss.at[it], raw_rs.at[it])

    loads[0].wait()
    loads[1].wait()

    def products(step_at, accs):
        accs = list(accs)
        for u in range(4):
            at = step_at * 4 + u
            r = tile_at(res, at)
            wr = r * row_at(w, at)
            accs[0] = accs[0] + wr * r
            for d in range(1, 5):
                accs[d] = accs[d] + wr * pltpu.roll(r, d, 0)
        return tuple(accs)

    accs = lax.fori_loop(0, tiles // 4, products, (jnp.zeros((8, LANES), F32),) * 5)
    first_row = row_of([jnp.sum(acc, axis=1, keepdims=True) for acc in accs])

    pl.semaphore_wait(barrier, len(peers) + len(zpeers))
    all_summed(first_row, 0)
    for load in loads[3:6]:
        load.wait()

    def slot_step(b, row):
        return jnp.where(lane == b, owner_sm[atom_sm[b]], row)

    slots = lax.fori_loop(0, batches, slot_step, jnp.full((8, LANES), -1, I32), unroll=4)
    slot_send[...] = slots[0:1]
    slot_recv[me] = slots[0:1]
    zslot_recv[z] = slots[0:1]
    to_peers(peers, slot_send, slot_recv, me, slot_ss, slot_rs)
    to_peers(zpeers, slot_send, zslot_recv, z, zslot_ss, zslot_rs)
    loads[2].wait()
    history_moments()
    for load in loads[6:]:
        load.wait()

    plane_sum(0)
    keep_moments(hist_sm[0])
    to_peers(alike, early_send, early.at[c], spot, early_ss, early_rs)

    arrived(peers, slot_recv, slot_rs)
    arrived(zpeers, zslot_recv, zslot_rs)
    first_slot = atom * 512 + y * LANES
    sources = []
    for pair in range(PLANE // 2):
        left = jnp.broadcast_to(slot_recv[2 * pair], (8, LANES))
        right = jnp.broadcast_to(slot_recv[2 * pair + 1], (8, LANES))
        sources.append(jnp.where(low, left, pltpu.roll(right, 64, 1)))

    def match_rows(at, wanted):
        for pair in range(PLANE // 2):
            halves = [jnp.where(sources[pair] == one, 1.0, 0.0) for one in wanted]
            match[pl.ds(at, 16), pl.ds(pair * LANES, LANES)] = jnp.concatenate(halves, axis=0).astype(jnp.bfloat16)

    for block, pz in enumerate(zorder):
        row = jnp.broadcast_to(zslot_recv[pz], (8, LANES)).astype(F32)

        def target_step(st, carry):
            wanted = []
            for h in range(2):
                hit = lane == sub + (st * 16 + h * 8)
                column = jnp.sum(jnp.where(hit, row, 0.0), axis=1, keepdims=True)
                wanted.append(jnp.broadcast_to(column, (8, LANES)).astype(I32))
            match_rows(pl.multiple_of(block * 64 + st * 16, 16), wanted)
            return carry

        lax.fori_loop(0, 4, target_step, 0)
    for st in range(LANES // 16):
        match_rows(NZ * 64 + st * 16, [sub + (first_slot + st * 16 + h * 8) for h in range(2)])

    total = slice_sum(0)
    for it in range(ITERS):
        last = it == ITERS - 1
        coeffs, column = mixing(total)
        if last:
            split = shares(coeffs, column, hist_sm[0])
            owner_partial(*split)
            to_peers(zpeers, part_send, part_recv, z, part_ss, part_rs)
            gather_parts(it, combined(*split))
        else:
            send_raw(it, raw_moments(coeffs, column))
            arrived(peers, raw_recv.at[it], raw_rs.at[it])
            to_peers(alike, keep_send, kept.at[c], spot, keep_ss, keep_rs)
            arrived(alike, early.at[0], early_rs)
            to_peers(other, early.at[c], early, c, epair_ss, epair_rs)
            gather_parts(it)
        for first in (0, 2, 4, 6):
            peer_values(it, first)
            for n, target in list(enumerate(zpeers))[first : first + 2]:
                to_peers([target], back_send.at[it, n], back_recv.at[it], z, back_ss.at[it], back_rs.at[it], True)
        sends.append((back_recv.at[it], len(zpeers), back_ss.at[it]))
        if last:
            arrived(zpeers, part_recv, part_rs)
            block = tree_sum([part_send[...]] + [part_recv[pslot] for _, _, pslot in zpeers]) * scale
            blk_send[...] = block
            to_peers(ypeers, blk_send, blk_recv, y, blk_ss, blk_rs)
            blk_recv[y] = block
        if not last:
            arrived(other, early, epair_rs)
            owner_kept(0, 5)
        arrived(zpeers, back_recv.at[it], back_rs.at[it])
        mine = both_tiles(
            lambda rows: tree_sum([back_send[it, NZ - 1, rows, :]] + [back_recv[it, pslot, rows, :] for _, _, pslot in zpeers])
        )
        at_batch = tuple(damped(kt, t) for kt, t in enumerate(unpacked(*mine)))
        hist_at = hist_sm[it]

        accs = []
        for group in range(batches // 4):
            rows = pl.ds(group * 8, 8)
            spread = [[jnp.broadcast_to(t[:, u : u + 1], (8, LANES)) for t in at_batch] for u in range(group * 4, group * 4 + 4)]
            parts = []
            for n in range(8):
                at = group * 8 + n
                v = column * (tile_at(rho, at) + BETA * tile_at(res, at))
                parts.append(v - tree_sum([basis_tile(kt, at) * spread[n // 2][kt] for kt in range(4)]))
            dens = merge_all(parts, 1, 0)
            if last:
                dens_out[rows, :] = dens
            else:
                new = tgt[rows, :] + cpl[rows, :] * jnp.tanh(dens) - dens
                fresh[rows, :] = new
                mixed[rows, :] = dens
                weighed = new * w[rows, :]
                for n in range(8):
                    r = jnp.where(
                        sub == hist_at, jnp.broadcast_to(new[n : n + 1], (8, LANES)), tile_at(res, group * 8 + n)
                    )
                    accs.append(r * jnp.broadcast_to(weighed[n : n + 1], (8, LANES)))
                accs = [tree_sum(accs)]

        if not last:
            mine_new = jnp.broadcast_to(jnp.sum(accs[0], axis=1, keepdims=True), (8, LANES))
            columns = [
                jnp.where(sub == hist_at, pltpu.roll(mine_new, d, 0) if d else mine_new, mine_new) for d in range(5)
            ]
            all_summed(row_of(columns), it + 1)
            send_raw(it + 1, fresh_moments())

            def replace(step_at, carry):
                for n in range(8):
                    at = step_at * 8 + n
                    cols = pl.ds(pl.multiple_of(at * LANES, LANES), LANES)
                    res[:, cols] = jnp.where(sub == hist_at, row_at(fresh, at), res[:, cols])
                    rho[:, cols] = jnp.where(sub == hist_at, row_at(mixed, at), rho[:, cols])
                return carry

            lax.fori_loop(0, tiles // 8, replace, 0)
            plane_sum(it + 1)
            arrived(alike, kept.at[0], keep_rs)
            to_peers(other, kept.at[c], kept, c, pair_ss, pair_rs)
            arrived(other, kept, pair_rs)
            owner_kept(5, 6)
            arrived(peers, raw_recv.at[it + 1], raw_rs.at[it + 1])
            owner_fresh(it + 1)
            row_i = lane % 8
            row_j = (row_i - lane // 8 + 8) % 8
            total = jnp.where((row_i == hist_at) | (row_j == hist_at), slice_sum(it + 1), total)

    arrived(ypeers, blk_recv, blk_rs)
    for q in range(NY):
        mom_out[:, q * LANES : (q + 1) * LANES] = blk_recv[q]
    for dst, count, ssem in sends:
        all_bytes(dst, count, ssem)


def local(weights, target, coupling, multipole_basis, rho_hist, res_hist, batch_atom, owner_slot, slot_index):
    points = weights.shape[0]
    batches = batch_atom.shape[0]
    tiles = points // LANES
    slots = owner_slot.shape[0]
    owned = slots // lax.axis_size("atom")
    scale = 1.0 / math.sqrt(points * lax.axis_size("grid") // owned)
    square = lambda v: v.reshape(tiles, LANES)
    vm, sm, dma = pltpu.VMEM, pltpu.SMEM, pltpu.SemaphoreType.DMA
    anywhere = pl.BlockSpec(memory_space=pl.ANY)
    vmem = pl.BlockSpec(memory_space=pltpu.VMEM)
    density, moments = pl.pallas_call(
        functools.partial(kernel, tiles, batches, scale),
        out_shape=(pltpu.VMEM((tiles, LANES), F32), pltpu.VMEM((LM, owned), F32)),
        in_specs=[anywhere] * 9,
        out_specs=(vmem, vmem),
        scratch_shapes=[
            vm((tiles, LANES), F32), vm((tiles, LANES), F32), vm((tiles, LANES), F32),
            vm((LM, points), F32), vm((H, points), F32), vm((H, points), F32),
            vm((tiles, LANES), F32), vm((tiles, LANES), F32), vm((16, 4, 8, LANES), F32), vm((batches // 8, 25, 8, LANES), F32), vm((25, 8, LANES), F32),
            sm((batches,), I32), sm((slots,), I32), sm((ITERS,), I32),
            vm((1, LANES), I32), vm((PLANE, 1, LANES), I32), vm((NZ, 1, LANES), I32),
            vm((ITERS, 1, LANES), F32), vm((ITERS, PLANE, 1, LANES), F32),
            vm((ITERS, 1, LANES), F32), vm((ITERS, NZ, 1, LANES), F32),
            vm((ITERS, 13, LANES), F32), vm((ITERS, PLANE, 13, LANES), F32),
            vm((LM, LANES), F32), vm((NZ, LM, LANES), F32),
            vm((ITERS, NZ, 13, LANES), F32), vm((ITERS, NZ, 13, LANES), F32),
            vm((LM, LANES), F32), vm((NY, LM, LANES), F32),
            vm((40, LANES), F32), vm((NC, NY * NX, 40, LANES), F32), vm((48, LANES), F32), vm((NC, NY * NX, 48, LANES), F32),
            vm((NZ * 64 + LANES, PLANE * 64), jnp.bfloat16), vm((96, PLANE * 64), jnp.bfloat16),
            vm((288, PLANE * 64), jnp.bfloat16), vm((176, LANES), F32), vm((32, LANES), F32),
            dma((9,)),
            dma, dma, dma, dma, dma((ITERS,)), dma((ITERS,)), dma((ITERS,)), dma((ITERS,)),
            dma((ITERS,)), dma((ITERS,)), dma, dma, dma((ITERS,)), dma((ITERS,)), dma, dma, dma, dma, dma, dma,
            dma, dma, dma, dma,
        ],
        compiler_params=pltpu.CompilerParams(collective_id=0, has_side_effects=True),
    )(
        square(weights), square(target), square(coupling), multipole_basis, rho_hist, res_hist,
        batch_atom, owner_slot, slot_index,
    )
    def finish(d_in, m_in, d_out, m_out, sem):
        copies = [pltpu.make_async_copy(d_in, d_out, sem.at[0]), pltpu.make_async_copy(m_in, m_out, sem.at[1])]
        for copy in copies:
            copy.start()
        for copy in copies:
            copy.wait()

    density, moments = pl.pallas_call(
        finish,
        out_shape=(jax.ShapeDtypeStruct((tiles, LANES), F32), jax.ShapeDtypeStruct((LM, owned), F32)),
        in_specs=[vmem] * 2,
        out_specs=(anywhere, anywhere),
        scratch_shapes=[dma((2,))],
    )(pltpu.with_memory_space_constraint(density, pltpu.VMEM), pltpu.with_memory_space_constraint(moments, pltpu.VMEM))
    return density.reshape(points), moments


def solution(mesh):
    both = ("grid", "atom")
    placed = (P(both), P(both), P(both), P(None, both), P(None, both), P(None, both), P(both), P(), P())
    return jax.shard_map(
        local, mesh=mesh, in_specs=placed, out_specs=(P(both), P(None, "atom")), check_vma=False
    )
```

```python
import functools
import math

import jax
import jax.numpy as jnp
import numpy as np
from jax import lax
from jax.experimental import pallas as pl
from jax.experimental.pallas import tpu as pltpu
from jax.sharding import PartitionSpec as P

H = 8
LM = 25
ITERS = 2
BETA = 0.5
RIDGE = 0.1
LANES = 128
NZ, NY, NX, NC = 8, 4, 4, 2
PLANE = NY * NX * NC
MESH = pl.DeviceIdType.MESH
F32 = jnp.float32
I32 = jnp.int32


def kernel(
    tiles, batches, scale,
    w_hbm, tgt_hbm, cpl_hbm, basis_hbm, rho_hbm, res_hbm, atom_hbm, owner_hbm, hist_hbm,
    dens_out, mom_out,
    w, tgt, cpl, basis, rho, res, fresh, mixed, weighted, merged, hist_moms,
    atom_sm, owner_sm, hist_sm,
    slot_send, slot_recv, zslot_recv, irow_send, irow_recv, zrow_send, zrow_recv,
    raw_send, raw_recv, part_send, part_recv, back_send, back_recv, blk_send, blk_recv,
    early_send, early, keep_send, kept, match, xparts, xkept, own_kept, own_fresh,
    load_sem,
    slot_ss, slot_rs, zslot_ss, zslot_rs, irow_ss, irow_rs, zrow_ss, zrow_rs,
    raw_ss, raw_rs, part_ss, part_rs, back_ss, back_rs, blk_ss, blk_rs, keep_ss, keep_rs, pair_ss, pair_rs,
    early_ss, early_rs, epair_ss, epair_rs,
):
    grid = lax.axis_index("grid")
    atom = lax.axis_index("atom")
    z, y = grid // NY, grid % NY
    x, c = atom // NC, atom % NC
    me = y * (NX * NC) + atom

    ys = [(y + d) % NY for d in range(NY)]
    xs = [(x + d) % NX for d in range(NX)]
    peers = []
    for dy in (2, 1, 3, 0):
        for dx in (2, 1, 3, 0):
            for core in (0, 1) if dy or dx else (1 - c,):
                pa = xs[dx] * NC + core
                peers.append((z * NY + ys[dy], pa, ys[dy] * (NX * NC) + pa))
    zpeers = []
    zorder = [(z + dz) % NZ for dz in (4, 3, 5, 2, 6, 1, 7, 0)]
    for pz in zorder[:-1]:
        zpeers.append((pz * NY + y, atom, pz))
    spot = y * NX + x
    alike = [(pg, xs[dx] * NC + c, 0) for dy in (2, 1, 3, 0) for dx in (2, 1, 3, 0) if dy or dx for pg in [z * NY + ys[dy]]]
    other = [(grid, x * NC + 1 - c, 0)]
    ypeers = [(z * NY + ys[dy], atom, ys[dy]) for dy in (2, 1, 3)]

    barrier = pltpu.get_barrier_semaphore()
    for pg, pa, _ in zpeers[:3] + peers + zpeers[3:]:
        pl.semaphore_signal(barrier, inc=1, device_id=(pg, pa), device_id_type=MESH)

    loads = [
        pltpu.make_async_copy(src, dst, load_sem.at[n])
        for n, (src, dst) in enumerate(
            [
                (w_hbm, w), (res_hbm, res), (basis_hbm, basis), (atom_hbm, atom_sm), (owner_hbm, owner_sm),
                (hist_hbm, hist_sm), (rho_hbm, rho), (tgt_hbm, tgt), (cpl_hbm, cpl),
            ]
        )
    ]
    for load in loads:
        load.start()

    sub = lax.broadcasted_iota(I32, (8, LANES), 0)
    lane = lax.broadcasted_iota(I32, (8, LANES), 1)
    low = lane < 64

    def to_peers(targets, src, dst, slot, ssem, rsem, later=False):
        for pg, pa, pslot in targets:
            pltpu.make_async_remote_copy(
                src_ref=src,
                dst_ref=dst.at[slot],
                send_sem=ssem,
                recv_sem=rsem,
                device_id=(pg, pa),
                device_id_type=MESH,
            ).start()
        if not later:
            sends.append((dst, len(targets), ssem))

    def all_bytes(dst, count, sem):
        span = dst.at[pl.ds(0, count)]
        pltpu.make_async_copy(span, span, sem).wait()

    def arrived(targets, dst, rsem):
        all_bytes(dst, len(targets), rsem)

    def tree_sum(parts):
        parts = list(parts)
        while len(parts) > 1:
            parts = [a + b for a, b in zip(parts[::2], parts[1::2])] + ([parts[-1]] if len(parts) % 2 else [])
        return parts[0]

    def over_subs(v):
        v = v + pltpu.roll(v, 4, 0)
        v = v + pltpu.roll(v, 2, 0)
        return v + pltpu.roll(v, 1, 0)

    def columns_of(at):
        return pl.ds(at * LANES if isinstance(at, int) else pl.multiple_of(at * LANES, LANES), LANES)

    def tile_at(ref, at):
        return ref[:, columns_of(at)]

    def row_at(ref, at):
        return jnp.broadcast_to(ref[pl.ds(at, 1), :], (8, LANES))

    def basis_tile(kt, at):
        cols = columns_of(at)
        if kt < 3:
            return basis[pl.ds(kt * 8, 8), cols]
        return jnp.broadcast_to(basis[pl.ds(24, 1), cols], (8, LANES))

    def row_of(columns):
        total = jnp.zeros((8, LANES), F32)
        for d, column in enumerate(columns):
            total = jnp.where(lane == d * 8 + sub, column, total)
        return over_subs(total)

    sends = []

    def all_summed(row, it):
        irow_send[it] = row[0:1]
        to_peers(peers, irow_send.at[it], irow_recv.at[it], me, irow_ss.at[it], irow_rs.at[it])
        return row

    def plane_sum(it):
        arrived(peers, irow_recv.at[it], irow_rs.at[it])
        row = tree_sum([irow_send[it]] + [irow_recv[it, pslot] for _, _, pslot in peers])
        zrow_send[it] = row
        to_peers(zpeers, zrow_send.at[it], zrow_recv.at[it], z, zrow_ss.at[it], zrow_rs.at[it])

    def slice_sum(it):
        arrived(zpeers, zrow_recv.at[it], zrow_rs.at[it])
        row = tree_sum([zrow_send[it]] + [zrow_recv[it, pslot] for _, _, pslot in zpeers])
        return jnp.broadcast_to(row, (8, LANES))

    def mixing(total):
        def entry(i, j):
            d = (i - j) % 8
            at = d * 8 + i if d <= 4 else (8 - d) * 8 + j
            return jnp.broadcast_to(total[:, at : at + 1], (8, LANES))

        a = {(i, j): entry(i, j) for i in range(H) for j in range(i + 1)}
        ridge = RIDGE * tree_sum([a[i, i] for i in range(H)]) / H
        for i in range(H):
            a[i, i] = a[i, i] + ridge
        ones = jnp.ones((8, LANES), F32)
        rhs = [ones] * H
        inverse = []
        factor = {}
        for k in range(H):
            inv = 1.0 / a[k, k]
            inverse.append(inv)
            for i in range(k + 1, H):
                factor[i, k] = a[i, k] * inv
            for i in range(k + 1, H):
                for j in range(k + 1, i + 1):
                    a[i, j] = a[i, j] - factor[i, k] * a[j, k]
                rhs[i] = rhs[i] - factor[i, k] * rhs[k]
        solved = [None] * H
        for k in reversed(range(H)):
            value = rhs[k] * inverse[k]
            for i in range(k + 1, H):
                value = value - factor[i, k] * solved[i]
            solved[k] = value
        share = 1.0 / tree_sum(solved)
        coeffs = [value * share for value in solved]
        column = coeffs[0]
        for i in range(1, H):
            column = jnp.where(sub == i, coeffs[i], column)
        return coeffs, column

    def merge(first, second, bit, axis):
        clear = ((lane if axis == 1 else sub) & bit) == 0
        return jnp.where(clear, first, second) + pltpu.roll(jnp.where(clear, second, first), bit, axis)

    def merge_all(values, bit, axis):
        while len(values) > 1:
            values = [merge(p, q, bit, axis) for p, q in zip(values[::2], values[1::2])]
            bit *= 2
        return values[0]

    def weigh(group):
        for u in range(16):
            at = group * 16 + u
            wrow = row_at(w, at)
            for kt in range(4):
                weighted[u, kt] = basis_tile(kt, at) * wrow

    def batch_sums(group, kt, field):
        return merge_all([weighted[2 * u, kt] * field(2 * u) + weighted[2 * u + 1, kt] * field(2 * u + 1) for u in range(8)], 1, 1)

    def joined(n):
        total = merge_all([merged[g, n] for g in range(batches // 8)], 8, 1)
        return total + pltpu.roll(total, 64, 1)

    def history_moments():
        def step(group, carry):
            weigh(group)

            def cols(u):
                return pl.ds(pl.multiple_of((group * 16 + u) * LANES, LANES), LANES)

            for i in range(H):
                for kt in range(3):
                    merged[group, i * 3 + kt] = batch_sums(
                        group, kt, lambda u: jnp.broadcast_to(res[pl.ds(i, 1), cols(u)], (8, LANES))
                    )
            merged[group, 24] = batch_sums(group, 3, lambda u: res[:, cols(u)])
            return carry

        lax.fori_loop(0, batches // 8, step, 0)
        for n in range(25):
            hist_moms[n] = joined(n)

    def fresh_moments():
        def step(group, carry):
            weigh(group)
            for kt in range(4):
                merged[group, kt] = batch_sums(group, kt, lambda u: row_at(fresh, group * 16 + u))
            return carry

        lax.fori_loop(0, batches // 8, step, 0)
        return [joined(kt) for kt in range(4)]

    def raw_moments(coeffs, column):
        return [tree_sum([coeffs[i] * hist_moms[i * 3 + kt] for i in range(H)]) for kt in range(3)] + [
            over_subs(column * hist_moms[24])
        ]

    def packed(t0, t1, t2, t3):
        first = jnp.where(low, t0, t1)
        second = jnp.where(
            sub < 4, jnp.where(low, t2, pltpu.roll(t2, 4, 0)), jnp.where((sub == 4) & low, t3, 0.0)
        )
        return first, second

    def unpacked(first, second):
        moved = pltpu.roll(second, 64, 1)
        t2 = jnp.where(sub < 4, second, pltpu.roll(moved, 4, 0))
        t3 = jnp.where(sub == 0, pltpu.roll(second, 4, 0), 0.0)
        return first, pltpu.roll(first, 64, 1), t2, t3

    def both_tiles(load):
        return load(pl.ds(0, 8)), pltpu.roll(load(pl.ds(5, 8)), 5, 0)

    def three(v):
        hi = v.astype(jnp.bfloat16)
        rest = v - hi.astype(F32)
        mid = rest.astype(jnp.bfloat16)
        lo = (rest - mid.astype(F32)).astype(jnp.bfloat16)
        return hi, mid, lo

    def pair_joined(a, b):
        return jnp.where(low, a, pltpu.roll(b, 64, 1)), jnp.where(low, pltpu.roll(a, 64, 1), b)

    def keep_moments(hist_at):
        def stays(j, kt):
            return jnp.where(hist_at > j, hist_moms[j * 3 + kt], hist_moms[(j + 1) * 3 + kt])

        tiles_of = [jnp.where(low, stays(j, 0), stays(j, 1)) for j in range(7)]
        tiles_of += [jnp.where(low, stays(2 * m, 2), stays(2 * m + 1, 2)) for m in range(3)]
        tiles_of += [jnp.where(low, stays(6, 2), hist_moms[24])]
        for n, value in enumerate(tiles_of):
            send, ref, at = (early_send, early, n) if n < 5 else (keep_send, kept, n - 5)
            send[at * 8 : at * 8 + 8, :] = value
            ref[c, spot, at * 8 : at * 8 + 8, :] = value

    def kept_tile(core, at, n):
        ref, n = (early, n) if n < 5 else (kept, n - 5)
        return ref[core, at, n * 8 : n * 8 + 8, :]

    def shares(coeffs, column, hist_at):
        own = [jnp.where(hist_at > j, coeffs[j], coeffs[j + 1]) for j in range(7)]
        fresh_share = tree_sum([jnp.where(hist_at == i, coeffs[i], 0.0) for i in range(H)])
        return own, fresh_share, jnp.where(sub == hist_at, 0.0, column)

    def combined(own, fresh_share, stay_column):
        doubles = [jnp.where(low, own[2 * m], own[2 * m + 1]) for m in range(3)]
        tail = jnp.where(low, own[6], stay_column)

        def of(core, at, new_first, new_second):
            t = [kept_tile(core, at, n) for n in range(11)]
            first = tree_sum([own[j] * t[j] for j in range(7)] + [fresh_share * new_first])
            u = tree_sum([doubles[m] * t[7 + m] for m in range(3)])
            v = tail * t[10]
            turned = pltpu.roll(v, 64, 1)
            t2 = u + pltpu.roll(u, 64, 1) + jnp.where(low, v, turned)
            second = jnp.where(
                sub < 4,
                jnp.where(low, t2, pltpu.roll(t2, 4, 0)),
                jnp.where((sub == 4) & low, over_subs(turned), 0.0),
            )
            return first, second + fresh_share * new_second

        return of

    def gather_parts(it, combine=None):
        for pair in range(PLANE // 2):
            cols = pl.ds(pair * LANES, LANES)
            raws = [both_tiles(lambda rows: raw_recv[it, 2 * pair + core, rows, :]) for core in range(2)]
            if combine:
                raws = [combine(core, pair, *raws[core]) for core in range(2)]
            for half in range(2):
                a, b = pair_joined(raws[0][half], raws[1][half])
                both = jnp.concatenate([a, b], axis=0)
                for n, part in enumerate(three(both)):
                    xparts[pl.ds(n * 32 + half * 16, 16), cols] = part

    def matched(first_row, count):
        sums = lax.dot_general(
            xparts[...], match[pl.ds(first_row, count), :], (((1,), (1,)), ((), ())), preferred_element_type=F32
        )
        return sums[0:32] + sums[32:64] + sums[64:96]

    def owner_kept(first, count):
        size = count * 16
        for pair in range(PLANE // 2):
            cols = pl.ds(pair * LANES, LANES)
            for n in range(count):
                both = pair_joined(kept_tile(0, pair, first + n), kept_tile(1, pair, first + n))
                for m, part in enumerate(three(jnp.concatenate(both, axis=0))):
                    xkept[pl.ds(m * size + n * 16, 16), cols] = part
        sums = lax.dot_general(
            xkept[pl.ds(0, 3 * size), :], match[pl.ds(NZ * 64, LANES), :], (((1,), (1,)), ((), ())), preferred_element_type=F32
        )
        own_kept[first * 16 : first * 16 + size] = sums[0:size] + sums[size : 2 * size] + sums[2 * size : 3 * size]

    def owner_fresh(it):
        gather_parts(it)
        own_fresh[...] = matched(NZ * 64, LANES)

    def owner_partial(own, fresh_share, stay_column):
        def of(n):
            return own_kept[n * 8 : n * 8 + 8]

        new = [fresh_share * own_fresh[n * 8 : n * 8 + 8] for n in range(4)]
        part_send[0:8] = tree_sum([own[j] * of(2 * j) for j in range(7)] + [new[0]])
        part_send[8:16] = tree_sum([own[j] * of(2 * j + 1) for j in range(7)] + [new[1]])
        part_send[16:24] = tree_sum(
            [own[j] * of(14 + j) for j in range(7)] + [jnp.where(sub < 4, new[2], pltpu.roll(new[3], 4, 0))]
        )
        part_send[24:25] = (over_subs(stay_column * of(21)) + pltpu.roll(new[2], 4, 0))[0:1]

    def peer_values(it, first):
        picked = matched(first * 64, LANES)
        for pair in range(1):
            cols = slice(pair * LANES, (pair + 1) * LANES)
            for half in range(2):
                values = pair_joined(picked[half * 16 : half * 16 + 8, cols], picked[half * 16 + 8 : half * 16 + 16, cols])
                for n, value in enumerate(values):
                    size = 5 if half else 8
                    back_send[it, first + 2 * pair + n, half * 8 : half * 8 + size, :] = value[0:size]

    def damped(kt, value):
        k = sub + kt * 8
        damp = jnp.where(k < 1, 1.0, jnp.where(k < 4, 1 / 2, jnp.where(k < 9, 1 / 3, jnp.where(k < 16, 1 / 4, 1 / 5))))
        return value * (damp * (scale * BETA))

    def send_raw(it, values):
        first, second = packed(*values)
        for ref, at in ((raw_send, (it,)), (raw_recv, (it, me))):
            ref[(*at, pl.ds(0, 8))] = first
            ref[(*at, pl.ds(8, 5))] = second[0:5]
        to_peers(peers, raw_send.at[it], raw_recv.at[it], me, raw_ss.at[it], raw_rs.at[it])

    loads[0].wait()
    loads[1].wait()

    def products(step_at, accs):
        accs = list(accs)
        for u in range(4):
            at = step_at * 4 + u
            r = tile_at(res, at)
            wr = r * row_at(w, at)
            accs[0] = accs[0] + wr * r
            for d in range(1, 5):
                accs[d] = accs[d] + wr * pltpu.roll(r, d, 0)
        return tuple(accs)

    accs = lax.fori_loop(0, tiles // 4, products, (jnp.zeros((8, LANES), F32),) * 5)
    first_row = row_of([jnp.sum(acc, axis=1, keepdims=True) for acc in accs])

    pl.semaphore_wait(barrier, len(peers) + len(zpeers))
    all_summed(first_row, 0)
    for load in loads[3:6]:
        load.wait()

    def slot_step(b, row):
        return jnp.where(lane == b, owner_sm[atom_sm[b]], row)

    slots = lax.fori_loop(0, batches, slot_step, jnp.full((8, LANES), -1, I32), unroll=4)
    slot_send[...] = slots[0:1]
    slot_recv[me] = slots[0:1]
    zslot_recv[z] = slots[0:1]
    to_peers(peers, slot_send, slot_recv, me, slot_ss, slot_rs)
    to_peers(zpeers, slot_send, zslot_recv, z, zslot_ss, zslot_rs)
    loads[2].wait()
    history_moments()
    for load in loads[6:]:
        load.wait()

    plane_sum(0)
    keep_moments(hist_sm[0])
    to_peers(alike, early_send, early.at[c], spot, early_ss, early_rs)

    arrived(peers, slot_recv, slot_rs)
    arrived(zpeers, zslot_recv, zslot_rs)
    first_slot = atom * 512 + y * LANES
    sources = []
    for pair in range(PLANE // 2):
        left = jnp.broadcast_to(slot_recv[2 * pair], (8, LANES))
        right = jnp.broadcast_to(slot_recv[2 * pair + 1], (8, LANES))
        sources.append(jnp.where(low, left, pltpu.roll(right, 64, 1)))

    def match_rows(at, wanted):
        for pair in range(PLANE // 2):
            halves = [jnp.where(sources[pair] == one, 1.0, 0.0) for one in wanted]
            match[pl.ds(at, 16), pl.ds(pair * LANES, LANES)] = jnp.concatenate(halves, axis=0).astype(jnp.bfloat16)

    for block, pz in enumerate(zorder):
        row = jnp.broadcast_to(zslot_recv[pz], (8, LANES)).astype(F32)

        def target_step(st, carry):
            wanted = []
            for h in range(2):
                hit = lane == sub + (st * 16 + h * 8)
                column = jnp.sum(jnp.where(hit, row, 0.0), axis=1, keepdims=True)
                wanted.append(jnp.broadcast_to(column, (8, LANES)).astype(I32))
            match_rows(pl.multiple_of(block * 64 + st * 16, 16), wanted)
            return carry

        lax.fori_loop(0, 4, target_step, 0)
    for st in range(LANES // 16):
        match_rows(NZ * 64 + st * 16, [sub + (first_slot + st * 16 + h * 8) for h in range(2)])

    total = slice_sum(0)
    for it in range(ITERS):
        last = it == ITERS - 1
        coeffs, column = mixing(total)
        if last:
            split = shares(coeffs, column, hist_sm[0])
            owner_partial(*split)
            to_peers(zpeers, part_send, part_recv, z, part_ss, part_rs)
            gather_parts(it, combined(*split))
        else:
            send_raw(it, raw_moments(coeffs, column))
            arrived(peers, raw_recv.at[it], raw_rs.at[it])
            to_peers(alike, keep_send, kept.at[c], spot, keep_ss, keep_rs)
            arrived(alike, early.at[0], early_rs)
            to_peers(other, early.at[c], early, c, epair_ss, epair_rs)
            gather_parts(it)
        for first in (0, 2, 4, 6):
            peer_values(it, first)
            for n, target in list(enumerate(zpeers))[first : first + 2]:
                to_peers([target], back_send.at[it, n], back_recv.at[it], z, back_ss.at[it], back_rs.at[it], True)
        sends.append((back_recv.at[it], len(zpeers), back_ss.at[it]))
        if last:
            arrived(zpeers, part_recv, part_rs)
            block = tree_sum([part_send[...]] + [part_recv[pslot] for _, _, pslot in zpeers]) * scale
            blk_send[...] = block
            to_peers(ypeers, blk_send, blk_recv, y, blk_ss, blk_rs)
            blk_recv[y] = block
        if not last:
            arrived(other, early, epair_rs)
            owner_kept(0, 5)
        arrived(zpeers, back_recv.at[it], back_rs.at[it])
        mine = both_tiles(
            lambda rows: tree_sum([back_send[it, NZ - 1, rows, :]] + [back_recv[it, pslot, rows, :] for _, _, pslot in zpeers])
        )
        at_batch = tuple(damped(kt, t) for kt, t in enumerate(unpacked(*mine)))
        hist_at = hist_sm[it]

        accs = []
        for group in range(batches // 4):
            rows = pl.ds(group * 8, 8)
            spread = [[jnp.broadcast_to(t[:, u : u + 1], (8, LANES)) for t in at_batch] for u in range(group * 4, group * 4 + 4)]
            parts = []
            for n in range(8):
                at = group * 8 + n
                v = column * (tile_at(rho, at) + BETA * tile_at(res, at))
                parts.append(v - tree_sum([basis_tile(kt, at) * spread[n // 2][kt] for kt in range(4)]))
            dens = merge_all(parts, 1, 0)
            if last:
                dens_out[rows, :] = dens
            else:
                new = tgt[rows, :] + cpl[rows, :] * jnp.tanh(dens) - dens
                fresh[rows, :] = new
                mixed[rows, :] = dens
                weighed = new * w[rows, :]
                for n in range(8):
                    r = jnp.where(
                        sub == hist_at, jnp.broadcast_to(new[n : n + 1], (8, LANES)), tile_at(res, group * 8 + n)
                    )
                    accs.append(r * jnp.broadcast_to(weighed[n : n + 1], (8, LANES)))
                accs = [tree_sum(accs)]

        if not last:
            mine_new = jnp.broadcast_to(jnp.sum(accs[0], axis=1, keepdims=True), (8, LANES))
            columns = [
                jnp.where(sub == hist_at, pltpu.roll(mine_new, d, 0) if d else mine_new, mine_new) for d in range(5)
            ]
            all_summed(row_of(columns), it + 1)
            send_raw(it + 1, fresh_moments())

            plane_sum(it + 1)
            def replace(step_at, carry):
                for n in range(8):
                    at = step_at * 8 + n
                    cols = pl.ds(pl.multiple_of(at * LANES, LANES), LANES)
                    res[:, cols] = jnp.where(sub == hist_at, row_at(fresh, at), res[:, cols])
                    rho[:, cols] = jnp.where(sub == hist_at, row_at(mixed, at), rho[:, cols])
                return carry

            lax.fori_loop(0, tiles // 8, replace, 0)
            arrived(alike, kept.at[0], keep_rs)
            to_peers(other, kept.at[c], kept, c, pair_ss, pair_rs)
            arrived(other, kept, pair_rs)
            owner_kept(5, 6)
            arrived(peers, raw_recv.at[it + 1], raw_rs.at[it + 1])
            owner_fresh(it + 1)
            row_i = lane % 8
            row_j = (row_i - lane // 8 + 8) % 8
            total = jnp.where((row_i == hist_at) | (row_j == hist_at), slice_sum(it + 1), total)

    arrived(ypeers, blk_recv, blk_rs)
    for q in range(NY):
        mom_out[:, q * LANES : (q + 1) * LANES] = blk_recv[q]
    for dst, count, ssem in sends:
        all_bytes(dst, count, ssem)


def local(weights, target, coupling, multipole_basis, rho_hist, res_hist, batch_atom, owner_slot, slot_index):
    points = weights.shape[0]
    batches = batch_atom.shape[0]
    tiles = points // LANES
    slots = owner_slot.shape[0]
    owned = slots // lax.axis_size("atom")
    scale = 1.0 / math.sqrt(points * lax.axis_size("grid") // owned)
    square = lambda v: v.reshape(tiles, LANES)
    vm, sm, dma = pltpu.VMEM, pltpu.SMEM, pltpu.SemaphoreType.DMA
    anywhere = pl.BlockSpec(memory_space=pl.ANY)
    vmem = pl.BlockSpec(memory_space=pltpu.VMEM)
    density, moments = pl.pallas_call(
        functools.partial(kernel, tiles, batches, scale),
        out_shape=(pltpu.VMEM((tiles, LANES), F32), pltpu.VMEM((LM, owned), F32)),
        in_specs=[anywhere] * 9,
        out_specs=(vmem, vmem),
        scratch_shapes=[
            vm((tiles, LANES), F32), vm((tiles, LANES), F32), vm((tiles, LANES), F32),
            vm((LM, points), F32), vm((H, points), F32), vm((H, points), F32),
            vm((tiles, LANES), F32), vm((tiles, LANES), F32), vm((16, 4, 8, LANES), F32), vm((batches // 8, 25, 8, LANES), F32), vm((25, 8, LANES), F32),
            sm((batches,), I32), sm((slots,), I32), sm((ITERS,), I32),
            vm((1, LANES), I32), vm((PLANE, 1, LANES), I32), vm((NZ, 1, LANES), I32),
            vm((ITERS, 1, LANES), F32), vm((ITERS, PLANE, 1, LANES), F32),
            vm((ITERS, 1, LANES), F32), vm((ITERS, NZ, 1, LANES), F32),
            vm((ITERS, 13, LANES), F32), vm((ITERS, PLANE, 13, LANES), F32),
            vm((LM, LANES), F32), vm((NZ, LM, LANES), F32),
            vm((ITERS, NZ, 13, LANES), F32), vm((ITERS, NZ, 13, LANES), F32),
            vm((LM, LANES), F32), vm((NY, LM, LANES), F32),
            vm((40, LANES), F32), vm((NC, NY * NX, 40, LANES), F32), vm((48, LANES), F32), vm((NC, NY * NX, 48, LANES), F32),
            vm((NZ * 64 + LANES, PLANE * 64), jnp.bfloat16), vm((96, PLANE * 64), jnp.bfloat16),
            vm((288, PLANE * 64), jnp.bfloat16), vm((176, LANES), F32), vm((32, LANES), F32),
            dma((9,)),
            dma, dma, dma, dma, dma((ITERS,)), dma((ITERS,)), dma((ITERS,)), dma((ITERS,)),
            dma((ITERS,)), dma((ITERS,)), dma, dma, dma((ITERS,)), dma((ITERS,)), dma, dma, dma, dma, dma, dma,
            dma, dma, dma, dma,
        ],
        compiler_params=pltpu.CompilerParams(collective_id=0, has_side_effects=True),
    )(
        square(weights), square(target), square(coupling), multipole_basis, rho_hist, res_hist,
        batch_atom, owner_slot, slot_index,
    )
    def finish(d_in, m_in, d_out, m_out, sem):
        copies = [pltpu.make_async_copy(d_in, d_out, sem.at[0]), pltpu.make_async_copy(m_in, m_out, sem.at[1])]
        for copy in copies:
            copy.start()
        for copy in copies:
            copy.wait()

    density, moments = pl.pallas_call(
        finish,
        out_shape=(jax.ShapeDtypeStruct((tiles, LANES), F32), jax.ShapeDtypeStruct((LM, owned), F32)),
        in_specs=[vmem] * 2,
        out_specs=(anywhere, anywhere),
        scratch_shapes=[dma((2,))],
    )(pltpu.with_memory_space_constraint(density, pltpu.VMEM), pltpu.with_memory_space_constraint(moments, pltpu.VMEM))
    return density.reshape(points), moments


def solution(mesh):
    both = ("grid", "atom")
    placed = (P(both), P(both), P(both), P(None, both), P(None, both), P(None, both), P(both), P(), P())
    return jax.shard_map(
        local, mesh=mesh, in_specs=placed, out_specs=(P(both), P(None, "atom")), check_vma=False
    )
```
